128 devices in a mesh: gx: 2 (over core), gy: 4 (over x), gz: 16 (over z, y).
Axes of the slice: x: 4, y: 4, z: 4, core: 2. Of those that a mesh axis runs over, the one named last changes fastest.
Arguments:
- right_side: float32 [96, 192, 768], P('gx', 'gy', 'gz'), may hold values from -6 to 6
- face_coef: float32 [3, 96, 192, 768], P(None, 'gx', 'gy', 'gz'), may hold values from 0.3 to 3
- absorption: float32 [96, 192, 768], P('gx', 'gy', 'gz'), may hold values from 0.001 to 0.01
Outputs:
- solution: float32 [96, 192, 768], P('gx', 'gy', 'gz')
- residual: float32 [96, 192, 768], P('gx', 'gy', 'gz')
- relative_norm: float32 [], replicated
The draws below stay inside these ranges and needn't reach their ends.
All inputs are finite; a program needn't handle non-finite values.
Results may differ from the reference program's by a relative error of at most 0.0003.
Values sent between devices are 32-bit elements.
A program may use at most 192 MiB of HBM per device.

```python
import math
import jax
import jax.numpy as jnp
from jax import lax

LEVELS = 5
SWEEPS = 3
BOTTOM = 6
NX = 96
NY = 192
NZ = 768


def block_scale(stream_key, shape, cuts, low, top_value):
    def one(axis_at, blocks):
        draws = jax.random.uniform(jax.random.fold_in(jax.random.fold_in(stream_key, 6), axis_at), (blocks,), jnp.float32, low / len(cuts), top_value / len(cuts))
        return jnp.repeat(jnp.exp(draws), shape[axis_at] // blocks).reshape((-1,) + (1,) * (len(shape) - axis_at - 1))

    level = one(*cuts[0])
    for cut in cuts[1:]:
        level = level * one(*cut)
    return level


def noise(rng, shape, spread, bound, split=(), kind=jnp.bfloat16):
    entries = spread * jax.random.normal(rng, shape, jnp.float32)
    if split:
        entries = entries * block_scale(rng, shape, split, -0.22, 0.18)
    return jnp.clip(entries, -bound, bound).astype(kind)


def setup_inputs(seed: int = 0) -> dict:
    streams_of = jax.random.split(jax.random.key(seed), 4)
    return {
        "right_side": noise(streams_of[0], (NX, NY, NZ), 1.0, 6.0, ((0, 2), (1, 4), (2, 16)), jnp.float32),
        "face_coef": jnp.clip(jnp.exp(math.log(3.0) - 2.3025851 * jax.random.uniform(streams_of[1], (3, NX, NY, NZ), jnp.float32) ** block_scale(streams_of[1], (3, NX, NY, NZ), ((1, 2), (2, 4), (3, 16)), -0.2, 0.2)), 0.3, 3.0),
        "absorption": jnp.clip(jnp.exp(math.log(0.01) - 2.30258502 * jax.random.uniform(streams_of[2], (NX, NY, NZ), jnp.float32) ** block_scale(streams_of[2], (NX, NY, NZ), ((0, 2), (1, 4), (2, 16)), -0.2, 0.2)), 0.001, 0.01),
    }


cheb_low = 0.25
cheb_high = 2.0

def apply_stencil(field, stencil, weight, padded):
    low_x = padded[:-2, 1:-1, 1:-1]
    high_x = padded[2:, 1:-1, 1:-1]
    low_y = padded[1:-1, :-2, 1:-1]
    high_y = padded[1:-1, 2:, 1:-1]
    low_z = padded[1:-1, 1:-1, :-2]
    high_z = padded[1:-1, 1:-1, 2:]
    flux = stencil[0] * (field - low_x) + stencil[3] * (field - high_x)
    flux = flux + stencil[1] * (field - low_y) + stencil[4] * (field - high_y)
    flux = flux + stencil[2] * (field - low_z) + stencil[5] * (field - high_z)
    return stencil[6] * field + weight * flux

def inverse_diagonal(stencil, weight):
    total = stencil[0] + stencil[3] + stencil[1] + stencil[4] + stencil[2] + stencil[5]
    return 1.0 / (stencil[6] + weight * total)

def chebyshev(iterate, source, stencil, weight, sweeps, from_zero, pad_field):
    centre = 0.5 * (cheb_high + cheb_low)
    half_width = 0.5 * (cheb_high - cheb_low)
    cheb_ratio = centre / half_width
    cheb_rho = 1.0 / cheb_ratio
    scaling = inverse_diagonal(stencil, weight)
    if from_zero:
        remainder = source
    else:
        remainder = source - apply_stencil(iterate, stencil, weight, pad_field(iterate))
    update = scaling * remainder * (1.0 / centre)
    for sweep in range(sweeps):
        iterate = iterate + update
        if sweep + 1 < sweeps:
            remainder = source - apply_stencil(iterate, stencil, weight, pad_field(iterate))
            next_rho = 1.0 / (2.0 * cheb_ratio - cheb_rho)
            update = next_rho * cheb_rho * update + 2.0 * next_rho / half_width * (scaling * remainder)
            cheb_rho = next_rho
    return iterate

def conjugate(source, stencil, weight, pad_field, total):
    iterate = jnp.zeros_like(source)
    remainder = source
    search = source
    norm_now = total(remainder * remainder)
    for step in range(BOTTOM):
        applied = apply_stencil(search, stencil, weight, pad_field(search))
        step_size = norm_now / total(search * applied)
        iterate = iterate + step_size * search
        if step + 1 < BOTTOM:
            remainder = remainder - step_size * applied
            norm_next = total(remainder * remainder)
            search = remainder + norm_next / norm_now * search
            norm_now = norm_next
    return iterate

def average_cells(field):
    blocks = field.reshape(field.shape[0] // 2, 2, field.shape[1] // 2, 2, field.shape[2] // 2, 2)
    return lax.optimization_barrier(jnp.sum(blocks, axis=(1, 3, 5))) * 0.125

def average_faces(faces):
    halves = (faces.shape[1] // 2, 2, faces.shape[2] // 2, 2, faces.shape[3] // 2, 2)
    along_x = faces[0].reshape(halves)[:, 0]
    along_y = faces[1].reshape(halves)[:, :, :, 0]
    along_z = faces[2].reshape(halves)[..., 0]
    return jnp.stack([lax.optimization_barrier(jnp.sum(along_x, axis=(2, 4))), lax.optimization_barrier(jnp.sum(along_y, axis=(1, 4))), lax.optimization_barrier(jnp.sum(along_z, axis=(1, 3)))]) * 0.25

def repeat_cells(field):
    shape = field.shape
    wide = jnp.broadcast_to(field[:, None, :, None, :, None], (shape[0], 2, shape[1], 2, shape[2], 2))
    return wide.reshape(2 * shape[0], 2 * shape[1], 2 * shape[2])

def pad_zero(field):
    return jnp.pad(field, 1)

def build_stencil(faces, cells):
    high_x = jnp.pad(faces[0, 1:], ((0, 1), (0, 0), (0, 0)))
    high_y = jnp.pad(faces[1, :, 1:], ((0, 0), (0, 1), (0, 0)))
    high_z = jnp.pad(faces[2, :, :, 1:], ((0, 0), (0, 0), (0, 1)))
    return jnp.stack([faces[0], faces[1], faces[2], high_x, high_y, high_z, cells])

def reference(right_side, face_coef, absorption):
    stencils = []
    faces = face_coef
    cells = absorption
    for level in range(LEVELS):
        stencils.append(build_stencil(faces, cells))
        if level + 1 < LEVELS:
            faces = average_faces(faces)
            cells = average_cells(cells)
    sources = []
    iterates = []
    source = right_side
    for level in range(LEVELS - 1):
        weight = 0.25 ** level
        iterate = chebyshev(jnp.zeros_like(source), source, stencils[level], weight, SWEEPS, True, pad_zero)
        remainder = source - apply_stencil(iterate, stencils[level], weight, pad_zero(iterate))
        sources.append(source)
        iterates.append(iterate)
        source = average_cells(remainder)
    correction = conjugate(source, stencils[LEVELS - 1], 0.25 ** (LEVELS - 1), pad_zero, jnp.sum)
    for level in reversed(range(LEVELS - 1)):
        weight = 0.25 ** level
        iterate = iterates[level] + repeat_cells(correction)
        correction = chebyshev(iterate, sources[level], stencils[level], weight, SWEEPS, False, pad_zero)
    residual = right_side - apply_stencil(correction, stencils[0], 1.0, pad_zero(correction))
    relative_norm = jnp.sqrt(jnp.sum(residual * residual) / jnp.sum(right_side * right_side))
    return (correction, residual, relative_norm)
```

```python
import functools

import jax
import jax.numpy as jnp
from jax import lax
from jax.experimental import pallas as pl
from jax.experimental.pallas import tpu as pltpu
from jax.sharding import PartitionSpec as P

BOTTOM = 6
THETA = 1.125
DELTA = 0.875
SIGMA = THETA / DELTA
RHO0 = 1.0 / SIGMA
RHO1 = 1.0 / (2.0 * SIGMA - RHO0)
RHO2 = 1.0 / (2.0 * SIGMA - RHO1)
STEP1 = (RHO1 * RHO0, 2.0 * RHO1 / DELTA)
STEP2 = (RHO2 * RHO1, 2.0 * RHO2 / DELTA)

F32 = jnp.float32
MESH = pl.DeviceIdType.MESH


class Level:
    def __init__(self, n, e, ways, rows, zo, width, pack_rows):
        self.n, self.e, self.ways, self.rows, self.zo, self.width, self.ep = n, e, ways, rows, zo, width, pack_rows
        self.half = n // ways
        self.planes = self.half + 2 * e
        self.span = 128 // ways
        self.slots = self.span // width
        self.packs = -(-self.planes // self.slots)


L0 = Level(48, 4, 2, 56, 8, 4, 4)
L1 = Level(24, 8, 2, 40, 16, 8, 8)
L2 = Level(12, 9, 1, 32, 16, 16, 16)


def lanes(rows):
    return lax.broadcasted_iota(jnp.int32, (rows, 128), 1)


def gather_lanes(value, index):
    return jnp.take_along_axis(value, index, axis=1)


def roll_lanes(value, shift):
    return pltpu.roll(value, shift % 128, 1)


def roll_rows(value, shift):
    return pltpu.roll(value, shift % value.shape[0], 0)


def tile_rows(start, size):
    return pl.ds(pl.multiple_of(start, 8), size)


class Exchange:
    def __init__(self, level, first, count):
        self.level, self.first, self.count = level, first, count

    def scratch(self):
        lv, na = self.level, self.count
        shapes = [
            (na, lv.e * lv.rows, 128),
            (2, na, lv.planes * lv.ep, 128),
            (2, na, lv.planes * lv.ep, 128),
            (2, na, lv.packs * lv.rows, 128),
            (2, na, lv.packs * lv.rows, 128),
            (2, 2, na, lv.packs * lv.ep, 128),
            (2, 2, na, lv.packs * lv.ep, 128),
        ]
        return [pltpu.VMEM(s, F32) for s in shapes] + [pltpu.SemaphoreType.DMA((9,)), pltpu.SemaphoreType.DMA((9,))]

    def bind(self, here, ref, scratch):
        self.here, self.ref = here, ref
        self.xr, self.yb, self.yr, self.zb, self.zr, self.db, self.dr, self.ssem, self.rsem = scratch
        gx, gy, gz, ny, nz = here
        lv = self.level
        e, r = lv.e, lv.rows
        start = e + (1 - gx) * (lv.half - e) if lv.ways == 2 else e + (1 - gx) * (lv.n - e)
        src = ref.at[pl.ds(self.first, self.count), tile_rows(start * r, e * r), :]
        self.copies = []

        def add(src, dst, gx, gy, gz):
            i = len(self.copies)
            self.copies.append(
                pltpu.make_async_remote_copy(
                    src_ref=src,
                    dst_ref=dst,
                    send_sem=self.ssem.at[i],
                    recv_sem=self.rsem.at[i],
                    device_id=(gx, gy, gz),
                    device_id_type=MESH,
                )
            )

        add(src, self.xr, 1 - gx, gy, gz)
        ys = [lax.rem(gy + ny - 1, ny), lax.rem(gy + 1, ny)]
        zs = [lax.rem(gz + nz - 1, nz), lax.rem(gz + 1, nz)]
        for s in range(2):
            add(self.yb.at[s], self.yr.at[1 - s], gx, ys[s], gz)
        for s in range(2):
            for t in range(2):
                add(self.db.at[s, t], self.dr.at[1 - s, 1 - t], gx, ys[s], zs[t])
        for t in range(2):
            add(self.zb.at[t], self.zr.at[1 - t], gx, gy, zs[t])
        self.has_y = [jnp.where(gy > 0, 1.0, 0.0).astype(F32), jnp.where(gy < ny - 1, 1.0, 0.0).astype(F32)]
        self.has_z = [jnp.where(gz > 0, 1.0, 0.0).astype(F32), jnp.where(gz < nz - 1, 1.0, 0.0).astype(F32)]
        self.has_x = [gx.astype(F32), (1 - gx).astype(F32)]
        return self

    def start_x(self):
        self.copies[0].start()

    def finish_x(self):
        lv, ref = self.level, self.ref
        e, r = lv.e, lv.rows
        self.copies[0].wait()
        low = lanes(r) < 64

        def body(i, carry):
            a, j = i // e, i % e
            got = self.xr[a, tile_rows(j * r, r), :]
            if lv.ways == 2:
                got = roll_lanes(got, 64)
                below = roll_lanes(ref[self.first + a, tile_rows((lv.half + j) * r, r), :], 64)
                above = roll_lanes(ref[self.first + a, tile_rows((e + j) * r, r), :], 64)
                below = jnp.where(low, got * self.has_x[0], below)
                above = jnp.where(low, above, got * self.has_x[1])
            else:
                below = got * self.has_x[0]
                above = got * self.has_x[1]
            ref[self.first + a, tile_rows(j * r, r), :] = below
            ref[self.first + a, tile_rows((e + lv.half + j) * r, r), :] = above
            return carry

        lax.fori_loop(0, self.count * e, body, 0)

    def pack(self, ref, rows, out, lead):
        lv = self.level
        slot = (lanes(rows) % lv.span) // lv.width
        shifts = (lv.zo, lv.zo + lv.n - lv.e)
        for k in range(lv.packs):
            acc = [jnp.zeros((rows, 128), F32)] * 2
            for s in range(min(lv.slots, lv.planes - k * lv.slots)):
                plane = ref((k * lv.slots + s) * rows, rows)
                for t in range(2):
                    acc[t] = jnp.where(slot == s, roll_lanes(plane, s * lv.width - shifts[t]), acc[t])
            for t in range(2):
                lead(t, k * rows, acc[t])

    def start_yz(self):
        lv, ref = self.level, self.ref
        r, ep, e = lv.rows, lv.ep, lv.e

        def pack_y(a, carry):
            for p in range(lv.planes):
                self.yb[0, a, pl.ds(p * ep, e), :] = ref[self.first + a, pl.ds(p * r + e, e), :]
                self.yb[1, a, pl.ds(p * ep, e), :] = ref[self.first + a, pl.ds(p * r + lv.n, e), :]
            return carry

        lax.fori_loop(0, self.count, pack_y, 0)
        self.copies[1].start()
        self.copies[2].start()

        def pack_z(a, carry):
            def put(t, row, value):
                self.zb[t, a, pl.ds(row, r), :] = value

            self.pack(lambda row, rows: ref[self.first + a, pl.ds(row, rows), :], r, self.zb, put)
            return carry

        lax.fori_loop(0, self.count, pack_z, 0)
        self.copies[7].start()
        self.copies[8].start()

        def pack_d(i, carry):
            s, a = i // self.count, i % self.count

            def put(t, row, value):
                self.db[s, t, a, pl.ds(row, ep), :] = value

            self.pack(lambda row, rows: self.yb[s, a, pl.ds(row, rows), :], ep, self.db, put)
            return carry

        lax.fori_loop(0, 2 * self.count, pack_d, 0)
        for i in range(3, 7):
            self.copies[i].start()

    def finish_yz(self):
        lv, ref = self.level, self.ref
        r, ep, e = lv.rows, lv.ep, lv.e
        for i in range(1, 9):
            self.copies[i].wait()
        lane = lanes(r) % lv.span
        at_low = (lane >= lv.zo - e) & (lane < lv.zo)
        at_high = (lane >= lv.zo + lv.n) & (lane < lv.zo + lv.n + e)

        def unpack(a, carry):
            for p in range(lv.planes):
                for s in range(2):
                    row = p * r + (e + lv.n) * s
                    ref[self.first + a, pl.ds(row, e), :] = self.yr[s, a, pl.ds(p * ep, e), :] * self.has_y[s]
            for k in range(lv.packs):
                for t in range(2):
                    self.zr[t, a, pl.ds(k * r, r), :] = self.zr[t, a, pl.ds(k * r, r), :] * self.has_z[t]
                    for s in range(2):
                        row = k * r + (e + lv.n) * s
                        both = self.has_y[s] * self.has_z[t]
                        self.zr[t, a, pl.ds(row, e), :] = self.dr[s, t, a, pl.ds(k * ep, e), :] * both
            for k in range(lv.packs):
                got = [self.zr[t, a, pl.ds(k * r, r), :] for t in range(2)]
                for s in range(min(lv.slots, lv.planes - k * lv.slots)):
                    p = k * lv.slots + s
                    value = ref[self.first + a, pl.ds(p * r, r), :]
                    value = jnp.where(at_low, roll_lanes(got[0], lv.zo - e - s * lv.width), value)
                    value = jnp.where(at_high, roll_lanes(got[1], lv.zo + lv.n - s * lv.width), value)
                    ref[self.first + a, pl.ds(p * r, r), :] = value
            return carry

        lax.fori_loop(0, self.count, unpack, 0)


def scaling(lv, fields, inverse, extent):
    r = lv.rows

    def body(p, carry):
        row = pl.multiple_of(p * r, 8)
        cells = fields[3, pl.ds(row, r), :]
        face_z = fields[2, pl.ds(row, r), :]
        total = cells + fields[0, pl.ds(row, r), :] + fields[0, pl.ds(row + r, r), :]
        total = total + fields[1, pl.ds(row, r), :] + fields[1, pl.ds(row + 1, r), :]
        total = total + face_z + roll_lanes(face_z, -1)
        inverse[0, pl.ds(row, r), :] = jnp.where(cells > 0.0, 1.0 / total, 0.0)
        return carry

    lax.fori_loop(lv.e - extent, lv.e + lv.half + extent, body, 0, unroll=2)


def sweep(lv, fields, x, extent, emit):
    r = lv.rows
    lo, hi = lv.e - extent, lv.e + lv.half + extent

    def body(p, carry):
        here, flux = carry
        row = pl.multiple_of(p * r, 8)
        after = x[0, pl.ds(row + r, r), :]
        flux_after = fields[0, pl.ds(row + r, r), :] * (after - here)
        low_y = x[0, pl.ds(row - 1, r), :]
        high_y = x[0, pl.ds(row + 1, r), :]
        flux_y = fields[1, pl.ds(row, r), :] * (here - low_y)
        flux_y = flux_y - fields[1, pl.ds(row + 1, r), :] * (high_y - here)
        flux_z = fields[2, pl.ds(row, r), :] * (here - roll_lanes(here, 1))
        flux_z = flux_z - roll_lanes(flux_z, -1)
        applied = fields[3, pl.ds(row, r), :] * here + ((flux - flux_after) + flux_y + flux_z)
        emit(p, row, here, applied)
        return after, flux_after

    row = lo * r
    here = x[0, pl.ds(row, r), :]
    flux = fields[0, pl.ds(row, r), :] * (here - x[0, pl.ds(row - r, r), :])
    lax.fori_loop(lo, hi, body, (here, flux), unroll=2)


def step(lv, fields, inverse, x, out, d, extent, first, coefs, keep):
    r = lv.rows

    def emit(p, row, here, applied):
        scaled = inverse[0, pl.ds(row, r), :] * (fields[4, pl.ds(row, r), :] - applied)
        if first == 0:
            update = scaled * (1.0 / THETA)
        elif first == 1:
            update = coefs[0] * here + coefs[1] * scaled
        else:
            update = coefs[0] * d[0, pl.ds(row, r), :] + coefs[1] * scaled
        if keep:
            d[0, pl.ds(row, r), :] = update
        out[0, pl.ds(row, r), :] = here + update

    sweep(lv, fields, x, extent, emit)


def smooth_from_zero(lv, fields, inverse, xa, xb, d, extent):
    r = lv.rows

    def body(p, carry):
        row = pl.multiple_of(p * r, 8)
        xa[0, pl.ds(row, r), :] = inverse[0, pl.ds(row, r), :] * fields[4, pl.ds(row, r), :] * (1.0 / THETA)
        return carry

    lax.fori_loop(lv.e - extent, lv.e + lv.half + extent, body, 0, unroll=2)
    step(lv, fields, inverse, xa, xb, d, extent - 1, 1, STEP1, True)
    step(lv, fields, inverse, xb, xa, d, extent - 2, 2, STEP2, False)


def smooth(lv, fields, inverse, xa, xb, d, extent):
    step(lv, fields, inverse, xa, xb, d, extent - 1, 0, None, True)
    step(lv, fields, inverse, xb, xa, d, extent - 2, 2, STEP1, True)
    step(lv, fields, inverse, xa, xb, d, extent - 3, 2, STEP2, False)


def coarse_lanes(lv, below, rows, half):
    lane = lanes(rows)
    if below is None:
        cell, at = lane, 0
    else:
        at = (lane // below.span) * 64 if below.ways == 2 else 0
        cell = lane % below.span - below.zo
    if lv.ways == 2 and half is not None:
        at = 64 * half
    inside = (cell >= 0) & (cell < lv.n // 2)
    index = jnp.where(inside, at + lv.zo + 2 * cell, 0)
    return index, inside


def place(lv, below, put, plane, value, pair):
    rows = value.shape[0]
    if pair:
        value = value + roll_lanes(value, -1)
    halves = [None] if below is not None and below.ways == lv.ways else range(lv.ways)
    for half in halves:
        index, inside = coarse_lanes(lv, below, rows, half)
        got = jnp.where(inside, gather_lanes(value, index), 0.0)
        put(plane if half is None else plane + half * (lv.half // 2), got)


def coarsen_fields(lv, below, fields, put):
    n2, e, r = lv.n // 2, lv.e, lv.rows

    def body(i, carry):
        row = (e + 2 * i) * r + e

        def rows(a, plane, odd):
            return fields[a, pl.ds(row + plane * r + odd, n2, stride=2), :]

        put_x = functools.partial(put, 0)
        put_y = functools.partial(put, 1)
        put_z = functools.partial(put, 2)
        put_c = functools.partial(put, 3)
        place(lv, below, put_x, i, (rows(0, 0, 0) + rows(0, 0, 1)) * 0.0625, True)
        place(lv, below, put_y, i, (rows(1, 0, 0) + rows(1, 1, 0)) * 0.0625, True)
        place(lv, below, put_z, i, (rows(2, 0, 0) + rows(2, 0, 1) + rows(2, 1, 0) + rows(2, 1, 1)) * 0.0625, False)
        place(lv, below, put_c, i, (rows(3, 0, 0) + rows(3, 0, 1) + rows(3, 1, 0) + rows(3, 1, 1)) * 0.125, True)
        return carry

    lax.fori_loop(0, lv.half // 2, body, 0)


def restrict(lv, below, fields, x, sums, put):
    r, n2 = lv.rows, lv.n // 2

    def emit(p, row, here, applied):
        sums[0, pl.ds((p - lv.e) * r, r), :] = fields[4, pl.ds(row, r), :] - applied

    sweep(lv, fields, x, 0, emit)

    def body(i, carry):
        total = None
        for plane in range(2):
            for odd in range(2):
                part = sums[0, pl.ds((2 * i + plane) * r + lv.e + odd, n2, stride=2), :]
                total = part if total is None else total + part
        place(lv, below, functools.partial(put, 4), i, total * 0.125, True)
        return carry

    lax.fori_loop(0, lv.half // 2, body, 0)


def fields_put(below, fields):
    def put(field, plane, value):
        fields[field, pl.ds((below.e + plane) * below.rows + below.e, below.n), :] = value

    return put


def prolong(lv, above, e, x, reach):
    r, rows = lv.rows, lv.n // 2 + 2 * reach
    lane = lanes(rows)
    cell = lane % 64 - lv.zo + 2 * reach
    inside = (cell >= 0) & (cell < 2 * rows)
    source = above.zo - reach + cell // 2
    if above.ways == 2:
        source = source + (lane // 64) * 64
    source = jnp.where(inside, source, 0)

    def body(i, carry):
        row = (above.e - reach + i) * above.rows + above.e - reach
        value = gather_lanes(e[0, pl.ds(row, rows), :], source)
        if above.ways == 1:
            other = gather_lanes(e[0, pl.ds(row + (lv.half // 2) * above.rows, rows), :], source)
            value = jnp.where(lane < 64, value, other)
        value = jnp.where(inside, value, 0.0)
        for plane in range(2):
            at = (lv.e - 2 * reach + 2 * i + plane) * r + lv.e - 2 * reach
            for odd in range(2):
                where = pl.ds(at + odd, rows, stride=2)
                x[0, where, :] = x[0, where, :] + value
        return carry

    lax.fori_loop(0, lv.half // 2 + 2 * reach, body, 0)


def whole_operator(ny, fields, v, scale):
    rows = lax.broadcasted_iota(jnp.int32, (128, 128), 0)
    z, y = rows % 8, lanes(128) % 6
    last = 6 - scale
    y_low, y_high, z_low, z_high = y == 0, y == last, z == 0, z == last
    bottom, top = rows == 0, rows == 120 + last
    zero = jnp.zeros((128, 128), F32)

    def below_y(g):
        other = roll_lanes(v[g - 1], -last) if g else zero
        return jnp.where(y_low, other, roll_lanes(v[g], scale))

    fluxes_y = [fields(1, g) * (v[g] - below_y(g)) for g in range(ny)]
    out = []
    for g in range(ny):
        flux = fields(0, g) * (v[g] - roll_lanes(v[g], 6 * scale))
        total = flux - roll_lanes(flux, -6 * scale)
        other = roll_lanes(fluxes_y[g + 1], last) if g + 1 < ny else zero
        total = total + (fluxes_y[g] - jnp.where(y_high, other, roll_lanes(fluxes_y[g], -scale)))
        jump = 8 - last
        other = jnp.where(bottom, 0.0, roll_rows(v[g], jump))
        flux = fields(2, g) * (v[g] - jnp.where(z_low, other, roll_rows(v[g], scale)))
        other = jnp.where(top, 0.0, roll_rows(flux, -jump))
        total = total + (flux - jnp.where(z_high, other, roll_rows(flux, -scale)))
        out.append(fields(3, g) * v[g] + total)
    return out


def whole_inverse(ny, fields):
    rows = lax.broadcasted_iota(jnp.int32, (128, 128), 0)
    z, y = rows % 8, lanes(128) % 6
    zero = jnp.zeros((128, 128), F32)
    out = []
    for g in range(ny):
        face_x, face_y, face_z, cells = (fields(a, g) for a in range(4))
        total = cells + face_x + roll_lanes(face_x, -6)
        other = roll_lanes(fields(1, g + 1), 5) if g + 1 < ny else zero
        total = total + face_y + jnp.where(y == 5, other, roll_lanes(face_y, -1))
        other = jnp.where(rows == 125, 0.0, roll_rows(face_z, -3))
        total = total + face_z + jnp.where(z == 5, other, roll_rows(face_z, -1))
        out.append(jnp.where(cells > 0.0, 1.0 / total, 0.0))
    return out


def children(value, axes):
    if "y" in axes:
        value = value + roll_lanes(value, -1)
    if "x" in axes:
        value = value + roll_lanes(value, -6)
    if "z" in axes:
        value = value + roll_rows(value, -1)
    return value


def coarse_solve(ny, gathered, source, inverse, bottom, xs, ds):
    nz = 16
    fields = lambda a, g: gathered[g, :, a].reshape(128, 128)
    f = lambda g: source[g].reshape(128, 128)

    def load(ref):
        return [ref[g] for g in range(ny)]

    def residual(v):
        applied = whole_operator(ny, fields, v, 1)
        return [f(g) - applied[g] for g in range(ny)]

    for g in range(ny):
        xs[g] = inverse[g] * f(g) * (1.0 / THETA)
        ds[g] = xs[g]
    for coefs in (STEP1, STEP2):
        remainder = residual(load(xs))
        for g in range(ny):
            update = coefs[0] * ds[g] + coefs[1] * (inverse[g] * remainder[g])
            ds[g] = update
            xs[g] = xs[g] + update
    remainder = residual(load(xs))
    inside = lambda g, value: jnp.where(bottom[3, g] > 0.0, value, 0.0)
    r = [inside(g, children(remainder[g], "xyz") * 0.125) for g in range(ny)]

    def total(values):
        values = functools.reduce(lambda a, b: a + b, values)
        return jnp.sum(jnp.sum(values, axis=0, keepdims=True), axis=1, keepdims=True)

    coarse = lambda a, g: bottom[a, g]
    e = [jnp.zeros((128, 128), F32)] * ny
    norm = total([a * a for a in r])

    def body(i, carry):
        e, r, p, norm = carry
        q = [inside(g, a) for g, a in enumerate(whole_operator(ny, coarse, p, 2))]
        size = norm / total([a * b for a, b in zip(p, q)])
        e = [a + size * b for a, b in zip(e, p)]
        r = [a - size * b for a, b in zip(r, q)]
        after = total([a * a for a in r])
        p = [a + after / norm * b for a, b in zip(r, p)]
        return e, r, p, after

    e, r, p, norm = lax.fori_loop(0, BOTTOM - 1, body, (e, r, r, norm))
    q = [inside(g, a) for g, a in enumerate(whole_operator(ny, coarse, p, 2))]
    size = norm / total([a * b for a, b in zip(p, q)])
    for g in range(ny):
        value = e[g] + size * p[g]
        value = value + roll_lanes(value, 1)
        value = value + roll_lanes(value, 6)
        xs[g] = xs[g] + (value + roll_rows(value, 1))
    for number, coefs in enumerate((None, STEP1, STEP2)):
        remainder = residual(load(xs))
        for g in range(ny):
            update = inverse[g] * remainder[g]
            if number == 0:
                update = update * (1.0 / THETA)
            else:
                update = coefs[0] * ds[g] + coefs[1] * update
            ds[g] = update
            xs[g] = xs[g] + update


def coarse_fields(ny, gathered, bottom):
    fields = lambda a, g: gathered[g, :, a].reshape(128, 128)
    rows = lax.broadcasted_iota(jnp.int32, (128, 128), 0)
    lane = lanes(128)
    even = (rows % 2 == 0) & (lane % 2 == 0) & ((lane // 6) % 2 == 0) & (lane < 72)
    for g in range(ny):
        for a, axes in enumerate(("yz", "xz", "xy", "xyz")):
            factor = 0.125 if a == 3 else 0.0625
            bottom[a, g] = jnp.where(even, children(fields(a, g), axes) * factor, 0.0)


def window(lv, gx, gy, gz, ny, xs, padded, turned, corner, x):
    nz = 16
    padded[...] = jnp.zeros_like(padded)
    for g in range(ny):
        padded[g + 1, pl.ds(1, nz)] = xs[g].reshape(nz, 8, 128)
    for dy in range(3):
        tiles = padded[gy + dy, pl.ds(gz, 3)].reshape(24, 128)
        tiles = jnp.concatenate([tiles, jnp.zeros((104, 128), F32)], axis=0)
        turned[dy, pl.ds(0, 24), :] = jnp.zeros((24, 128), F32)
        turned[dy, pl.ds(24, 128), :] = tiles.T
    lane = lanes(16)
    cell = lane - lv.zo + 6
    inside = (cell >= 0) & (cell < 24)
    coarse = jnp.where(inside, cell // 2 + 3, 0)
    source = (coarse // 6) * 8 + coarse % 6

    def body(i, carry):
        base = 6 + 36 * gx + 6 * i
        corner[pl.ds(0, 3), :] = turned[0, pl.ds(base + 3, 3), :]
        corner[pl.ds(3, 6), :] = turned[1, pl.ds(base, 6), :]
        corner[pl.ds(9, 3), :] = turned[2, pl.ds(base, 3), :]
        value = jnp.where(inside, gather_lanes(corner[...], source), 0.0)[0:12]
        for plane in range(2):
            at = (lv.e - 6 + 2 * i + plane) * lv.rows + lv.e - 6
            for odd in range(2):
                where = pl.ds(at + odd, 12, stride=2)
                x[0, where, :] = x[0, where, :] + value
        return carry

    lax.fori_loop(0, 12, body, 0)


def cycle(ny, nz, names, *refs):
    refs = list(refs)
    right_hbm, faces_hbm, cells_hbm, solution_hbm, residual_hbm, norm_out = refs[:6]
    s = dict(zip(names, refs[6:]))
    gx, gy, gz = lax.axis_index("gx"), lax.axis_index("gy"), lax.axis_index("gz")
    here = (gx, gy, gz, ny, nz)

    loads = [pltpu.make_async_copy(faces_hbm.at[d], s["land"].at[d], s["load_sem"].at[d]) for d in range(3)]
    loads.append(pltpu.make_async_copy(cells_hbm, s["land"].at[3], s["load_sem"].at[3]))
    loads.append(pltpu.make_async_copy(right_hbm, s["land"].at[4], s["load_sem"].at[4]))
    for copy in loads:
        copy.start()

    def other(t):
        return lax.rem(gy + t // nz, ny), lax.rem(gz + t % nz, nz)

    barrier = pltpu.get_barrier_semaphore()

    def greet(t, carry):
        oy, oz = other(t)
        pl.semaphore_signal(barrier, inc=1, device_id=(gx, oy, oz), device_id_type=MESH)
        return carry

    pl.semaphore_signal(barrier, inc=1, device_id=(1 - gx, gy, gz), device_id_type=MESH)
    lax.fori_loop(1, ny * nz, greet, 0)

    f0, f1, f2 = s["f0"], s["f1"], s["f2"]
    ex = {k: Exchange(*v) for k, v in EXCHANGES.items()}
    for k, target in (("e0", f0), ("c1", f1), ("c2", f2), ("e1", f1), ("e2", f2), ("x0", s["x0a"])):
        ex[k].bind(here, target, [s[k + str(i)] for i in range(9)])

    low = lanes(48) < 64
    for a in range(5):
        loads[a].wait()

        def load(i, carry, a=a):
            first = jnp.pad(s["land"][a, i], ((0, 0), (0, 80)))
            second = jnp.pad(s["land"][a, i + 24], ((0, 0), (0, 80)))
            value = roll_lanes(first, L0.zo) + roll_lanes(second, 64 + L0.zo)
            f0[a, pl.ds((L0.e + i) * L0.rows + L0.e, 48), :] = value
            return carry

        lax.fori_loop(0, 24, load, 0, unroll=2)

    f1[...] = jnp.zeros_like(f1)
    f2[...] = jnp.zeros_like(f2)
    s["square"][...] = jnp.zeros_like(s["square"])

    def square(i, carry):
        value = f0[4, pl.ds((L0.e + i) * L0.rows + L0.e, 48), :]
        return carry + value * value

    squares = lax.fori_loop(0, 24, square, jnp.zeros((48, 128), F32), unroll=2)
    coarsen_fields(L0, L1, f0, fields_put(L1, f1))
    coarsen_fields(L1, L2, f1, fields_put(L2, f2))

    block = s["block"]
    block[...] = jnp.zeros_like(block)

    def block_put(field, plane, value):
        block[field, pl.ds(plane * 6, 6), :] = value

    coarsen_fields(L2, None, f2, block_put)

    def tile_of(field):
        return roll_lanes(block[field].T[0:8], gx * 36)

    own4, pair4, own1, pair1, own_n, pair_n = (s[k] for k in ("own4", "pair4", "own1", "pair1", "own_n", "pair_n"))
    for field in range(4):
        own4[field] = tile_of(field)

    pl.semaphore_wait(barrier, ny * nz)

    def partner(src, dst, i):
        return pltpu.make_async_remote_copy(
            src_ref=src,
            dst_ref=dst,
            send_sem=s["pair_send"].at[i],
            recv_sem=s["pair_recv"].at[i],
            device_id=(1 - gx, gy, gz),
            device_id_type=MESH,
        )

    def spread(src, dst, i):
        def copy(t, to):
            oy, oz = other(t if to else ny * nz - t)
            sy, sz = (gy, gz) if to else (oy, oz)
            return oy, oz, sy, sz

        def start(t, carry):
            oy, oz = other(t)
            pltpu.make_async_remote_copy(
                src_ref=src,
                dst_ref=dst.at[gy, gz],
                send_sem=s["all_send"].at[i, t],
                recv_sem=s["all_recv"].at[i, t],
                device_id=(gx, oy, oz),
                device_id_type=MESH,
            ).start()
            return carry

        def finish(t, carry):
            oy = lax.rem(gy + ny - t // nz, ny)
            oz = lax.rem(gz + nz - t % nz, nz)
            pltpu.make_async_remote_copy(
                src_ref=src,
                dst_ref=dst.at[oy, oz],
                send_sem=s["all_send"].at[i, t],
                recv_sem=s["all_recv"].at[i, t],
                device_id=(gx, oy, oz),
                device_id_type=MESH,
            ).wait()
            return carry

        return (
            lambda: lax.fori_loop(1, ny * nz, start, 0),
            lambda: lax.fori_loop(1, ny * nz, finish, 0),
        )

    ex["e0"].start_x()
    pair_coef = partner(own4, pair4, 0)
    pair_coef.start()
    ex["e0"].finish_x()
    ex["e0"].start_yz()
    ex["c1"].start_x()
    ex["c2"].start_x()
    ex["c1"].finish_x()
    ex["c2"].finish_x()
    pair_coef.wait()
    merged = s["merged4"]
    merged[...] = own4[...] + pair4[...]
    g4, g1, gn = s["g4"], s["g1"], s["gn"]
    g4[gy, gz] = merged[...]
    coef_start, coef_finish = spread(merged, g4, 0)

    ex["e0"].finish_yz()
    ex["c1"].start_yz()
    ex["c2"].start_yz()
    coef_start()
    scaling(L0, f0, s["i0"], 3)
    smooth_from_zero(L0, f0, s["i0"], s["x0a"], s["x0b"], s["d0"], 3)
    restrict(L0, L1, f0, s["x0a"], s["sums"], fields_put(L1, f1))
    ex["e1"].start_x()
    ex["x0"].start_x()
    ex["c1"].finish_yz()
    ex["c2"].finish_yz()
    ex["e1"].finish_x()
    ex["e1"].start_yz()
    ex["x0"].finish_x()
    scaling(L1, f1, s["i1"], 7)
    scaling(L2, f2, s["i2"], 8)
    ex["e1"].finish_yz()
    ex["x0"].start_yz()
    smooth_from_zero(L1, f1, s["i1"], s["x1a"], s["x1b"], s["d1"], 7)
    restrict(L1, L2, f1, s["x1a"], s["sums"], fields_put(L2, f2))
    ex["e2"].start_x()
    ex["e2"].finish_x()
    ex["e2"].start_yz()
    coef_finish()
    gathered = lambda a, g: g4[g, :, a].reshape(128, 128)
    inverse = whole_inverse(ny, gathered)
    for g in range(ny):
        s["i3"][g] = inverse[g]
    coarse_fields(ny, g4, s["bottom"])
    ex["x0"].finish_yz()
    ex["e2"].finish_yz()
    smooth_from_zero(L2, f2, s["i2"], s["x2a"], s["x2b"], s["d2"], 8)
    restrict(L2, None, f2, s["x2a"], s["sums"], block_put)
    own1[...] = tile_of(4)
    pair_source = partner(own1, pair1, 1)
    pair_source.start()
    pair_source.wait()
    s["merged1"][...] = own1[...] + pair1[...]
    g1[gy, gz] = s["merged1"][...]
    source_start, source_finish = spread(s["merged1"], g1, 1)
    source_start()
    source_finish()
    coarse_solve(ny, g4, g1, s["i3"], s["bottom"], s["x3"], s["d3"])
    window(L2, gx, gy, gz, ny, s["x3"], s["padded"], s["turned"], s["corner"], s["x2a"])
    smooth(L2, f2, s["i2"], s["x2a"], s["x2b"], s["d2"], 6)
    prolong(L1, L2, s["x2b"], s["x1a"], 3)
    smooth(L1, f1, s["i1"], s["x1a"], s["x1b"], s["d1"], 5)
    prolong(L0, L1, s["x1b"], s["x0a"], 2)
    smooth(L0, f0, s["i0"], s["x0a"], s["x0b"], s["d0"], 4)

    land = s["land"]
    r0 = L0.rows

    def unload(slot, i, value):
        for half in range(2):
            moved = roll_lanes(value, -(L0.zo + 64 * half))
            land[slot, i + 24 * half] = moved[:, 0:48]

    def out_solution(i, carry):
        unload(0, i, s["x0b"][0, pl.ds((L0.e + i) * r0 + L0.e, 48), :])
        return carry

    lax.fori_loop(0, 24, out_solution, 0, unroll=2)
    out0 = pltpu.make_async_copy(land.at[0], solution_hbm, s["out_sem"].at[0])
    out0.start()

    def final(p, row, here_x, applied):
        s["sums"][0, pl.ds((p - L0.e) * r0, r0), :] = f0[4, pl.ds(row, r0), :] - applied

    sweep(L0, f0, s["x0b"], 0, final)
    lane48 = lanes(48) % 64
    inside = (lane48 >= L0.zo) & (lane48 < L0.zo + 48)

    def out_residual(i, carry):
        value = s["sums"][0, pl.ds(i * r0 + L0.e, 48), :]
        unload(1, i, value)
        value = jnp.where(inside, value, 0.0)
        return carry + value * value

    ends = lax.fori_loop(0, 24, out_residual, jnp.zeros((48, 128), F32), unroll=2)
    out1 = pltpu.make_async_copy(land.at[1], residual_hbm, s["out_sem"].at[1])
    out1.start()

    def fold(value):
        return jnp.sum(value, axis=0, keepdims=True)

    own_n[...] = jnp.concatenate([fold(squares), fold(ends), jnp.zeros((6, 128), F32)], axis=0)
    pair_norm = partner(own_n, pair_n, 2)
    pair_norm.start()
    pair_norm.wait()
    s["merged_n"][...] = jnp.where(gx == 0, own_n[...] + pair_n[...], pair_n[...] + own_n[...])
    gn[gy, gz] = s["merged_n"][...]
    norm_start, norm_finish = spread(s["merged_n"], gn, 2)
    norm_start()
    norm_finish()
    all_n = jnp.sum(gn[...].reshape(ny * nz, 8, 128), axis=0)
    sums = jnp.sum(all_n, axis=1, keepdims=True)
    norm = jnp.sqrt(sums[1:2] / sums[0:1])
    norm_out[0, 0] = norm[0, 0]
    out0.wait()
    out1.wait()


EXCHANGES = {
    "e0": (L0, 0, 5),
    "c1": (L1, 0, 4),
    "c2": (L2, 0, 4),
    "e1": (L1, 4, 1),
    "e2": (L2, 4, 1),
    "x0": (L0, 0, 1),
}


def scratch_of(ny, nz):
    vmem = lambda *shape: pltpu.VMEM(shape, F32)
    size = lambda lv: lv.planes * lv.rows
    scratch = {"land": vmem(5, 48, 48, 48), "load_sem": pltpu.SemaphoreType.DMA((5,)), "out_sem": pltpu.SemaphoreType.DMA((2,))}
    for i, lv in enumerate((L0, L1, L2)):
        scratch[f"f{i}"] = vmem(5, size(lv), 128)
        for k in ("i", "d"):
            scratch[f"{k}{i}"] = vmem(1, size(lv), 128)
        scratch[f"x{i}a"] = vmem(1, size(lv), 128)
        scratch[f"x{i}b"] = vmem(1, size(lv), 128)
    scratch["sums"] = vmem(1, 24 * 56, 128)
    scratch["square"] = vmem(8, 128)
    scratch["block"] = vmem(5, 128, 128)
    for k in ("own4", "pair4", "merged4"):
        scratch[k] = vmem(4, 8, 128)
    for k in ("own1", "pair1", "merged1", "own_n", "pair_n", "merged_n"):
        scratch[k] = vmem(8, 128)
    scratch["g4"] = vmem(ny, nz, 4, 8, 128)
    scratch["g1"] = vmem(ny, nz, 8, 128)
    scratch["gn"] = vmem(ny, nz, 8, 128)
    for k in ("pair_send", "pair_recv"):
        scratch[k] = pltpu.SemaphoreType.DMA((3,))
    for k in ("all_send", "all_recv"):
        scratch[k] = pltpu.SemaphoreType.DMA((3, ny * nz))
    for k in ("i3", "x3", "d3"):
        scratch[k] = vmem(ny, 128, 128)
    scratch["bottom"] = vmem(4, ny, 128, 128)
    scratch["padded"] = vmem(ny + 2, nz + 2, 8, 128)
    scratch["turned"] = vmem(3, 152, 128)
    scratch["corner"] = vmem(16, 128)
    for k, v in EXCHANGES.items():
        for i, shape in enumerate(Exchange(*v).scratch()):
            scratch[k + str(i)] = shape
    return scratch


def solution(mesh):
    ny, nz = mesh.shape["gy"], mesh.shape["gz"]
    scratch = scratch_of(ny, nz)

    def shards(right_side, face_coef, absorption):
        field = jax.ShapeDtypeStruct((48, 48, 48), F32)
        solved, residual, norm = pl.pallas_call(
            functools.partial(cycle, ny, nz, tuple(scratch)),
            out_shape=(field, field, jax.ShapeDtypeStruct((1, 1), F32)),
            in_specs=[pl.BlockSpec(memory_space=pl.ANY)] * 3,
            out_specs=(
                pl.BlockSpec(memory_space=pl.ANY),
                pl.BlockSpec(memory_space=pl.ANY),
                pl.BlockSpec(memory_space=pltpu.SMEM),
            ),
            scratch_shapes=list(scratch.values()),
            compiler_params=pltpu.CompilerParams(
                collective_id=0, has_side_effects=True, vmem_limit_bytes=62 * 1024 * 1024
            ),
        )(right_side, face_coef, absorption)
        return solved, residual, norm[0, 0]

    in_specs = (P("gx", "gy", "gz"), P(None, "gx", "gy", "gz"), P("gx", "gy", "gz"))
    out_specs = (P("gx", "gy", "gz"), P("gx", "gy", "gz"), P())
    return jax.shard_map(shards, mesh=mesh, in_specs=in_specs, out_specs=out_specs, check_vma=False)
```

```python
import functools

import jax
import jax.numpy as jnp
from jax import lax
from jax.experimental import pallas as pl
from jax.experimental.pallas import tpu as pltpu
from jax.sharding import PartitionSpec as P

BOTTOM = 6
THETA = 1.125
DELTA = 0.875
SIGMA = THETA / DELTA
RHO0 = 1.0 / SIGMA
RHO1 = 1.0 / (2.0 * SIGMA - RHO0)
RHO2 = 1.0 / (2.0 * SIGMA - RHO1)
STEP1 = (RHO1 * RHO0, 2.0 * RHO1 / DELTA)
STEP2 = (RHO2 * RHO1, 2.0 * RHO2 / DELTA)

F32 = jnp.float32
MESH = pl.DeviceIdType.MESH


class Level:
    def __init__(self, n, e, ways, rows, zo, width, width_y, unroll):
        self.n, self.e, self.ways, self.rows, self.zo, self.width = n, e, ways, rows, zo, width
        self.width_y, self.unroll = width_y, unroll
        self.half = n // ways
        self.planes = self.half + 2 * e
        self.span = 128 // ways
        self.slots, self.slots_y = self.span // width, self.span // width_y
        self.packs, self.packs_y = -(-self.planes // self.slots), -(-self.planes // self.slots_y)


L0 = Level(48, 4, 2, 56, 8, 4, 64, 4)
L1 = Level(24, 6, 2, 40, 16, 8, 32, 4)
L2 = Level(12, 6, 1, 24, 16, 8, 16, 6)


def lanes(rows):
    return lax.broadcasted_iota(jnp.int32, (rows, 128), 1)


def gather_lanes(value, index):
    return jnp.take_along_axis(value, index, axis=1)


def roll_lanes(value, shift):
    return pltpu.roll(value, shift % 128, 1)


def roll_rows(value, shift):
    return pltpu.roll(value, shift % value.shape[0], 0)


def tile_rows(start, size):
    return pl.ds(pl.multiple_of(start, 8), size)


def loop(lo, hi, body, carry, unroll):
    count = (hi - lo) // unroll

    def chunk(i, carry):
        for k in range(unroll):
            carry = body(lo + i * unroll + k, carry)
        return carry

    carry = lax.fori_loop(0, count, chunk, carry)
    for k in range(lo + count * unroll, hi):
        carry = body(k, carry)
    return carry


class Exchange:
    def __init__(self, level, first, count):
        self.level, self.first, self.count = level, first, count

    def scratch(self):
        lv, na = self.level, self.count
        shapes = [
            (na, lv.e * lv.rows, 128),
            (2, na, lv.packs_y * lv.e, 128),
            (2, na, lv.packs_y * lv.e, 128),
            (2, na, lv.packs * lv.n, 128),
            (2, na, lv.packs * lv.n, 128),
            (2, 2, na, lv.packs * lv.e, 128),
            (2, 2, na, lv.packs * lv.e, 128),
            (2, na, lv.packs * lv.rows, 128),
        ]
        return [pltpu.VMEM(s, F32) for s in shapes] + [pltpu.SemaphoreType.DMA((9,)), pltpu.SemaphoreType.DMA((9,))]

    def bind(self, here, ref, scratch):
        self.here, self.ref = here, ref
        self.xr, self.yb, self.yr, self.zb, self.zr, self.db, self.dr, self.zf, self.ssem, self.rsem = scratch
        gx, gy, gz, ny, nz = here
        lv = self.level
        e, r = lv.e, lv.rows
        start = e + (1 - gx) * (lv.half - e) if lv.ways == 2 else e + (1 - gx) * (lv.n - e)
        src = ref.at[pl.ds(self.first, self.count), tile_rows(start * r, e * r), :]
        self.copies = []

        def add(src, dst, gx, gy, gz):
            i = len(self.copies)
            self.copies.append(
                pltpu.make_async_remote_copy(
                    src_ref=src,
                    dst_ref=dst,
                    send_sem=self.ssem.at[i],
                    recv_sem=self.rsem.at[i],
                    device_id=(gx, gy, gz),
                    device_id_type=MESH,
                )
            )

        add(src, self.xr, 1 - gx, gy, gz)
        ys = [lax.rem(gy + ny - 1, ny), lax.rem(gy + 1, ny)]
        zs = [lax.rem(gz + nz - 1, nz), lax.rem(gz + 1, nz)]
        for s in range(2):
            add(self.yb.at[s], self.yr.at[1 - s], gx, ys[s], gz)
        for s in range(2):
            for t in range(2):
                add(self.db.at[s, t], self.dr.at[1 - s, 1 - t], gx, ys[s], zs[t])
        for t in range(2):
            add(self.zb.at[t], self.zr.at[1 - t], gx, gy, zs[t])
        self.has_y = [jnp.where(gy > 0, 1.0, 0.0).astype(F32), jnp.where(gy < ny - 1, 1.0, 0.0).astype(F32)]
        self.has_z = [jnp.where(gz > 0, 1.0, 0.0).astype(F32), jnp.where(gz < nz - 1, 1.0, 0.0).astype(F32)]
        self.has_x = [gx.astype(F32), (1 - gx).astype(F32)]
        return self

    def start_x(self):
        self.copies[0].start()

    def finish_x(self):
        lv, ref = self.level, self.ref
        e, r = lv.e, lv.rows
        self.copies[0].wait()
        low = lanes(r) < 64

        def finish(a, j):
            got = self.xr[a, tile_rows(j * r, r), :]
            if lv.ways == 2:
                got = roll_lanes(got, 64)
                below = roll_lanes(ref[self.first + a, tile_rows((lv.half + j) * r, r), :], 64)
                above = roll_lanes(ref[self.first + a, tile_rows((e + j) * r, r), :], 64)
                below = jnp.where(low, got * self.has_x[0], below)
                above = jnp.where(low, above, got * self.has_x[1])
            else:
                below = got * self.has_x[0]
                above = got * self.has_x[1]
            ref[self.first + a, tile_rows(j * r, r), :] = below
            ref[self.first + a, tile_rows((e + lv.half + j) * r, r), :] = above

        def body(a, carry):
            for j in range(e):
                finish(a, j)
            return carry

        lax.fori_loop(0, self.count, body, 0)

    def pack(self, plane, rows, width, shifts, put):
        lv = self.level
        slot = (lanes(rows) % lv.span) // width
        slots = lv.span // width
        for k in range(-(-lv.planes // slots)):
            acc = None
            for s in range(min(slots, lv.planes - k * slots)):
                moved = [roll_lanes(value, s * width - shift) for value, shift in zip(plane(k * slots + s), shifts)]
                acc = moved if s == 0 else [jnp.where(slot == s, new, old) for new, old in zip(moved, acc)]
            put(k, acc)

    def start_yz(self):
        lv, ref = self.level, self.ref
        r, n, e, zo = lv.rows, lv.n, lv.e, lv.zo
        z_shifts = (zo, zo + n - e)

        def pack_y(a, carry):
            def plane(p):
                return [ref[self.first + a, pl.ds(p * r + row, e), :] for row in (e, n)]

            def put(k, values):
                for s in range(2):
                    self.yb[s, a, pl.ds(k * e, e), :] = values[s]

            if lv.slots_y == 1:
                for p in range(lv.planes):
                    put(p, plane(p))
            else:
                self.pack(plane, e, lv.width_y, (zo, zo), put)
            return carry

        lax.fori_loop(0, self.count, pack_y, 0)
        self.copies[1].start()
        self.copies[2].start()

        def pack_z(a, carry):
            def plane(p):
                return [ref[self.first + a, pl.ds(p * r + e, n), :]] * 2

            def put(k, values):
                for t in range(2):
                    self.zb[t, a, pl.ds(k * n, n), :] = values[t]

            self.pack(plane, n, lv.width, z_shifts, put)
            return carry

        lax.fori_loop(0, self.count, pack_z, 0)
        self.copies[7].start()
        self.copies[8].start()

        def pack_d(a, carry):
            def plane(p):
                low, high = (ref[self.first + a, pl.ds(p * r + row, e), :] for row in (e, n))
                return low, low, high, high

            def put(k, values):
                for i in range(4):
                    self.db[i // 2, i % 2, a, pl.ds(k * e, e), :] = values[i]

            self.pack(plane, e, lv.width, z_shifts * 2, put)
            return carry

        lax.fori_loop(0, self.count, pack_d, 0)
        for i in range(3, 7):
            self.copies[i].start()

    def finish_yz(self):
        lv, ref = self.level, self.ref
        r, n, e, zo = lv.rows, lv.n, lv.e, lv.zo
        for i in range(1, 9):
            with jax.named_scope("copy" + str(i)):
                self.copies[i].wait()
        lane = lanes(r) % lv.span
        at_low = (lane >= zo - e) & (lane < zo)
        at_high = (lane >= zo + n) & (lane < zo + n + e)

        def unpack(a, carry):
            for s in range(2):
                for k in range(lv.packs_y):
                    got = self.yr[s, a, pl.ds(k * e, e), :] * self.has_y[s]
                    for slot in range(min(lv.slots_y, lv.planes - k * lv.slots_y)):
                        row = (k * lv.slots_y + slot) * r + (e + n) * s
                        moved = roll_lanes(got, zo - slot * lv.width_y) if lv.slots_y > 1 else got
                        ref[self.first + a, pl.ds(row, e), :] = moved
            for k in range(lv.packs):
                for t in range(2):
                    self.zf[t, a, pl.ds(k * r + e, n), :] = self.zr[t, a, pl.ds(k * n, n), :] * self.has_z[t]
                    for s in range(2):
                        both = self.has_y[s] * self.has_z[t]
                        self.zf[t, a, pl.ds(k * r + (e + n) * s, e), :] = self.dr[s, t, a, pl.ds(k * e, e), :] * both
            for k in range(lv.packs):
                got = [self.zf[t, a, pl.ds(k * r, r), :] for t in range(2)]
                for s in range(min(lv.slots, lv.planes - k * lv.slots)):
                    p = k * lv.slots + s
                    value = ref[self.first + a, pl.ds(p * r, r), :]
                    value = jnp.where(at_low, roll_lanes(got[0], zo - e - s * lv.width), value)
                    value = jnp.where(at_high, roll_lanes(got[1], zo + n - s * lv.width), value)
                    ref[self.first + a, pl.ds(p * r, r), :] = value
            return carry

        lax.fori_loop(0, self.count, unpack, 0)


def scaling(lv, fields, inverse, upper, extent):
    r = lv.rows

    def body(p, carry):
        row = pl.multiple_of(p * r, 8)
        cells = fields[3, pl.ds(row, r), :]
        face_z = fields[2, pl.ds(row, r), :]
        total = cells + fields[0, pl.ds(row, r), :] + fields[0, pl.ds(row + r, r), :]
        total = total + fields[1, pl.ds(row, r), :] + fields[1, pl.ds(row + 1, r), :]
        above = roll_lanes(face_z, -1)
        upper[0, pl.ds(row, r), :] = above
        total = total + face_z + above
        inverse[0, pl.ds(row, r), :] = jnp.where(cells > 0.0, 1.0 / total, 0.0)
        return carry

    loop(lv.e - extent, lv.e + lv.half + extent, body, 0, lv.unroll)


def sweep(lv, fields, upper, x, extent, emit, carry=0):
    r = lv.rows
    lo, hi = lv.e - extent, lv.e + lv.half + extent

    def body(p, carry):
        here, flux, kept = carry
        row = pl.multiple_of(p * r, 8)
        after = x[0, pl.ds(row + r, r), :]
        flux_after = fields[0, pl.ds(row + r, r), :] * (after - here)
        low_y = x[0, pl.ds(row - 1, r), :]
        high_y = x[0, pl.ds(row + 1, r), :]
        flux_y = fields[1, pl.ds(row, r), :] * (here - low_y)
        flux_y = flux_y - fields[1, pl.ds(row + 1, r), :] * (high_y - here)
        flux_z = fields[2, pl.ds(row, r), :] * (here - roll_lanes(here, 1))
        flux_z = flux_z - upper[0, pl.ds(row, r), :] * (roll_lanes(here, -1) - here)
        applied = fields[3, pl.ds(row, r), :] * here + ((flux - flux_after) + flux_y + flux_z)
        return after, flux_after, emit(p, row, here, applied, kept)

    row = lo * r
    here = x[0, pl.ds(row, r), :]
    flux = fields[0, pl.ds(row, r), :] * (here - x[0, pl.ds(row - r, r), :])
    return loop(lo, hi, body, (here, flux, carry), lv.unroll)[2]


def step(lv, fields, inverse, upper, x, out, d, extent, first, coefs, keep):
    r = lv.rows

    def emit(p, row, here, applied, kept):
        scaled = inverse[0, pl.ds(row, r), :] * (fields[4, pl.ds(row, r), :] - applied)
        if first == 0:
            update = scaled * (1.0 / THETA)
        elif first == 1:
            update = coefs[0] * here + coefs[1] * scaled
        else:
            update = coefs[0] * d[0, pl.ds(row, r), :] + coefs[1] * scaled
        if keep:
            d[0, pl.ds(row, r), :] = update
        out[0, pl.ds(row, r), :] = here + update
        return kept

    sweep(lv, fields, upper, x, extent, emit)


def smooth_from_zero(lv, fields, inverse, upper, xa, xb, d, extent):
    r = lv.rows

    def body(p, carry):
        row = pl.multiple_of(p * r, 8)
        xa[0, pl.ds(row, r), :] = inverse[0, pl.ds(row, r), :] * fields[4, pl.ds(row, r), :] * (1.0 / THETA)
        return carry

    loop(lv.e - extent, lv.e + lv.half + extent, body, 0, lv.unroll)
    step(lv, fields, inverse, upper, xa, xb, d, extent - 1, 1, STEP1, True)
    step(lv, fields, inverse, upper, xb, xa, d, extent - 2, 2, STEP2, False)


def smooth(lv, fields, inverse, upper, xa, xb, d, extent):
    step(lv, fields, inverse, upper, xa, xb, d, extent - 1, 0, None, True)
    step(lv, fields, inverse, upper, xb, xa, d, extent - 2, 2, STEP1, True)
    step(lv, fields, inverse, upper, xa, xb, d, extent - 3, 2, STEP2, False)


def coarse_lanes(lv, below, rows, half):
    lane = lanes(rows)
    if below is None:
        cell, at = lane, 0
    else:
        at = (lane // below.span) * 64 if below.ways == 2 else 0
        cell = lane % below.span - below.zo
    if lv.ways == 2 and half is not None:
        at = 64 * half
    inside = (cell >= 0) & (cell < lv.n // 2)
    index = jnp.where(inside, at + lv.zo + 2 * cell, 0)
    return index, inside


def place(lv, below, put, plane, value, pair):
    rows = value.shape[0]
    if pair:
        value = value + roll_lanes(value, -1)
    halves = [None] if below is not None and below.ways == lv.ways else range(lv.ways)
    for half in halves:
        index, inside = coarse_lanes(lv, below, rows, half)
        got = jnp.where(inside, gather_lanes(value, index), 0.0)
        put(plane if half is None else plane + half * (lv.half // 2), got)


def coarsen_fields(lv, below, fields, put):
    n2, e, r = lv.n // 2, lv.e, lv.rows

    def body(i, carry):
        row = (e + 2 * i) * r + e

        def rows(a, plane, odd):
            return fields[a, pl.ds(row + plane * r + odd, n2, stride=2), :]

        put_x = functools.partial(put, 0)
        put_y = functools.partial(put, 1)
        put_z = functools.partial(put, 2)
        put_c = functools.partial(put, 3)
        place(lv, below, put_x, i, (rows(0, 0, 0) + rows(0, 0, 1)) * 0.0625, True)
        place(lv, below, put_y, i, (rows(1, 0, 0) + rows(1, 1, 0)) * 0.0625, True)
        place(lv, below, put_z, i, (rows(2, 0, 0) + rows(2, 0, 1) + rows(2, 1, 0) + rows(2, 1, 1)) * 0.0625, False)
        place(lv, below, put_c, i, (rows(3, 0, 0) + rows(3, 0, 1) + rows(3, 1, 0) + rows(3, 1, 1)) * 0.125, True)
        return carry

    loop(0, lv.half // 2, body, 0, 3)


def restrict(lv, below, fields, upper, x, sums, put):
    r, n2 = lv.rows, lv.n // 2

    def emit(p, row, here, applied, kept):
        sums[0, pl.ds((p - lv.e) * r, r), :] = fields[4, pl.ds(row, r), :] - applied
        return kept

    sweep(lv, fields, upper, x, 0, emit)

    def body(i, carry):
        total = None
        for plane in range(2):
            for odd in range(2):
                part = sums[0, pl.ds((2 * i + plane) * r + lv.e + odd, n2, stride=2), :]
                total = part if total is None else total + part
        place(lv, below, functools.partial(put, 4), i, total * 0.125, True)
        return carry

    loop(0, lv.half // 2, body, 0, 6)


def fields_put(below, fields):
    def put(field, plane, value):
        fields[field, pl.ds((below.e + plane) * below.rows + below.e, below.n), :] = value

    return put


def prolong(lv, above, e, x, reach):
    r, rows = lv.rows, lv.n // 2 + 2 * reach
    lane = lanes(rows)
    cell = lane % 64 - lv.zo + 2 * reach
    inside = (cell >= 0) & (cell < 2 * rows)
    source = above.zo - reach + cell // 2
    if above.ways == 2:
        source = source + (lane // 64) * 64
    source = jnp.where(inside, source, 0)

    def body(i, carry):
        row = (above.e - reach + i) * above.rows + above.e - reach
        value = gather_lanes(e[0, pl.ds(row, rows), :], source)
        if above.ways == 1:
            other = gather_lanes(e[0, pl.ds(row + (lv.half // 2) * above.rows, rows), :], source)
            value = jnp.where(lane < 64, value, other)
        value = jnp.where(inside, value, 0.0)
        for plane in range(2):
            at = (lv.e - 2 * reach + 2 * i + plane) * r + lv.e - 2 * reach
            for odd in range(2):
                where = pl.ds(at + odd, rows, stride=2)
                x[0, where, :] = x[0, where, :] + value
        return carry

    loop(0, lv.half // 2 + 2 * reach, body, 0, 4)


def whole_operator(ny, fields, v, scale):
    rows = lax.broadcasted_iota(jnp.int32, (128, 128), 0)
    z, y = rows % 8, lanes(128) % 6
    last = 6 - scale
    y_low, y_high, z_low, z_high = y == 0, y == last, z == 0, z == last
    bottom, top = rows == 0, rows == 120 + last
    zero = jnp.zeros((128, 128), F32)

    def below_y(g):
        other = roll_lanes(v[g - 1], -last) if g else zero
        return jnp.where(y_low, other, roll_lanes(v[g], scale))

    fluxes_y = [fields(1, g) * (v[g] - below_y(g)) for g in range(ny)]
    out = []
    for g in range(ny):
        flux = fields(0, g) * (v[g] - roll_lanes(v[g], 6 * scale))
        total = flux - roll_lanes(flux, -6 * scale)
        other = roll_lanes(fluxes_y[g + 1], last) if g + 1 < ny else zero
        total = total + (fluxes_y[g] - jnp.where(y_high, other, roll_lanes(fluxes_y[g], -scale)))
        jump = 8 - last
        other = jnp.where(bottom, 0.0, roll_rows(v[g], jump))
        flux = fields(2, g) * (v[g] - jnp.where(z_low, other, roll_rows(v[g], scale)))
        other = jnp.where(top, 0.0, roll_rows(flux, -jump))
        total = total + (flux - jnp.where(z_high, other, roll_rows(flux, -scale)))
        out.append(fields(3, g) * v[g] + total)
    return out


def whole_inverse(ny, fields):
    rows = lax.broadcasted_iota(jnp.int32, (128, 128), 0)
    z, y = rows % 8, lanes(128) % 6
    zero = jnp.zeros((128, 128), F32)
    out = []
    for g in range(ny):
        face_x, face_y, face_z, cells = (fields(a, g) for a in range(4))
        total = cells + face_x + roll_lanes(face_x, -6)
        other = roll_lanes(fields(1, g + 1), 5) if g + 1 < ny else zero
        total = total + face_y + jnp.where(y == 5, other, roll_lanes(face_y, -1))
        other = jnp.where(rows == 125, 0.0, roll_rows(face_z, -3))
        total = total + face_z + jnp.where(z == 5, other, roll_rows(face_z, -1))
        out.append(jnp.where(cells > 0.0, 1.0 / total, 0.0))
    return out


def children(value, axes):
    if "y" in axes:
        value = value + roll_lanes(value, -1)
    if "x" in axes:
        value = value + roll_lanes(value, -6)
    if "z" in axes:
        value = value + roll_rows(value, -1)
    return value


def coarse_solve(ny, gathered, source, inverse, bottom, xs, ds):
    nz = 16
    fields = lambda a, g: gathered[g, :, a].reshape(128, 128)
    f = lambda g: source[g].reshape(128, 128)

    def load(ref):
        return [ref[g] for g in range(ny)]

    def residual(v):
        applied = whole_operator(ny, fields, v, 1)
        return [f(g) - applied[g] for g in range(ny)]

    for g in range(ny):
        xs[g] = inverse[g] * f(g) * (1.0 / THETA)
        ds[g] = xs[g]
    for coefs in (STEP1, STEP2):
        remainder = residual(load(xs))
        for g in range(ny):
            update = coefs[0] * ds[g] + coefs[1] * (inverse[g] * remainder[g])
            ds[g] = update
            xs[g] = xs[g] + update
    remainder = residual(load(xs))
    inside = lambda g, value: jnp.where(bottom[3, g] > 0.0, value, 0.0)
    r = [inside(g, children(remainder[g], "xyz") * 0.125) for g in range(ny)]

    def total(values):
        values = functools.reduce(lambda a, b: a + b, values)
        return jnp.sum(jnp.sum(values, axis=0, keepdims=True), axis=1, keepdims=True)

    coarse = lambda a, g: bottom[a, g]
    e = [jnp.zeros((128, 128), F32)] * ny
    norm = total([a * a for a in r])

    def body(i, carry):
        e, r, p, norm = carry
        q = [inside(g, a) for g, a in enumerate(whole_operator(ny, coarse, p, 2))]
        size = norm / total([a * b for a, b in zip(p, q)])
        e = [a + size * b for a, b in zip(e, p)]
        r = [a - size * b for a, b in zip(r, q)]
        after = total([a * a for a in r])
        p = [a + after / norm * b for a, b in zip(r, p)]
        return e, r, p, after

    e, r, p, norm = lax.fori_loop(0, BOTTOM - 1, body, (e, r, r, norm))
    q = [inside(g, a) for g, a in enumerate(whole_operator(ny, coarse, p, 2))]
    size = norm / total([a * b for a, b in zip(p, q)])
    for g in range(ny):
        value = e[g] + size * p[g]
        value = value + roll_lanes(value, 1)
        value = value + roll_lanes(value, 6)
        xs[g] = xs[g] + (value + roll_rows(value, 1))
    for number, coefs in enumerate((None, STEP1, STEP2)):
        remainder = residual(load(xs))
        for g in range(ny):
            update = inverse[g] * remainder[g]
            if number == 0:
                update = update * (1.0 / THETA)
            else:
                update = coefs[0] * ds[g] + coefs[1] * update
            ds[g] = update
            xs[g] = xs[g] + update


def coarse_fields(ny, gathered, bottom):
    fields = lambda a, g: gathered[g, :, a].reshape(128, 128)
    rows = lax.broadcasted_iota(jnp.int32, (128, 128), 0)
    lane = lanes(128)
    even = (rows % 2 == 0) & (lane % 2 == 0) & ((lane // 6) % 2 == 0) & (lane < 72)
    for g in range(ny):
        for a, axes in enumerate(("yz", "xz", "xy", "xyz")):
            factor = 0.125 if a == 3 else 0.0625
            bottom[a, g] = jnp.where(even, children(fields(a, g), axes) * factor, 0.0)


def window(lv, gx, gy, gz, ny, xs, padded, turned, corner, x):
    nz = 16
    padded[...] = jnp.zeros_like(padded)
    for g in range(ny):
        padded[g + 1, pl.ds(1, nz)] = xs[g].reshape(nz, 8, 128)
    for dy in range(3):
        tiles = padded[gy + dy, pl.ds(gz, 3)].reshape(24, 128)
        tiles = jnp.concatenate([tiles, jnp.zeros((104, 128), F32)], axis=0)
        turned[dy, pl.ds(0, 24), :] = jnp.zeros((24, 128), F32)
        turned[dy, pl.ds(24, 128), :] = tiles.T
    lane = lanes(16)
    cell = lane - lv.zo + 6
    inside = (cell >= 0) & (cell < 24)
    coarse = jnp.where(inside, cell // 2 + 3, 0)
    source = (coarse // 6) * 8 + coarse % 6

    def body(i, carry):
        base = 6 + 36 * gx + 6 * i
        corner[pl.ds(0, 3), :] = turned[0, pl.ds(base + 3, 3), :]
        corner[pl.ds(3, 6), :] = turned[1, pl.ds(base, 6), :]
        corner[pl.ds(9, 3), :] = turned[2, pl.ds(base, 3), :]
        value = jnp.where(inside, gather_lanes(corner[...], source), 0.0)[0:12]
        for plane in range(2):
            at = (lv.e - 6 + 2 * i + plane) * lv.rows + lv.e - 6
            for odd in range(2):
                where = pl.ds(at + odd, 12, stride=2)
                x[0, where, :] = x[0, where, :] + value
        return carry

    loop(0, 12, body, 0, 4)


def hops(t, nz):
    return sum(min(d, 4 - d) for d in (t // nz % 4, t % nz // 4, t % 4))


def cycle(ny, nz, names, *refs):
    refs = list(refs)
    right_hbm, faces_hbm, cells_hbm, solution_hbm, residual_hbm, norm_out = refs[:6]
    s = dict(zip(names, refs[6:]))
    gx, gy, gz = lax.axis_index("gx"), lax.axis_index("gy"), lax.axis_index("gz")
    here = (gx, gy, gz, ny, nz)
    scope = jax.named_scope

    loads = [pltpu.make_async_copy(faces_hbm.at[d], s["land"].at[d], s["load_sem"].at[d]) for d in range(3)]
    loads.append(pltpu.make_async_copy(cells_hbm, s["land"].at[3], s["load_sem"].at[3]))
    loads.append(pltpu.make_async_copy(right_hbm, s["land"].at[4], s["load_sem"].at[4]))
    for copy in loads:
        copy.start()

    def other(t):
        return lax.rem(gy + t // nz, ny), lax.rem(gz + t % nz, nz)

    order = sorted(range(1, ny * nz), key=lambda t: -hops(t, nz))
    barrier = pltpu.get_barrier_semaphore()
    with scope("greet"):
        for t in order:
            oy, oz = other(t)
            pl.semaphore_signal(barrier, inc=1, device_id=(gx, oy, oz), device_id_type=MESH)
        pl.semaphore_signal(barrier, inc=1, device_id=(1 - gx, gy, gz), device_id_type=MESH)

    f0, f1, f2 = s["f0"], s["f1"], s["f2"]
    ex = {k: Exchange(*v) for k, v in EXCHANGES.items()}
    targets = {"e0": f0, "c1": f1, "c2": f2, "e1": f1, "e2": f2, "x0": s["x0a"], "x1": s["x1a"], "x2": s["x2a"]}
    for k, target in targets.items():
        ex[k].bind(here, target, [s[k + str(i)] for i in range(10)])

    def partner(src, dst, i):
        return pltpu.make_async_remote_copy(
            src_ref=src,
            dst_ref=dst,
            send_sem=s["pair_send"].at[i],
            recv_sem=s["pair_recv"].at[i],
            device_id=(1 - gx, gy, gz),
            device_id_type=MESH,
        )

    def spread(src, slot, i):
        def one(t, y, z):
            oy, oz = other(t)
            return pltpu.make_async_remote_copy(
                src_ref=src,
                dst_ref=slot(y, z),
                send_sem=s["all_send"].at[i, t],
                recv_sem=s["all_recv"].at[i, t],
                device_id=(gx, oy, oz),
                device_id_type=MESH,
            )

        def start():
            for t in order:
                one(t, gy, gz).start()

        def finish():
            def body(t, carry):
                one(t, lax.rem(gy + ny - t // nz, ny), lax.rem(gz + nz - t % nz, nz)).wait()
                return carry

            lax.fori_loop(1, ny * nz, body, 0)

        return start, finish

    f1[...] = jnp.zeros_like(f1)
    f2[...] = jnp.zeros_like(f2)
    block = s["block"]
    block[...] = jnp.zeros_like(block)

    def block_put(field, plane, value):
        block[field, pl.ds(plane * 6, 6), :] = value

    for a in range(5):
        with scope("load_wait"):
            loads[a].wait()

        def load(i, carry, a=a):
            first = jnp.pad(s["land"][a, i], ((0, 0), (0, 80)))
            second = jnp.pad(s["land"][a, i + 24], ((0, 0), (0, 80)))
            value = roll_lanes(first, L0.zo) + roll_lanes(second, 64 + L0.zo)
            f0[a, pl.ds((L0.e + i) * L0.rows + L0.e, 48), :] = value
            return carry

        with scope("layout"):
            loop(0, 24, load, 0, 6)

    with scope("barrier"):
        pl.semaphore_wait(barrier, ny * nz)
    ex["e0"].start_x()
    with scope("coarsen_0"):
        coarsen_fields(L0, L1, f0, fields_put(L1, f1))
    ex["c1"].start_x()
    with scope("e0_finish_x"):
        ex["e0"].finish_x()
    with scope("e0_start_yz"):
        ex["e0"].start_yz()
    with scope("coarsen_1"):
        coarsen_fields(L1, L2, f1, fields_put(L2, f2))
    ex["c2"].start_x()
    with scope("coarsen_2"):
        coarsen_fields(L2, None, f2, block_put)

    def tile_of(field):
        return roll_lanes(block[field].T[0:8], gx * 36)

    own4, pair4, own1, pair1, own_n, pair_n = (s[k] for k in ("own4", "pair4", "own1", "pair1", "own_n", "pair_n"))
    for field in range(4):
        own4[field] = tile_of(field)
    pair_coef = partner(own4, pair4, 0)
    pair_coef.start()

    def square(i, carry):
        value = f0[4, pl.ds((L0.e + i) * L0.rows + L0.e, 48), :]
        return carry + value * value

    with scope("square"):
        squares = loop(0, 24, square, jnp.zeros((48, 128), F32), 4)
    with scope("c1_finish_x"):
        ex["c1"].finish_x()
    with scope("c1_start_yz"):
        ex["c1"].start_yz()
    with scope("c2_finish_x"):
        ex["c2"].finish_x()
    with scope("c2_start_yz"):
        ex["c2"].start_yz()
    g4, g1, gn = s["g4"], s["g1"], s["gn"]
    with scope("pair_coef"):
        pair_coef.wait()
    merged = s["merged4"]
    merged[...] = own4[...] + pair4[...]
    mine = pl.ds(2 * gx, 2)
    g4[gy, gz, mine] = merged[mine]
    coef_start, coef_finish = spread(merged.at[mine], lambda y, z: g4.at[y, z, mine], 0)
    with scope("coef_start"):
        coef_start()
    with scope("e0_finish_yz"):
        ex["e0"].finish_yz()
    with scope("scaling_0"):
        scaling(L0, f0, s["i0"], s["u0"], 3)
    with scope("smooth_0"):
        smooth_from_zero(L0, f0, s["i0"], s["u0"], s["x0a"], s["x0b"], s["d0"], 3)
    with scope("restrict_0"):
        restrict(L0, L1, f0, s["u0"], s["x0a"], s["sums"], fields_put(L1, f1))
    ex["e1"].start_x()
    with scope("c1_finish_yz"):
        ex["c1"].finish_yz()
    with scope("e1_finish_x"):
        ex["e1"].finish_x()
    with scope("e1_start_yz"):
        ex["e1"].start_yz()
    ex["x0"].start_x()
    with scope("c2_finish_yz"):
        ex["c2"].finish_yz()
    with scope("scaling_12"):
        scaling(L1, f1, s["i1"], s["u1"], 4)
        scaling(L2, f2, s["i2"], s["u2"], 5)
    with scope("e1_finish_yz"):
        ex["e1"].finish_yz()
    with scope("smooth_1"):
        smooth_from_zero(L1, f1, s["i1"], s["u1"], s["x1a"], s["x1b"], s["d1"], 3)
    with scope("restrict_1"):
        restrict(L1, L2, f1, s["u1"], s["x1a"], s["sums"], fields_put(L2, f2))
    ex["e2"].start_x()
    ex["x1"].start_x()
    with scope("x0_finish_x"):
        ex["x0"].finish_x()
    with scope("e2_finish_x"):
        ex["e2"].finish_x()
    with scope("e2_start_yz"):
        ex["e2"].start_yz()
    with scope("coef_finish"):
        coef_finish()
    other_half = pltpu.make_async_remote_copy(
        src_ref=g4.at[:, :, mine],
        dst_ref=g4.at[:, :, mine],
        send_sem=s["pair_send"].at[3],
        recv_sem=s["pair_recv"].at[3],
        device_id=(1 - gx, gy, gz),
        device_id_type=MESH,
    )
    other_half.start()
    with scope("x0_start_yz"):
        ex["x0"].start_yz()
    with scope("e2_finish_yz"):
        ex["e2"].finish_yz()
    with scope("smooth_2"):
        smooth_from_zero(L2, f2, s["i2"], s["u2"], s["x2a"], s["x2b"], s["d2"], 3)
    with scope("restrict_2"):
        restrict(L2, None, f2, s["u2"], s["x2a"], s["sums"], block_put)
    own1[...] = tile_of(4)
    pair_source = partner(own1, pair1, 1)
    pair_source.start()
    ex["x2"].start_x()
    with scope("other_half"):
        other_half.wait()
    with scope("pair_source"):
        pair_source.wait()
    s["merged1"][...] = own1[...] + pair1[...]
    g1[gy, gz] = s["merged1"][...]
    source_start, source_finish = spread(s["merged1"], lambda y, z: g1.at[y, z], 1)
    with scope("source_start"):
        source_start()
    gathered = lambda a, g: g4[g, :, a].reshape(128, 128)
    with scope("coarse_fields"):
        inverse = whole_inverse(ny, gathered)
        for g in range(ny):
            s["i3"][g] = inverse[g]
        coarse_fields(ny, g4, s["bottom"])
    with scope("hidden"):
        ex["x1"].finish_x()
        ex["x1"].start_yz()
        ex["x2"].finish_x()
        ex["x2"].start_yz()
        ex["x0"].finish_yz()
    with scope("source_finish"):
        source_finish()
    with scope("coarse_solve"):
        coarse_solve(ny, g4, g1, s["i3"], s["bottom"], s["x3"], s["d3"])
    with scope("x2_finish_yz"):
        ex["x2"].finish_yz()
    with scope("window"):
        window(L2, gx, gy, gz, ny, s["x3"], s["padded"], s["turned"], s["corner"], s["x2a"])
    with scope("post_2"):
        smooth(L2, f2, s["i2"], s["u2"], s["x2a"], s["x2b"], s["d2"], 6)
    with scope("x1_finish_yz"):
        ex["x1"].finish_yz()
    with scope("prolong_1"):
        prolong(L1, L2, s["x2b"], s["x1a"], 3)
    with scope("post_1"):
        smooth(L1, f1, s["i1"], s["u1"], s["x1a"], s["x1b"], s["d1"], 5)
    with scope("prolong_0"):
        prolong(L0, L1, s["x1b"], s["x0a"], 2)
    with scope("post_0"):
        smooth(L0, f0, s["i0"], s["u0"], s["x0a"], s["x0b"], s["d0"], 4)

    land = s["land"]
    r0 = L0.rows
    lane48 = lanes(48) % 64
    inside = (lane48 >= L0.zo) & (lane48 < L0.zo + 48)

    def final(p, row, here_x, applied, kept):
        s["sums"][0, pl.ds((p - L0.e) * r0, r0), :] = f0[4, pl.ds(row, r0), :] - applied
        return kept

    with scope("final"):
        sweep(L0, f0, s["u0"], s["x0b"], 0, final)

    def out_square(i, carry):
        value = jnp.where(inside, s["sums"][0, pl.ds(i * r0 + L0.e, 48), :], 0.0)
        return carry + value * value

    with scope("square"):
        ends = loop(0, 24, out_square, jnp.zeros((48, 128), F32), 4)

    def fold(value):
        return jnp.sum(value, axis=0, keepdims=True)

    own_n[...] = jnp.concatenate([fold(squares), fold(ends), jnp.zeros((6, 128), F32)], axis=0)
    pair_norm = partner(own_n, pair_n, 2)
    pair_norm.start()

    def unload(slot, i, value):
        for half in range(2):
            moved = roll_lanes(value, -(L0.zo + 64 * half))
            land[slot, i + 24 * half] = moved[:, 0:48]

    def out_solution(i, carry):
        unload(0, i, s["x0b"][0, pl.ds((L0.e + i) * r0 + L0.e, 48), :])
        return carry

    def out_residual(i, carry):
        unload(1, i, s["sums"][0, pl.ds(i * r0 + L0.e, 48), :])
        return carry

    with scope("unload_solution"):
        loop(0, 24, out_solution, 0, 6)
    out0 = pltpu.make_async_copy(land.at[0], solution_hbm, s["out_sem"].at[0])
    out0.start()
    with scope("pair_norm"):
        pair_norm.wait()
    s["merged_n"][...] = jnp.where(gx == 0, own_n[...] + pair_n[...], pair_n[...] + own_n[...])
    gn[gy, gz] = s["merged_n"][...]
    norm_start, norm_finish = spread(s["merged_n"], lambda y, z: gn.at[y, z], 2)
    with scope("norm_start"):
        norm_start()
    with scope("unload_residual"):
        loop(0, 24, out_residual, 0, 6)
    out1 = pltpu.make_async_copy(land.at[1], residual_hbm, s["out_sem"].at[1])
    out1.start()
    with scope("norm_finish"):
        norm_finish()
    all_n = jnp.sum(gn[...].reshape(ny * nz, 8, 128), axis=0)
    sums = jnp.sum(all_n, axis=1, keepdims=True)
    norm = jnp.sqrt(sums[1:2] / sums[0:1])
    norm_out[0, 0] = norm[0, 0]
    with scope("out_wait"):
        out0.wait()
        out1.wait()


EXCHANGES = {
    "e0": (L0, 0, 5),
    "c1": (L1, 0, 4),
    "c2": (L2, 0, 4),
    "e1": (L1, 4, 1),
    "e2": (L2, 4, 1),
    "x0": (L0, 0, 1),
    "x1": (L1, 0, 1),
    "x2": (L2, 0, 1),
}


def scratch_of(ny, nz):
    vmem = lambda *shape: pltpu.VMEM(shape, F32)
    size = lambda lv: lv.planes * lv.rows
    scratch = {"land": vmem(5, 48, 48, 48), "load_sem": pltpu.SemaphoreType.DMA((5,)), "out_sem": pltpu.SemaphoreType.DMA((2,))}
    for i, lv in enumerate((L0, L1, L2)):
        scratch[f"f{i}"] = vmem(5, size(lv), 128)
        for k in ("i", "d", "u"):
            scratch[f"{k}{i}"] = vmem(1, size(lv), 128)
        scratch[f"x{i}a"] = vmem(1, size(lv), 128)
        scratch[f"x{i}b"] = vmem(1, size(lv), 128)
    scratch["sums"] = vmem(1, 24 * 56, 128)
    scratch["block"] = vmem(5, 128, 128)
    for k in ("own4", "pair4", "merged4"):
        scratch[k] = vmem(4, 8, 128)
    for k in ("own1", "pair1", "merged1", "own_n", "pair_n", "merged_n"):
        scratch[k] = vmem(8, 128)
    scratch["g4"] = vmem(ny, nz, 4, 8, 128)
    scratch["g1"] = vmem(ny, nz, 8, 128)
    scratch["gn"] = vmem(ny, nz, 8, 128)
    for k in ("pair_send", "pair_recv"):
        scratch[k] = pltpu.SemaphoreType.DMA((4,))
    for k in ("all_send", "all_recv"):
        scratch[k] = pltpu.SemaphoreType.DMA((3, ny * nz))
    for k in ("i3", "x3", "d3"):
        scratch[k] = vmem(ny, 128, 128)
    scratch["bottom"] = vmem(4, ny, 128, 128)
    scratch["padded"] = vmem(ny + 2, nz + 2, 8, 128)
    scratch["turned"] = vmem(3, 152, 128)
    scratch["corner"] = vmem(16, 128)
    for k, v in EXCHANGES.items():
        for i, shape in enumerate(Exchange(*v).scratch()):
            scratch[k + str(i)] = shape
    return scratch


def solution(mesh):
    ny, nz = mesh.shape["gy"], mesh.shape["gz"]
    scratch = scratch_of(ny, nz)

    def shards(right_side, face_coef, absorption):
        field = jax.ShapeDtypeStruct((48, 48, 48), F32)
        solved, residual, norm = pl.pallas_call(
            functools.partial(cycle, ny, nz, tuple(scratch)),
            out_shape=(field, field, jax.ShapeDtypeStruct((1, 1), F32)),
            in_specs=[pl.BlockSpec(memory_space=pl.ANY)] * 3,
            out_specs=(
                pl.BlockSpec(memory_space=pl.ANY),
                pl.BlockSpec(memory_space=pl.ANY),
                pl.BlockSpec(memory_space=pltpu.SMEM),
            ),
            scratch_shapes=list(scratch.values()),
            compiler_params=pltpu.CompilerParams(
                collective_id=0, has_side_effects=True, vmem_limit_bytes=62 * 1024 * 1024
            ),
        )(right_side, face_coef, absorption)
        return solved, residual, norm[0, 0]

    in_specs = (P("gx", "gy", "gz"), P(None, "gx", "gy", "gz"), P("gx", "gy", "gz"))
    out_specs = (P("gx", "gy", "gz"), P("gx", "gy", "gz"), P())
    return jax.shard_map(shards, mesh=mesh, in_specs=in_specs, out_specs=out_specs, check_vma=False)
```

```python
import functools

import jax
import jax.numpy as jnp
from jax import lax
from jax.experimental import pallas as pl
from jax.experimental.pallas import tpu as pltpu
from jax.sharding import PartitionSpec as P

BOTTOM = 6
THETA = 1.125
DELTA = 0.875
SIGMA = THETA / DELTA
RHO0 = 1.0 / SIGMA
RHO1 = 1.0 / (2.0 * SIGMA - RHO0)
RHO2 = 1.0 / (2.0 * SIGMA - RHO1)
STEP1 = (RHO1 * RHO0, 2.0 * RHO1 / DELTA)
STEP2 = (RHO2 * RHO1, 2.0 * RHO2 / DELTA)

F32 = jnp.float32
MESH = pl.DeviceIdType.MESH


class Level:
    def __init__(self, n, e, ways, rows, zo, width, width_y, unroll):
        self.n, self.e, self.ways, self.rows, self.zo, self.width = n, e, ways, rows, zo, width
        self.width_y, self.unroll = width_y, unroll
        self.half = n // ways
        self.planes = self.half + 2 * e
        self.span = 128 // ways
        self.slots, self.slots_y = self.span // width, self.span // width_y
        self.packs, self.packs_y = -(-self.half // self.slots), -(-self.half // self.slots_y)


L0 = Level(48, 4, 2, 56, 8, 4, 64, 4)
L1 = Level(24, 6, 2, 40, 16, 8, 32, 4)
L2 = Level(12, 6, 1, 24, 16, 8, 16, 6)


def lanes(rows):
    return lax.broadcasted_iota(jnp.int32, (rows, 128), 1)


def gather_lanes(value, index):
    return jnp.take_along_axis(value, index, axis=1)


def roll_lanes(value, shift):
    return pltpu.roll(value, shift % 128, 1)


def roll_rows(value, shift):
    return pltpu.roll(value, shift % value.shape[0], 0)


def tile_rows(start, size):
    return pl.ds(pl.multiple_of(start, 8), size)


def loop(lo, hi, body, carry, unroll):
    count = (hi - lo) // unroll

    def chunk(i, carry):
        for k in range(unroll):
            carry = body(lo + i * unroll + k, carry)
        return carry

    carry = lax.fori_loop(0, count, chunk, carry)
    for k in range(lo + count * unroll, hi):
        carry = body(k, carry)
    return carry


class Exchange:
    def __init__(self, level, first, count):
        self.level, self.first, self.count = level, first, count
        lv = level
        sizes = [-(-rows // 8) * 8 for rows in (lv.packs_y * lv.e, lv.packs * lv.n, lv.packs * lv.e)]
        self.sizes = [sizes[0]] * 2 + [sizes[1]] * 2 + [sizes[2]] * 4
        self.starts = [sum(self.sizes[:i]) for i in range(9)]

    def scratch(self):
        lv, na = self.level, self.count
        shapes = [
            (na, lv.e * lv.rows, 128),
            (na, self.starts[8], 128),
            (na, self.starts[8], 128),
            (2, na, lv.packs * lv.rows, 128),
        ]
        return [pltpu.VMEM(s, F32) for s in shapes] + [pltpu.SemaphoreType.DMA((2,)), pltpu.SemaphoreType.DMA((2,))]

    def bind(self, here, ref, scratch):
        self.here, self.ref = here, ref
        self.xr, self.out, self.got, self.zf, self.ssem, self.rsem = scratch
        gx, gy, gz, ny, nz = here
        lv = self.level
        start = lv.e + (1 - gx) * (lv.half - lv.e if lv.ways == 2 else lv.n - lv.e)

        def copy(src, dst, i, gx, gy, gz):
            return pltpu.make_async_remote_copy(
                src_ref=src,
                dst_ref=dst,
                send_sem=self.ssem.at[i],
                recv_sem=self.rsem.at[i],
                device_id=(gx, gy, gz),
                device_id_type=MESH,
            )

        src = ref.at[pl.ds(self.first, self.count), tile_rows(start * lv.rows, lv.e * lv.rows), :]
        self.copy_x = copy(src, self.xr, 0, 1 - gx, gy, gz)
        ys = [lax.rem(gy + ny - 1, ny), lax.rem(gy + 1, ny)]
        zs = [lax.rem(gz + nz - 1, nz), lax.rem(gz + 1, nz)]
        targets = [(ys[0], gz), (ys[1], gz), (gy, zs[0]), (gy, zs[1])] + [(y, z) for y in ys for z in zs]
        lands = [1, 0, 3, 2, 7, 6, 5, 4]
        self.copies = [
            copy(
                self.out.at[:, pl.ds(self.starts[i], self.sizes[i]), :],
                self.got.at[:, pl.ds(self.starts[lands[i]], self.sizes[i]), :],
                1,
                gx,
                *targets[i],
            )
            for i in range(8)
        ]
        self.all = copy(self.out, self.got, 1, gx, *targets[0])
        self.has_y = [jnp.where(gy > 0, 1.0, 0.0).astype(F32), jnp.where(gy < ny - 1, 1.0, 0.0).astype(F32)]
        self.has_z = [jnp.where(gz > 0, 1.0, 0.0).astype(F32), jnp.where(gz < nz - 1, 1.0, 0.0).astype(F32)]
        self.has_x = [gx.astype(F32), (1 - gx).astype(F32)]
        return self

    def start_x(self):
        self.copy_x.start()

    def finish_x(self):
        lv, ref = self.level, self.ref
        e, r = lv.e, lv.rows
        self.copy_x.wait()
        low = lanes(r) < 64

        def finish(a, j):
            got = self.xr[a, tile_rows(j * r, r), :]
            if lv.ways == 2:
                got = roll_lanes(got, 64)
                below = roll_lanes(ref[self.first + a, tile_rows((lv.half + j) * r, r), :], 64)
                above = roll_lanes(ref[self.first + a, tile_rows((e + j) * r, r), :], 64)
                below = jnp.where(low, got * self.has_x[0], below)
                above = jnp.where(low, above, got * self.has_x[1])
            else:
                below = got * self.has_x[0]
                above = got * self.has_x[1]
            ref[self.first + a, tile_rows(j * r, r), :] = below
            ref[self.first + a, tile_rows((e + lv.half + j) * r, r), :] = above

        def body(a, carry):
            for j in range(e):
                finish(a, j)
            return carry

        lax.fori_loop(0, self.count, body, 0)

    def pack(self, plane, rows, width, shifts, put):
        lv = self.level
        slot = (lanes(rows) % lv.span) // width
        slots = lv.span // width
        for k in range(-(-lv.half // slots)):
            acc = None
            for s in range(min(slots, lv.half - k * slots)):
                moved = [roll_lanes(v, s * width - shift) for v, shift in zip(plane(lv.e + k * slots + s), shifts)]
                acc = moved if s == 0 else [jnp.where(slot == s, new, old) for new, old in zip(moved, acc)]
            put(k, acc)

    def pack_yz(self, send):
        lv, ref = self.level, self.ref
        r, n, e, zo = lv.rows, lv.n, lv.e, lv.zo
        z_shifts = (zo, zo + n - e)

        def put_at(first, rows, a):
            def put(k, values):
                for i, value in enumerate(values):
                    self.out[a, pl.ds(self.starts[first + i] + k * rows, rows), :] = value

            return put

        def edges(a, p):
            return [ref[self.first + a, pl.ds(p * r + row, e), :] for row in (e, n)]

        def pack_d(a, carry):
            def plane(p):
                low, high = edges(a, p)
                return low, low, high, high

            self.pack(plane, e, lv.width, z_shifts * 2, put_at(4, e, a))
            return carry

        def pack_z(a, carry):
            def plane(p):
                return [ref[self.first + a, pl.ds(p * r + e, n), :]] * 2

            self.pack(plane, n, lv.width, z_shifts, put_at(2, n, a))
            return carry

        def pack_y(a, carry):
            if lv.slots_y == 1:
                for k in range(lv.half):
                    put_at(0, e, a)(k, edges(a, e + k))
            else:
                self.pack(lambda p: edges(a, p), e, lv.width_y, (zo, zo), put_at(0, e, a))
            return carry

        for body, which in ((pack_d, range(4, 8)), (pack_z, (2, 3)), (pack_y, (0, 1))):
            lax.fori_loop(0, self.count, body, 0)
            if send:
                for i in which:
                    self.copies[i].start()

    def send_yz(self):
        for i in (4, 5, 6, 7, 2, 3, 0, 1):
            self.copies[i].start()

    def start_yz(self):
        self.pack_yz(True)

    def finish_yz(self):
        lv, ref = self.level, self.ref
        r, n, e, zo = lv.rows, lv.n, lv.e, lv.zo
        with jax.named_scope("arrive"):
            self.all.wait()
        lane = lanes(r) % lv.span
        at_low = (lane >= zo - e) & (lane < zo)
        at_high = (lane >= zo + n) & (lane < zo + n + e)

        def unpack(a, carry):
            def got(i, row, rows):
                return self.got[a, pl.ds(self.starts[i] + row, rows), :]

            for s in range(2):
                for k in range(lv.packs_y):
                    value = got(s, k * e, e) * self.has_y[s]
                    for slot in range(min(lv.slots_y, lv.half - k * lv.slots_y)):
                        row = (e + k * lv.slots_y + slot) * r + (e + n) * s
                        moved = roll_lanes(value, zo - slot * lv.width_y) if lv.slots_y > 1 else value
                        ref[self.first + a, pl.ds(row, e), :] = moved
            for k in range(lv.packs):
                for t in range(2):
                    self.zf[t, a, pl.ds(k * r + e, n), :] = got(2 + t, k * n, n) * self.has_z[t]
                    for s in range(2):
                        both = self.has_y[s] * self.has_z[t]
                        self.zf[t, a, pl.ds(k * r + (e + n) * s, e), :] = got(4 + 2 * s + t, k * e, e) * both
            for k in range(lv.packs):
                sides = [self.zf[t, a, pl.ds(k * r, r), :] for t in range(2)]
                for s in range(min(lv.slots, lv.half - k * lv.slots)):
                    p = e + k * lv.slots + s
                    value = ref[self.first + a, pl.ds(p * r, r), :]
                    value = jnp.where(at_low, roll_lanes(sides[0], zo - e - s * lv.width), value)
                    value = jnp.where(at_high, roll_lanes(sides[1], zo + n - s * lv.width), value)
                    ref[self.first + a, pl.ds(p * r, r), :] = value
            return carry

        lax.fori_loop(0, self.count, unpack, 0)


def scaling(lv, fields, inverse, upper, extent):
    r = lv.rows

    def body(p, carry):
        row = pl.multiple_of(p * r, 8)
        cells = fields[3, pl.ds(row, r), :]
        face_z = fields[2, pl.ds(row, r), :]
        total = cells + fields[0, pl.ds(row, r), :] + fields[0, pl.ds(row + r, r), :]
        total = total + fields[1, pl.ds(row, r), :] + fields[1, pl.ds(row + 1, r), :]
        above = roll_lanes(face_z, -1)
        upper[0, pl.ds(row, r), :] = above
        total = total + face_z + above
        inverse[0, pl.ds(row, r), :] = jnp.where(cells > 0.0, 1.0 / total, 0.0)
        return carry

    loop(lv.e - extent, lv.e + lv.half + extent, body, 0, lv.unroll)


def sweep(lv, fields, upper, x, extent, emit, carry=0):
    r = lv.rows
    lo, hi = lv.e - extent, lv.e + lv.half + extent

    def body(p, carry):
        here, flux, kept = carry
        row = pl.multiple_of(p * r, 8)
        after = x[0, pl.ds(row + r, r), :]
        flux_after = fields[0, pl.ds(row + r, r), :] * (after - here)
        low_y = x[0, pl.ds(row - 1, r), :]
        high_y = x[0, pl.ds(row + 1, r), :]
        flux_y = fields[1, pl.ds(row, r), :] * (here - low_y)
        flux_y = flux_y - fields[1, pl.ds(row + 1, r), :] * (high_y - here)
        flux_z = fields[2, pl.ds(row, r), :] * (here - roll_lanes(here, 1))
        flux_z = flux_z - upper[0, pl.ds(row, r), :] * (roll_lanes(here, -1) - here)
        applied = fields[3, pl.ds(row, r), :] * here + ((flux - flux_after) + flux_y + flux_z)
        return after, flux_after, emit(p, row, here, applied, kept)

    row = lo * r
    here = x[0, pl.ds(row, r), :]
    flux = fields[0, pl.ds(row, r), :] * (here - x[0, pl.ds(row - r, r), :])
    return loop(lo, hi, body, (here, flux, carry), lv.unroll)[2]


def step(lv, fields, inverse, upper, x, out, d, extent, first, coefs, keep):
    r = lv.rows

    def emit(p, row, here, applied, kept):
        scaled = inverse[0, pl.ds(row, r), :] * (fields[4, pl.ds(row, r), :] - applied)
        if first == 0:
            update = scaled * (1.0 / THETA)
        elif first == 1:
            update = coefs[0] * here + coefs[1] * scaled
        else:
            update = coefs[0] * d[0, pl.ds(row, r), :] + coefs[1] * scaled
        if keep:
            d[0, pl.ds(row, r), :] = update
        out[0, pl.ds(row, r), :] = here + update
        return kept

    sweep(lv, fields, upper, x, extent, emit)


def smooth_from_zero(lv, fields, inverse, upper, xa, xb, d, extent):
    r = lv.rows

    def body(p, carry):
        row = pl.multiple_of(p * r, 8)
        xa[0, pl.ds(row, r), :] = inverse[0, pl.ds(row, r), :] * fields[4, pl.ds(row, r), :] * (1.0 / THETA)
        return carry

    loop(lv.e - extent, lv.e + lv.half + extent, body, 0, lv.unroll)
    step(lv, fields, inverse, upper, xa, xb, d, extent - 1, 1, STEP1, True)
    step(lv, fields, inverse, upper, xb, xa, d, extent - 2, 2, STEP2, False)


def smooth(lv, fields, inverse, upper, xa, xb, d, extent):
    step(lv, fields, inverse, upper, xa, xb, d, extent - 1, 0, None, True)
    step(lv, fields, inverse, upper, xb, xa, d, extent - 2, 2, STEP1, True)
    step(lv, fields, inverse, upper, xa, xb, d, extent - 3, 2, STEP2, False)


def coarse_lanes(lv, below, rows, half):
    lane = lanes(rows)
    if below is None:
        cell, at = lane, 0
    else:
        at = (lane // below.span) * 64 if below.ways == 2 else 0
        cell = lane % below.span - below.zo
    if lv.ways == 2 and half is not None:
        at = 64 * half
    inside = (cell >= 0) & (cell < lv.n // 2)
    index = jnp.where(inside, at + lv.zo + 2 * cell, 0)
    return index, inside


def place(lv, below, put, plane, value, pair):
    rows = value.shape[0]
    if pair:
        value = value + roll_lanes(value, -1)
    halves = [None] if below is not None and below.ways == lv.ways else range(lv.ways)
    for half in halves:
        index, inside = coarse_lanes(lv, below, rows, half)
        got = jnp.where(inside, gather_lanes(value, index), 0.0)
        put(plane if half is None else plane + half * (lv.half // 2), got)


def coarsen_fields(lv, below, fields, put):
    n2, e, r = lv.n // 2, lv.e, lv.rows

    def body(i, carry):
        row = (e + 2 * i) * r + e

        def rows(a, plane, odd):
            return fields[a, pl.ds(row + plane * r + odd, n2, stride=2), :]

        put_x = functools.partial(put, 0)
        put_y = functools.partial(put, 1)
        put_z = functools.partial(put, 2)
        put_c = functools.partial(put, 3)
        place(lv, below, put_x, i, (rows(0, 0, 0) + rows(0, 0, 1)) * 0.0625, True)
        place(lv, below, put_y, i, (rows(1, 0, 0) + rows(1, 1, 0)) * 0.0625, True)
        place(lv, below, put_z, i, (rows(2, 0, 0) + rows(2, 0, 1) + rows(2, 1, 0) + rows(2, 1, 1)) * 0.0625, False)
        place(lv, below, put_c, i, (rows(3, 0, 0) + rows(3, 0, 1) + rows(3, 1, 0) + rows(3, 1, 1)) * 0.125, True)
        return carry

    loop(0, lv.half // 2, body, 0, 3)


def restrict(lv, below, fields, upper, x, sums, put):
    r, n2 = lv.rows, lv.n // 2

    def emit(p, row, here, applied, kept):
        sums[0, pl.ds((p - lv.e) * r, r), :] = fields[4, pl.ds(row, r), :] - applied
        return kept

    sweep(lv, fields, upper, x, 0, emit)

    def body(i, carry):
        total = None
        for plane in range(2):
            for odd in range(2):
                part = sums[0, pl.ds((2 * i + plane) * r + lv.e + odd, n2, stride=2), :]
                total = part if total is None else total + part
        place(lv, below, functools.partial(put, 4), i, total * 0.125, True)
        return carry

    loop(0, lv.half // 2, body, 0, 6)


def fields_put(below, fields):
    def put(field, plane, value):
        fields[field, pl.ds((below.e + plane) * below.rows + below.e, below.n), :] = value

    return put


def prolong(lv, above, e, x, reach):
    r, rows = lv.rows, lv.n // 2 + 2 * reach
    lane = lanes(rows)
    cell = lane % 64 - lv.zo + 2 * reach
    inside = (cell >= 0) & (cell < 2 * rows)
    source = above.zo - reach + cell // 2
    if above.ways == 2:
        source = source + (lane // 64) * 64
    source = jnp.where(inside, source, 0)

    def body(i, carry):
        row = (above.e - reach + i) * above.rows + above.e - reach
        value = gather_lanes(e[0, pl.ds(row, rows), :], source)
        if above.ways == 1:
            other = gather_lanes(e[0, pl.ds(row + (lv.half // 2) * above.rows, rows), :], source)
            value = jnp.where(lane < 64, value, other)
        value = jnp.where(inside, value, 0.0)
        for plane in range(2):
            at = (lv.e - 2 * reach + 2 * i + plane) * r + lv.e - 2 * reach
            for odd in range(2):
                where = pl.ds(at + odd, rows, stride=2)
                x[0, where, :] = x[0, where, :] + value
        return carry

    loop(0, lv.half // 2 + 2 * reach, body, 0, 4)


def whole_operator(ny, fields, v, scale):
    rows = lax.broadcasted_iota(jnp.int32, (128, 128), 0)
    z, y = rows % 8, lanes(128) % 6
    last = 6 - scale
    y_low, y_high, z_low, z_high = y == 0, y == last, z == 0, z == last
    bottom, top = rows == 0, rows == 120 + last
    zero = jnp.zeros((128, 128), F32)

    def below_y(g):
        other = roll_lanes(v[g - 1], -last) if g else zero
        return jnp.where(y_low, other, roll_lanes(v[g], scale))

    fluxes_y = [fields(1, g) * (v[g] - below_y(g)) for g in range(ny)]
    out = []
    for g in range(ny):
        flux = fields(0, g) * (v[g] - roll_lanes(v[g], 6 * scale))
        total = flux - roll_lanes(flux, -6 * scale)
        other = roll_lanes(fluxes_y[g + 1], last) if g + 1 < ny else zero
        total = total + (fluxes_y[g] - jnp.where(y_high, other, roll_lanes(fluxes_y[g], -scale)))
        jump = 8 - last
        other = jnp.where(bottom, 0.0, roll_rows(v[g], jump))
        flux = fields(2, g) * (v[g] - jnp.where(z_low, other, roll_rows(v[g], scale)))
        other = jnp.where(top, 0.0, roll_rows(flux, -jump))
        total = total + (flux - jnp.where(z_high, other, roll_rows(flux, -scale)))
        out.append(fields(3, g) * v[g] + total)
    return out


def whole_inverse(ny, fields):
    rows = lax.broadcasted_iota(jnp.int32, (128, 128), 0)
    z, y = rows % 8, lanes(128) % 6
    zero = jnp.zeros((128, 128), F32)
    out = []
    for g in range(ny):
        face_x, face_y, face_z, cells = (fields(a, g) for a in range(4))
        total = cells + face_x + roll_lanes(face_x, -6)
        other = roll_lanes(fields(1, g + 1), 5) if g + 1 < ny else zero
        total = total + face_y + jnp.where(y == 5, other, roll_lanes(face_y, -1))
        other = jnp.where(rows == 125, 0.0, roll_rows(face_z, -3))
        total = total + face_z + jnp.where(z == 5, other, roll_rows(face_z, -1))
        out.append(jnp.where(cells > 0.0, 1.0 / total, 0.0))
    return out


def children(value, axes):
    if "y" in axes:
        value = value + roll_lanes(value, -1)
    if "x" in axes:
        value = value + roll_lanes(value, -6)
    if "z" in axes:
        value = value + roll_rows(value, -1)
    return value


def coarse_solve(ny, fields, f, inverse, bottom, xs, ds):
    def load(ref):
        return [ref[g] for g in range(ny)]

    def residual(v):
        applied = whole_operator(ny, fields, v, 1)
        return [f(g) - applied[g] for g in range(ny)]

    for g in range(ny):
        xs[g] = inverse[g] * f(g) * (1.0 / THETA)
        ds[g] = xs[g]
    for coefs in (STEP1, STEP2):
        remainder = residual(load(xs))
        for g in range(ny):
            update = coefs[0] * ds[g] + coefs[1] * (inverse[g] * remainder[g])
            ds[g] = update
            xs[g] = xs[g] + update
    remainder = residual(load(xs))
    inside = lambda g, value: jnp.where(bottom[3, g] > 0.0, value, 0.0)
    r = [inside(g, children(remainder[g], "xyz") * 0.125) for g in range(ny)]

    def total(values):
        values = functools.reduce(lambda a, b: a + b, values)
        return jnp.sum(jnp.sum(values, axis=0, keepdims=True), axis=1, keepdims=True)

    coarse = lambda a, g: bottom[a, g]
    e = [jnp.zeros((128, 128), F32)] * ny
    norm = total([a * a for a in r])

    def body(i, carry):
        e, r, p, norm = carry
        q = [inside(g, a) for g, a in enumerate(whole_operator(ny, coarse, p, 2))]
        size = norm / total([a * b for a, b in zip(p, q)])
        e = [a + size * b for a, b in zip(e, p)]
        r = [a - size * b for a, b in zip(r, q)]
        after = total([a * a for a in r])
        p = [a + after / norm * b for a, b in zip(r, p)]
        return e, r, p, after

    e, r, p, norm = lax.fori_loop(0, BOTTOM - 1, body, (e, r, r, norm))
    q = [inside(g, a) for g, a in enumerate(whole_operator(ny, coarse, p, 2))]
    size = norm / total([a * b for a, b in zip(p, q)])
    for g in range(ny):
        value = e[g] + size * p[g]
        value = value + roll_lanes(value, 1)
        value = value + roll_lanes(value, 6)
        xs[g] = xs[g] + (value + roll_rows(value, 1))
    for number, coefs in enumerate((None, STEP1, STEP2)):
        remainder = residual(load(xs))
        for g in range(ny):
            update = inverse[g] * remainder[g]
            if number == 0:
                update = update * (1.0 / THETA)
            else:
                update = coefs[0] * ds[g] + coefs[1] * update
            ds[g] = update
            xs[g] = xs[g] + update


def coarse_fields(ny, fields, bottom):
    rows = lax.broadcasted_iota(jnp.int32, (128, 128), 0)
    lane = lanes(128)
    even = (rows % 2 == 0) & (lane % 2 == 0) & ((lane // 6) % 2 == 0) & (lane < 72)
    for g in range(ny):
        for a, axes in enumerate(("yz", "xz", "xy", "xyz")):
            factor = 0.125 if a == 3 else 0.0625
            bottom[a, g] = jnp.where(even, children(fields(a, g), axes) * factor, 0.0)


def window(lv, gx, gy, gz, ny, xs, padded, turned, corner, x):
    nz = 16
    padded[...] = jnp.zeros_like(padded)
    for g in range(ny):
        padded[g + 1, pl.ds(1, nz)] = xs[g].reshape(nz, 8, 128)
    for dy in range(3):
        tiles = padded[gy + dy, pl.ds(gz, 3)].reshape(24, 128)
        tiles = jnp.concatenate([tiles, jnp.zeros((104, 128), F32)], axis=0)
        turned[dy, pl.ds(0, 24), :] = jnp.zeros((24, 128), F32)
        turned[dy, pl.ds(24, 128), :] = tiles.T
    lane = lanes(16)
    cell = lane - lv.zo + 6
    inside = (cell >= 0) & (cell < 24)
    coarse = jnp.where(inside, cell // 2 + 3, 0)
    source = (coarse // 6) * 8 + coarse % 6

    def body(i, carry):
        base = 6 + 36 * gx + 6 * i
        corner[pl.ds(0, 3), :] = turned[0, pl.ds(base + 3, 3), :]
        corner[pl.ds(3, 6), :] = turned[1, pl.ds(base, 6), :]
        corner[pl.ds(9, 3), :] = turned[2, pl.ds(base, 3), :]
        value = jnp.where(inside, gather_lanes(corner[...], source), 0.0)[0:12]
        for plane in range(2):
            at = (lv.e - 6 + 2 * i + plane) * lv.rows + lv.e - 6
            for odd in range(2):
                where = pl.ds(at + odd, 12, stride=2)
                x[0, where, :] = x[0, where, :] + value
        return carry

    loop(0, 12, body, 0, 4)


def hops(t, nz):
    return sum(min(d, 4 - d) for d in (t // nz % 4, t % nz // 4, t % 4))


def cycle(ny, nz, names, *refs):
    refs = list(refs)
    right_hbm, faces_hbm, cells_hbm, solution_hbm, residual_hbm, norm_out = refs[:6]
    s = dict(zip(names, refs[6:]))
    gx, gy, gz = lax.axis_index("gx"), lax.axis_index("gy"), lax.axis_index("gz")
    here = (gx, gy, gz, ny, nz)
    scope = jax.named_scope

    loads = [pltpu.make_async_copy(faces_hbm.at[d], s["land"].at[d], s["load_sem"].at[d]) for d in range(3)]
    loads.append(pltpu.make_async_copy(cells_hbm, s["land"].at[3], s["load_sem"].at[3]))
    loads.append(pltpu.make_async_copy(right_hbm, s["land"].at[4], s["load_sem"].at[4]))
    for copy in loads:
        copy.start()

    def other(t):
        return lax.rem(gy + t // nz, ny), lax.rem(gz + t % nz, nz)

    order = sorted(range(1, ny * nz), key=lambda t: -hops(t, nz))
    barrier = pltpu.get_barrier_semaphore()
    with scope("greet"):
        for t in order:
            oy, oz = other(t)
            pl.semaphore_signal(barrier, inc=1, device_id=(gx, oy, oz), device_id_type=MESH)
        pl.semaphore_signal(barrier, inc=1, device_id=(1 - gx, gy, gz), device_id_type=MESH)

    f0, f1, f2 = s["f0"], s["f1"], s["f2"]
    ex = {k: Exchange(*v) for k, v in EXCHANGES.items()}
    targets = {"e0": f0, "c1": f1, "c2": f2, "e1": f1, "e2": f2, "x0": s["x0a"], "x1": s["x1a"], "x2": s["x2a"]}
    for k, target in targets.items():
        ex[k].bind(here, target, [s[k + str(i)] for i in range(6)])

    def partner(src, dst, i):
        return pltpu.make_async_remote_copy(
            src_ref=src,
            dst_ref=dst,
            send_sem=s["pair_send"].at[i],
            recv_sem=s["pair_recv"].at[i],
            device_id=(1 - gx, gy, gz),
            device_id_type=MESH,
        )

    me = gy * nz + gz

    def spread(src, whole, part, i):
        def copy(src, dst, oy, oz):
            return pltpu.make_async_remote_copy(
                src_ref=src,
                dst_ref=dst,
                send_sem=s["all_send"].at[i],
                recv_sem=s["all_recv"].at[i],
                device_id=(gx, oy, oz),
                device_id_type=MESH,
            )

        def start():
            for t in order:
                copy(src, part(whole.at[me]), *other(t)).start()

        def finish():
            most = whole.at[pl.ds(0, ny * nz - 1)]
            most = most.at[:, pl.ds(0, 2)] if i == 0 else most
            copy(most, most, *other(1)).wait()

        return start, finish

    f1[...] = jnp.zeros_like(f1)
    f2[...] = jnp.zeros_like(f2)
    block = s["block"]
    block[...] = jnp.zeros_like(block)

    def block_put(field, plane, value):
        block[field, pl.ds(plane * 6, 6), :] = value

    for a in range(5):
        with scope("load_wait"):
            loads[a].wait()

        def load(i, carry, a=a):
            first = jnp.pad(s["land"][a, i], ((0, 0), (0, 80)))
            second = jnp.pad(s["land"][a, i + 24], ((0, 0), (0, 80)))
            value = roll_lanes(first, L0.zo) + roll_lanes(second, 64 + L0.zo)
            f0[a, pl.ds((L0.e + i) * L0.rows + L0.e, 48), :] = value
            return carry

        with scope("layout"):
            loop(0, 24, load, 0, 6)

    with scope("e0_pack"):
        ex["e0"].pack_yz(False)
    with scope("barrier"):
        pl.semaphore_wait(barrier, ny * nz)
    ex["e0"].send_yz()
    with scope("coarsen_0"):
        coarsen_fields(L0, L1, f0, fields_put(L1, f1))
    with scope("c1_start_yz"):
        ex["c1"].start_yz()
    with scope("coarsen_1"):
        coarsen_fields(L1, L2, f1, fields_put(L2, f2))
    with scope("c2_start_yz"):
        ex["c2"].start_yz()
    with scope("coarsen_2"):
        coarsen_fields(L2, None, f2, block_put)

    def tile_of(field):
        return roll_lanes(block[field].T[0:8], gx * 36)

    own4, pair4, own1, pair1, own_n, pair_n = (s[k] for k in ("own4", "pair4", "own1", "pair1", "own_n", "pair_n"))
    for field in range(4):
        own4[field] = tile_of(field)
    pair_coef = partner(own4, pair4, 0)
    pair_coef.start()

    def square(i, carry):
        value = f0[4, pl.ds((L0.e + i) * L0.rows + L0.e, 48), :]
        return carry + value * value

    with scope("square"):
        squares = loop(0, 24, square, jnp.zeros((48, 128), F32), 4)
    with scope("e0_finish_yz"):
        ex["e0"].finish_yz()
    ex["e0"].start_x()
    g4, g1, gn = s["g4"], s["g1"], s["gn"]
    with scope("pair_coef"):
        pair_coef.wait()
    merged = s["merged4"]
    merged[...] = own4[...] + pair4[...]
    mine = pl.ds(2 * gx, 2)
    g4[me, mine] = merged[mine]
    coef_start, coef_finish = spread(merged.at[mine], g4, lambda slot: slot.at[mine], 0)
    with scope("coef_start"):
        coef_start()
    with scope("e0_finish_x"):
        ex["e0"].finish_x()
    with scope("scaling_0"):
        scaling(L0, f0, s["i0"], s["u0"], 3)
    with scope("smooth_0"):
        smooth_from_zero(L0, f0, s["i0"], s["u0"], s["x0a"], s["x0b"], s["d0"], 3)
    with scope("restrict_0"):
        restrict(L0, L1, f0, s["u0"], s["x0a"], s["sums"], fields_put(L1, f1))
    with scope("e1_start_yz"):
        ex["e1"].start_yz()
    with scope("c1_finish_yz"):
        ex["c1"].finish_yz()
    ex["c1"].start_x()
    with scope("x0_start_yz"):
        ex["x0"].start_yz()
    with scope("c1_finish_x"):
        ex["c1"].finish_x()
    with scope("scaling_1"):
        scaling(L1, f1, s["i1"], s["u1"], 4)
    with scope("e1_finish_yz"):
        ex["e1"].finish_yz()
    ex["e1"].start_x()
    with scope("c2_finish_yz"):
        ex["c2"].finish_yz()
    with scope("e1_finish_x"):
        ex["e1"].finish_x()
    with scope("smooth_1"):
        smooth_from_zero(L1, f1, s["i1"], s["u1"], s["x1a"], s["x1b"], s["d1"], 3)
    with scope("restrict_1"):
        restrict(L1, L2, f1, s["u1"], s["x1a"], s["sums"], fields_put(L2, f2))
    with scope("e2_start_yz"):
        ex["e2"].start_yz()
    ex["c2"].start_x()
    with scope("x1_start_yz"):
        ex["x1"].start_yz()
    with scope("c2_finish_x"):
        ex["c2"].finish_x()
    with scope("scaling_2"):
        scaling(L2, f2, s["i2"], s["u2"], 5)
    with scope("coef_finish"):
        coef_finish()
    other_half = pltpu.make_async_remote_copy(
        src_ref=g4.at[:, mine],
        dst_ref=g4.at[:, mine],
        send_sem=s["pair_send"].at[3],
        recv_sem=s["pair_recv"].at[3],
        device_id=(1 - gx, gy, gz),
        device_id_type=MESH,
    )
    with scope("e2_finish_yz"):
        ex["e2"].finish_yz()
    ex["e2"].start_x()
    other_half.start()
    with scope("x0_finish_yz"):
        ex["x0"].finish_yz()
    with scope("e2_finish_x"):
        ex["e2"].finish_x()
    with scope("smooth_2"):
        smooth_from_zero(L2, f2, s["i2"], s["u2"], s["x2a"], s["x2b"], s["d2"], 3)
    with scope("restrict_2"):
        restrict(L2, None, f2, s["u2"], s["x2a"], s["sums"], block_put)
    own1[...] = tile_of(4)
    pair_source = partner(own1, pair1, 1)
    pair_source.start()
    ex["x0"].start_x()
    with scope("x2_start_yz"):
        ex["x2"].start_yz()
    with scope("pair_source"):
        pair_source.wait()
    s["merged1"][...] = own1[...] + pair1[...]
    g1[me] = s["merged1"][...]
    source_start, source_finish = spread(s["merged1"], g1, lambda slot: slot, 1)
    with scope("source_start"):
        source_start()
    with scope("other_half"):
        other_half.wait()
    gathered = lambda a, g: g4[pl.ds(g * nz, nz), a].reshape(128, 128)
    with scope("coarse_fields"):
        inverse = whole_inverse(ny, gathered)
        for g in range(ny):
            s["i3"][g] = inverse[g]
        coarse_fields(ny, gathered, s["bottom"])
    with scope("hidden"):
        ex["x1"].finish_yz()
        ex["x1"].start_x()
        ex["x0"].finish_x()
        ex["x2"].finish_yz()
        ex["x2"].start_x()
        ex["x1"].finish_x()
        ex["x2"].finish_x()
    with scope("source_finish"):
        source_finish()
    with scope("coarse_solve"):
        coarse_solve(ny, gathered, lambda g: g1[pl.ds(g * nz, nz)].reshape(128, 128), s["i3"], s["bottom"], s["x3"], s["d3"])
    with scope("window"):
        window(L2, gx, gy, gz, ny, s["x3"], s["padded"], s["turned"], s["corner"], s["x2a"])
    with scope("post_2"):
        smooth(L2, f2, s["i2"], s["u2"], s["x2a"], s["x2b"], s["d2"], 6)
    with scope("prolong_1"):
        prolong(L1, L2, s["x2b"], s["x1a"], 3)
    with scope("post_1"):
        smooth(L1, f1, s["i1"], s["u1"], s["x1a"], s["x1b"], s["d1"], 5)
    with scope("prolong_0"):
        prolong(L0, L1, s["x1b"], s["x0a"], 2)
    with scope("post_0"):
        smooth(L0, f0, s["i0"], s["u0"], s["x0a"], s["x0b"], s["d0"], 4)

    land = s["land"]
    r0 = L0.rows
    lane48 = lanes(48) % 64
    inside = (lane48 >= L0.zo) & (lane48 < L0.zo + 48)

    def final(p, row, here_x, applied, kept):
        s["sums"][0, pl.ds((p - L0.e) * r0, r0), :] = f0[4, pl.ds(row, r0), :] - applied
        return kept

    with scope("final"):
        sweep(L0, f0, s["u0"], s["x0b"], 0, final)

    def out_square(i, carry):
        value = jnp.where(inside, s["sums"][0, pl.ds(i * r0 + L0.e, 48), :], 0.0)
        return carry + value * value

    with scope("square"):
        ends = loop(0, 24, out_square, jnp.zeros((48, 128), F32), 4)

    def fold(value):
        return jnp.sum(value, axis=0, keepdims=True)

    own_n[...] = jnp.concatenate([fold(squares), fold(ends), jnp.zeros((6, 128), F32)], axis=0)
    pair_norm = partner(own_n, pair_n, 2)
    pair_norm.start()

    def unload(slot, i, value):
        for half in range(2):
            moved = roll_lanes(value, -(L0.zo + 64 * half))
            land[slot, i + 24 * half] = moved[:, 0:48]

    def out_solution(i, carry):
        unload(0, i, s["x0b"][0, pl.ds((L0.e + i) * r0 + L0.e, 48), :])
        return carry

    def out_residual(i, carry):
        unload(1, i, s["sums"][0, pl.ds(i * r0 + L0.e, 48), :])
        return carry

    with scope("unload_solution"):
        loop(0, 24, out_solution, 0, 6)
    out0 = pltpu.make_async_copy(land.at[0], solution_hbm, s["out_sem"].at[0])
    out0.start()
    with scope("pair_norm"):
        pair_norm.wait()
    s["merged_n"][...] = jnp.where(gx == 0, own_n[...] + pair_n[...], pair_n[...] + own_n[...])
    gn[me] = s["merged_n"][...]
    norm_start, norm_finish = spread(s["merged_n"], gn, lambda slot: slot, 2)
    with scope("norm_start"):
        norm_start()
    with scope("unload_residual"):
        loop(0, 24, out_residual, 0, 6)
    out1 = pltpu.make_async_copy(land.at[1], residual_hbm, s["out_sem"].at[1])
    out1.start()
    with scope("norm_finish"):
        norm_finish()
    all_n = jnp.sum(gn[...], axis=0)
    sums = jnp.sum(all_n, axis=1, keepdims=True)
    norm = jnp.sqrt(sums[1:2] / sums[0:1])
    norm_out[0, 0] = norm[0, 0]
    with scope("out_wait"):
        out0.wait()
        out1.wait()


EXCHANGES = {
    "e0": (L0, 0, 5),
    "c1": (L1, 0, 4),
    "c2": (L2, 0, 4),
    "e1": (L1, 4, 1),
    "e2": (L2, 4, 1),
    "x0": (L0, 0, 1),
    "x1": (L1, 0, 1),
    "x2": (L2, 0, 1),
}


def scratch_of(ny, nz):
    vmem = lambda *shape: pltpu.VMEM(shape, F32)
    size = lambda lv: lv.planes * lv.rows
    scratch = {"land": vmem(5, 48, 48, 48), "load_sem": pltpu.SemaphoreType.DMA((5,)), "out_sem": pltpu.SemaphoreType.DMA((2,))}
    for i, lv in enumerate((L0, L1, L2)):
        scratch[f"f{i}"] = vmem(5, size(lv), 128)
        for k in ("i", "d", "u"):
            scratch[f"{k}{i}"] = vmem(1, size(lv), 128)
        scratch[f"x{i}a"] = vmem(1, size(lv), 128)
        scratch[f"x{i}b"] = vmem(1, size(lv), 128)
    scratch["sums"] = vmem(1, 24 * 56, 128)
    scratch["block"] = vmem(5, 128, 128)
    for k in ("own4", "pair4", "merged4"):
        scratch[k] = vmem(4, 8, 128)
    for k in ("own1", "pair1", "merged1", "own_n", "pair_n", "merged_n"):
        scratch[k] = vmem(8, 128)
    scratch["g4"] = vmem(ny * nz, 4, 8, 128)
    scratch["g1"] = vmem(ny * nz, 8, 128)
    scratch["gn"] = vmem(ny * nz, 8, 128)
    for k in ("pair_send", "pair_recv"):
        scratch[k] = pltpu.SemaphoreType.DMA((4,))
    for k in ("all_send", "all_recv"):
        scratch[k] = pltpu.SemaphoreType.DMA((3,))
    for k in ("i3", "x3", "d3"):
        scratch[k] = vmem(ny, 128, 128)
    scratch["bottom"] = vmem(4, ny, 128, 128)
    scratch["padded"] = vmem(ny + 2, nz + 2, 8, 128)
    scratch["turned"] = vmem(3, 152, 128)
    scratch["corner"] = vmem(16, 128)
    for k, v in EXCHANGES.items():
        for i, shape in enumerate(Exchange(*v).scratch()):
            scratch[k + str(i)] = shape
    return scratch


def solution(mesh):
    ny, nz = mesh.shape["gy"], mesh.shape["gz"]
    scratch = scratch_of(ny, nz)

    def shards(right_side, face_coef, absorption):
        field = jax.ShapeDtypeStruct((48, 48, 48), F32)
        solved, residual, norm = pl.pallas_call(
            functools.partial(cycle, ny, nz, tuple(scratch)),
            out_shape=(field, field, jax.ShapeDtypeStruct((1, 1), F32)),
            in_specs=[pl.BlockSpec(memory_space=pl.ANY)] * 3,
            out_specs=(
                pl.BlockSpec(memory_space=pl.ANY),
                pl.BlockSpec(memory_space=pl.ANY),
                pl.BlockSpec(memory_space=pltpu.SMEM),
            ),
            scratch_shapes=list(scratch.values()),
            compiler_params=pltpu.CompilerParams(
                collective_id=0, has_side_effects=True, vmem_limit_bytes=62 * 1024 * 1024
            ),
        )(right_side, face_coef, absorption)
        return solved, residual, norm[0, 0]

    in_specs = (P("gx", "gy", "gz"), P(None, "gx", "gy", "gz"), P("gx", "gy", "gz"))
    out_specs = (P("gx", "gy", "gz"), P("gx", "gy", "gz"), P())
    return jax.shard_map(shards, mesh=mesh, in_specs=in_specs, out_specs=out_specs, check_vma=False)
```

```python
import functools

import jax
import jax.numpy as jnp
from jax import lax
from jax.experimental import pallas as pl
from jax.experimental.pallas import tpu as pltpu
from jax.sharding import PartitionSpec as P

BOTTOM = 6
THETA = 1.125
DELTA = 0.875
SIGMA = THETA / DELTA
RHO0 = 1.0 / SIGMA
RHO1 = 1.0 / (2.0 * SIGMA - RHO0)
RHO2 = 1.0 / (2.0 * SIGMA - RHO1)
STEP1 = (RHO1 * RHO0, 2.0 * RHO1 / DELTA)
STEP2 = (RHO2 * RHO1, 2.0 * RHO2 / DELTA)

F32 = jnp.float32
MESH = pl.DeviceIdType.MESH


class Level:
    def __init__(self, n, e, ways, rows, zo, width, width_y, unroll):
        self.n, self.e, self.ways, self.rows, self.zo, self.width = n, e, ways, rows, zo, width
        self.width_y, self.unroll = width_y, unroll
        self.half = n // ways
        self.planes = self.half + 2 * e
        self.span = 128 // ways
        self.slots, self.slots_y = self.span // width, self.span // width_y
        self.packs, self.packs_y = -(-self.half // self.slots), -(-self.half // self.slots_y)


L0 = Level(48, 4, 2, 56, 8, 4, 64, 4)
L1 = Level(24, 6, 2, 40, 16, 8, 32, 4)
L2 = Level(12, 6, 1, 24, 16, 8, 16, 6)


def lanes(rows):
    return lax.broadcasted_iota(jnp.int32, (rows, 128), 1)


def gather_lanes(value, index):
    return jnp.take_along_axis(value, index, axis=1)


def roll_lanes(value, shift):
    return pltpu.roll(value, shift % 128, 1)


def roll_rows(value, shift):
    return pltpu.roll(value, shift % value.shape[0], 0)


def tile_rows(start, size):
    return pl.ds(pl.multiple_of(start, 8), size)


def loop(lo, hi, body, carry, unroll):
    count = (hi - lo) // unroll

    def chunk(i, carry):
        for k in range(unroll):
            carry = body(lo + i * unroll + k, carry)
        return carry

    carry = lax.fori_loop(0, count, chunk, carry)
    for k in range(lo + count * unroll, hi):
        carry = body(k, carry)
    return carry


class Exchange:
    def __init__(self, level, first, count):
        self.level, self.first, self.count = level, first, count
        lv = level
        sizes = [-(-rows // 8) * 8 for rows in (lv.packs_y * lv.e, lv.packs * lv.n, lv.packs * lv.e)]
        self.sizes = [sizes[0]] * 2 + [sizes[1]] * 2 + [sizes[2]] * 4
        self.starts = [sum(self.sizes[:i]) for i in range(9)]

    def scratch(self):
        lv, na = self.level, self.count
        shapes = [
            (na, lv.e * lv.rows, 128),
            (na, self.starts[8], 128),
            (na, self.starts[8], 128),
            (na, self.starts[8], 128),
            (2, na, lv.packs * lv.rows, 128),
        ]
        return [pltpu.VMEM(s, F32) for s in shapes] + [pltpu.SemaphoreType.DMA((2,)), pltpu.SemaphoreType.DMA((2,))]

    def bind(self, here, ref, scratch):
        self.here, self.ref = here, ref
        self.xr, self.out, self.got, self.spare, self.zf, self.ssem, self.rsem = scratch
        gx, gy, gz, ny, nz = here
        lv = self.level
        start = lv.e + (1 - gx) * (lv.half - lv.e if lv.ways == 2 else lv.n - lv.e)

        def copy(src, dst, i, gx, gy, gz):
            return pltpu.make_async_remote_copy(
                src_ref=src,
                dst_ref=dst,
                send_sem=self.ssem.at[i],
                recv_sem=self.rsem.at[i],
                device_id=(gx, gy, gz),
                device_id_type=MESH,
            )

        src = ref.at[pl.ds(self.first, self.count), tile_rows(start * lv.rows, lv.e * lv.rows), :]
        self.copy_x = copy(src, self.xr, 0, 1 - gx, gy, gz)
        ys = [lax.rem(gy + ny - 1, ny), lax.rem(gy + 1, ny)]
        zs = [lax.rem(gz + nz - 1, nz), lax.rem(gz + 1, nz)]
        targets = [(ys[0], gz), (ys[1], gz), (gy, zs[0]), (gy, zs[1])] + [(y, z) for y in ys for z in zs]
        lands = [1, 0, 3, 2, 7, 6, 5, 4]
        self.copies = [
            copy(
                self.out.at[:, pl.ds(self.starts[i], self.sizes[i]), :],
                self.got.at[:, pl.ds(self.starts[lands[i]], self.sizes[i]), :],
                1,
                gx,
                *targets[i],
            )
            for i in range(8)
        ]
        y_side, z_side = [gy > 0, gy < ny - 1], [gz > 0, gz < nz - 1]
        self.exists = y_side + z_side + [a & b for a in y_side for b in z_side]
        self.all = copy(self.out, self.got, 1, gx, *targets[0])
        self.has_y = [jnp.where(gy > 0, 1.0, 0.0).astype(F32), jnp.where(gy < ny - 1, 1.0, 0.0).astype(F32)]
        self.has_z = [jnp.where(gz > 0, 1.0, 0.0).astype(F32), jnp.where(gz < nz - 1, 1.0, 0.0).astype(F32)]
        self.has_x = [gx.astype(F32), (1 - gx).astype(F32)]
        return self

    def send(self, i):
        part = (slice(None), pl.ds(self.starts[i], self.sizes[i]), slice(None))

        @pl.when(self.exists[i])
        def _():
            self.copies[i].start()

        @pl.when(jnp.logical_not(self.exists[i]))
        def _():
            pltpu.make_async_copy(self.out.at[part], self.got.at[part], self.rsem.at[1]).start()
            pltpu.make_async_copy(self.out.at[part], self.spare.at[part], self.ssem.at[1]).start()

    def start_x(self):
        self.copy_x.start()

    def finish_x(self):
        lv, ref = self.level, self.ref
        e, r = lv.e, lv.rows
        self.copy_x.wait()
        low = lanes(r) < 64

        def finish(a, j):
            got = self.xr[a, tile_rows(j * r, r), :]
            if lv.ways == 2:
                got = roll_lanes(got, 64)
                below = roll_lanes(ref[self.first + a, tile_rows((lv.half + j) * r, r), :], 64)
                above = roll_lanes(ref[self.first + a, tile_rows((e + j) * r, r), :], 64)
                below = jnp.where(low, got * self.has_x[0], below)
                above = jnp.where(low, above, got * self.has_x[1])
            else:
                below = got * self.has_x[0]
                above = got * self.has_x[1]
            return below, above

        def body(a, carry):
            for first in range(0, e, 2):
                planes = range(first, min(first + 2, e))
                values = [finish(a, j) for j in planes]
                for j, (below, above) in zip(planes, values):
                    ref[self.first + a, tile_rows(j * r, r), :] = below
                    ref[self.first + a, tile_rows((e + lv.half + j) * r, r), :] = above
            return carry

        lax.fori_loop(0, self.count, body, 0)

    def pack(self, plane, rows, width, shifts, put):
        lv = self.level
        slot = (lanes(rows) % lv.span) // width
        slots = lv.span // width
        for k in range(-(-lv.half // slots)):
            acc = None
            for s in range(min(slots, lv.half - k * slots)):
                moved = [roll_lanes(v, s * width - shift) for v, shift in zip(plane(lv.e + k * slots + s), shifts)]
                acc = moved if s == 0 else [jnp.where(slot == s, new, old) for new, old in zip(moved, acc)]
            put(k, acc)

    def pack_yz(self, send):
        lv, ref = self.level, self.ref
        r, n, e, zo = lv.rows, lv.n, lv.e, lv.zo
        z_shifts = (zo, zo + n - e)

        def put_at(first, rows, a):
            def put(k, values):
                for i, value in enumerate(values):
                    self.out[a, pl.ds(self.starts[first + i] + k * rows, rows), :] = value

            return put

        def edges(a, p):
            return [ref[self.first + a, pl.ds(p * r + row, e), :] for row in (e, n)]

        def pack_d(a, carry):
            def plane(p):
                low, high = edges(a, p)
                return low, low, high, high

            self.pack(plane, e, lv.width, z_shifts * 2, put_at(4, e, a))
            return carry

        def pack_z(a, carry):
            def plane(p):
                return [ref[self.first + a, pl.ds(p * r + e, n), :]] * 2

            self.pack(plane, n, lv.width, z_shifts, put_at(2, n, a))
            return carry

        def pack_y(a, carry):
            if lv.slots_y == 1:
                for k in range(lv.half):
                    put_at(0, e, a)(k, edges(a, e + k))
            else:
                self.pack(lambda p: edges(a, p), e, lv.width_y, (zo, zo), put_at(0, e, a))
            return carry

        for body, which in ((pack_d, range(4, 8)), (pack_z, (2, 3)), (pack_y, (0, 1))):
            lax.fori_loop(0, self.count, body, 0)
            if send:
                for i in which:
                    self.send(i)

    def send_yz(self):
        for i in (4, 5, 6, 7, 2, 3, 0, 1):
            self.send(i)

    def start_yz(self):
        self.pack_yz(True)

    def finish_yz(self):
        lv, ref = self.level, self.ref
        r, n, e, zo = lv.rows, lv.n, lv.e, lv.zo
        with jax.named_scope("arrive"):
            self.all.wait()
        lane = lanes(r) % lv.span
        at_low = (lane >= zo - e) & (lane < zo)
        at_high = (lane >= zo + n) & (lane < zo + n + e)

        def unpack(a, carry):
            def got(i, row, rows):
                return self.got[a, pl.ds(self.starts[i] + row, rows), :]

            for s in range(2):
                for k in range(lv.packs_y):
                    value = got(s, k * e, e) * self.has_y[s]
                    for slot in range(min(lv.slots_y, lv.half - k * lv.slots_y)):
                        row = (e + k * lv.slots_y + slot) * r + (e + n) * s
                        moved = roll_lanes(value, zo - slot * lv.width_y) if lv.slots_y > 1 else value
                        ref[self.first + a, pl.ds(row, e), :] = moved
            for k in range(lv.packs):
                for t in range(2):
                    self.zf[t, a, pl.ds(k * r + e, n), :] = got(2 + t, k * n, n) * self.has_z[t]
                    for s in range(2):
                        both = self.has_y[s] * self.has_z[t]
                        self.zf[t, a, pl.ds(k * r + (e + n) * s, e), :] = got(4 + 2 * s + t, k * e, e) * both
            for k in range(lv.packs):
                sides = [self.zf[t, a, pl.ds(k * r, r), :] for t in range(2)]
                count = min(lv.slots, lv.half - k * lv.slots)
                for first in range(0, count, 4):
                    slots = range(first, min(first + 4, count))
                    values = []
                    for s in slots:
                        value = ref[self.first + a, pl.ds((e + k * lv.slots + s) * r, r), :]
                        value = jnp.where(at_low, roll_lanes(sides[0], zo - e - s * lv.width), value)
                        values.append(jnp.where(at_high, roll_lanes(sides[1], zo + n - s * lv.width), value))
                    for s, value in zip(slots, values):
                        ref[self.first + a, pl.ds((e + k * lv.slots + s) * r, r), :] = value
            return carry

        lax.fori_loop(0, self.count, unpack, 0)


def scaling(lv, fields, inverse, upper, extent):
    r = lv.rows

    def body(p, carry):
        row = pl.multiple_of(p * r, 8)
        cells = fields[3, pl.ds(row, r), :]
        face_z = fields[2, pl.ds(row, r), :]
        total = cells + fields[0, pl.ds(row, r), :] + fields[0, pl.ds(row + r, r), :]
        total = total + fields[1, pl.ds(row, r), :] + fields[1, pl.ds(row + 1, r), :]
        above = roll_lanes(face_z, -1)
        upper[0, pl.ds(row, r), :] = above
        total = total + face_z + above
        inverse[0, pl.ds(row, r), :] = jnp.where(cells > 0.0, 1.0 / total, 0.0)
        return carry

    loop(lv.e - extent, lv.e + lv.half + extent, body, 0, lv.unroll)


def sweep(lv, fields, upper, x, extent, emit, carry=0):
    r = lv.rows
    lo, hi = lv.e - extent, lv.e + lv.half + extent

    def body(p, carry):
        here, flux, kept = carry
        row = pl.multiple_of(p * r, 8)
        after = x[0, pl.ds(row + r, r), :]
        flux_after = fields[0, pl.ds(row + r, r), :] * (after - here)
        low_y = x[0, pl.ds(row - 1, r), :]
        high_y = x[0, pl.ds(row + 1, r), :]
        flux_y = fields[1, pl.ds(row, r), :] * (here - low_y)
        flux_y = flux_y - fields[1, pl.ds(row + 1, r), :] * (high_y - here)
        flux_z = fields[2, pl.ds(row, r), :] * (here - roll_lanes(here, 1))
        flux_z = flux_z - upper[0, pl.ds(row, r), :] * (roll_lanes(here, -1) - here)
        applied = fields[3, pl.ds(row, r), :] * here + ((flux - flux_after) + flux_y + flux_z)
        return after, flux_after, emit(p, row, here, applied, kept)

    row = lo * r
    here = x[0, pl.ds(row, r), :]
    flux = fields[0, pl.ds(row, r), :] * (here - x[0, pl.ds(row - r, r), :])
    return loop(lo, hi, body, (here, flux, carry), lv.unroll)[2]


def step(lv, fields, inverse, upper, x, out, d, extent, first, coefs, keep):
    r = lv.rows

    def emit(p, row, here, applied, kept):
        scaled = inverse[0, pl.ds(row, r), :] * (fields[4, pl.ds(row, r), :] - applied)
        if first == 0:
            update = scaled * (1.0 / THETA)
        elif first == 1:
            update = coefs[0] * here + coefs[1] * scaled
        else:
            update = coefs[0] * d[0, pl.ds(row, r), :] + coefs[1] * scaled
        if keep:
            d[0, pl.ds(row, r), :] = update
        out[0, pl.ds(row, r), :] = here + update
        return kept

    sweep(lv, fields, upper, x, extent, emit)


def smooth_from_zero(lv, fields, inverse, upper, xa, xb, d, extent):
    r = lv.rows

    def body(p, carry):
        row = pl.multiple_of(p * r, 8)
        xa[0, pl.ds(row, r), :] = inverse[0, pl.ds(row, r), :] * fields[4, pl.ds(row, r), :] * (1.0 / THETA)
        return carry

    loop(lv.e - extent, lv.e + lv.half + extent, body, 0, lv.unroll)
    step(lv, fields, inverse, upper, xa, xb, d, extent - 1, 1, STEP1, True)
    step(lv, fields, inverse, upper, xb, xa, d, extent - 2, 2, STEP2, False)


def smooth(lv, fields, inverse, upper, xa, xb, d, extent):
    step(lv, fields, inverse, upper, xa, xb, d, extent - 1, 0, None, True)
    step(lv, fields, inverse, upper, xb, xa, d, extent - 2, 2, STEP1, True)
    step(lv, fields, inverse, upper, xa, xb, d, extent - 3, 2, STEP2, False)


def coarse_lanes(lv, below, rows, half):
    lane = lanes(rows)
    if below is None:
        cell, at = lane, 0
    else:
        at = (lane // below.span) * 64 if below.ways == 2 else 0
        cell = lane % below.span - below.zo
    if lv.ways == 2 and half is not None:
        at = 64 * half
    inside = (cell >= 0) & (cell < lv.n // 2)
    index = jnp.where(inside, at + lv.zo + 2 * cell, 0)
    return index, inside


def place(lv, below, put, plane, value, pair):
    rows = value.shape[0]
    if pair:
        value = value + roll_lanes(value, -1)
    halves = [None] if below is not None and below.ways == lv.ways else range(lv.ways)
    for half in halves:
        index, inside = coarse_lanes(lv, below, rows, half)
        got = jnp.where(inside, gather_lanes(value, index), 0.0)
        put(plane if half is None else plane + half * (lv.half // 2), got)


def coarsen_fields(lv, below, fields, put):
    n2, e, r = lv.n // 2, lv.e, lv.rows

    def body(i, carry):
        row = (e + 2 * i) * r + e

        def rows(a, plane, odd):
            return fields[a, pl.ds(row + plane * r + odd, n2, stride=2), :]

        put_x = functools.partial(put, 0)
        put_y = functools.partial(put, 1)
        put_z = functools.partial(put, 2)
        put_c = functools.partial(put, 3)
        place(lv, below, put_x, i, (rows(0, 0, 0) + rows(0, 0, 1)) * 0.0625, True)
        place(lv, below, put_y, i, (rows(1, 0, 0) + rows(1, 1, 0)) * 0.0625, True)
        place(lv, below, put_z, i, (rows(2, 0, 0) + rows(2, 0, 1) + rows(2, 1, 0) + rows(2, 1, 1)) * 0.0625, False)
        place(lv, below, put_c, i, (rows(3, 0, 0) + rows(3, 0, 1) + rows(3, 1, 0) + rows(3, 1, 1)) * 0.125, True)
        return carry

    loop(0, lv.half // 2, body, 0, 3)


def restrict(lv, below, fields, upper, x, sums, put):
    r, n2 = lv.rows, lv.n // 2

    def emit(p, row, here, applied, kept):
        sums[0, pl.ds((p - lv.e) * r, r), :] = fields[4, pl.ds(row, r), :] - applied
        return kept

    sweep(lv, fields, upper, x, 0, emit)

    def body(i, carry):
        total = None
        for plane in range(2):
            for odd in range(2):
                part = sums[0, pl.ds((2 * i + plane) * r + lv.e + odd, n2, stride=2), :]
                total = part if total is None else total + part
        place(lv, below, functools.partial(put, 4), i, total * 0.125, True)
        return carry

    loop(0, lv.half // 2, body, 0, 6)


def fields_put(below, fields):
    def put(field, plane, value):
        fields[field, pl.ds((below.e + plane) * below.rows + below.e, below.n), :] = value

    return put


def prolong(lv, above, e, x, reach):
    r, rows = lv.rows, lv.n // 2 + 2 * reach
    lane = lanes(rows)
    cell = lane % 64 - lv.zo + 2 * reach
    inside = (cell >= 0) & (cell < 2 * rows)
    source = above.zo - reach + cell // 2
    if above.ways == 2:
        source = source + (lane // 64) * 64
    source = jnp.where(inside, source, 0)

    def body(i, carry):
        row = (above.e - reach + i) * above.rows + above.e - reach
        value = gather_lanes(e[0, pl.ds(row, rows), :], source)
        if above.ways == 1:
            other = gather_lanes(e[0, pl.ds(row + (lv.half // 2) * above.rows, rows), :], source)
            value = jnp.where(lane < 64, value, other)
        value = jnp.where(inside, value, 0.0)
        for plane in range(2):
            at = (lv.e - 2 * reach + 2 * i + plane) * r + lv.e - 2 * reach
            for odd in range(2):
                where = pl.ds(at + odd, rows, stride=2)
                x[0, where, :] = x[0, where, :] + value
        return carry

    loop(0, lv.half // 2 + 2 * reach, body, 0, 4)


PAD = 8


def row_of(rows):
    return lax.broadcasted_iota(jnp.int32, (rows, 128), 0)


def whole_neighbours(ny, value, rows):
    z, y = row_of(128) % 8, lanes(128) % 6
    out = []
    for g in range(ny):
        here = value(g)
        low_y, high_y = roll_lanes(here, 1), roll_lanes(here, -1)
        if g:
            low_y = jnp.where(y == 0, roll_lanes(value(g - 1), -5), low_y)
        if g + 1 < ny:
            high_y = jnp.where(y == 5, roll_lanes(value(g + 1), 5), high_y)
        low_z = jnp.where(z == 0, rows(g, -3), rows(g, -1))
        high_z = jnp.where(z == 5, rows(g, 3), rows(g, 1))
        out.append((roll_lanes(here, 6), roll_lanes(here, -6), low_y, high_y, low_z, high_z))
    return out


def whole_prepare(ny, fields, coefs, diagonal, inverse):
    z, y, row = row_of(128) % 8, lanes(128) % 6, row_of(128)
    moved = lambda a: whole_neighbours(ny, lambda g: fields(a, g), lambda g, d: roll_rows(fields(a, g), -d))
    high = [[near[1] for near in moved(0)], [near[3] for near in moved(1)], [near[5] for near in moved(2)]]
    for g in range(ny):
        inside = fields(3, g) > 0.0
        high_y = jnp.where(y == 5, 0.0, high[1][g]) if g + 1 == ny else high[1][g]
        high_z = jnp.where(row == 125, 0.0, high[2][g])
        sides = [fields(0, g), high[0][g], fields(1, g), high_y, fields(2, g), high_z]
        total = functools.reduce(lambda a, b: a + b, sides) + fields(3, g)
        scale = jnp.where(inside, 1.0 / total, 0.0)
        diagonal[g] = jnp.where(inside, total, 0.0)
        inverse[g] = scale
        if g == 0:
            sides[2] = jnp.where(y == 0, 0.0, sides[2])
        sides[4] = jnp.where(row == 0, 0.0, sides[4])
        for i in range(6):
            coefs[i, g] = sides[i] * scale


def children(value, axes):
    if "y" in axes:
        value = value + roll_lanes(value, -1)
    if "x" in axes:
        value = value + roll_lanes(value, -6)
    if "z" in axes:
        value = value + roll_rows(value, -1)
    return value


def even_cells():
    row, lane = row_of(128), lanes(128)
    return (row % 2 == 0) & (row % 8 < 6) & (lane % 2 == 0) & ((lane // 6) % 2 == 0) & (lane < 72)


def fold_level(values):
    even = even_cells()
    values = [jnp.where(even, v, 0.0) for v in values]
    both = (values[0] + roll_lanes(values[1], 1)) + (roll_lanes(values[2], 6) + roll_lanes(values[3], 7))
    return both[0:64] + roll_rows(both[64:128], 1)


def unfold_level(value):
    both = jnp.concatenate([value, roll_rows(value, -1)], axis=0)
    even = even_cells()
    return [jnp.where(even, roll_lanes(both, -shift), 0.0) for shift in (0, 1, 6, 7)]


def bottom_neighbours(v):
    row, lane = row_of(64), lanes(64)
    z, y = (row % 8) // 2, (lane % 6) // 2
    odd = lane % 2 == 1
    low_y = jnp.where(y > 0, roll_lanes(v, 2), jnp.where(odd, roll_lanes(v, -3), roll_lanes(v, 1)))
    high_y = jnp.where(y < 2, roll_lanes(v, -2), jnp.where(odd, roll_lanes(v, -1), roll_lanes(v, 3)))
    low_z = jnp.where(z > 0, roll_rows(v, 2), jnp.where(row == 1, roll_rows(v, 5), roll_rows(v, 4)))
    high_z = jnp.where(z < 2, roll_rows(v, -2), jnp.where(row == 60, roll_rows(v, -5), roll_rows(v, -4)))
    return roll_lanes(v, 12), roll_lanes(v, -12), low_y, high_y, low_z, high_z


def bottom_prepare(ny, fields, bottom):
    row, lane = row_of(64), lanes(64)
    y = (lane % 6) // 2
    first = (lane % 2 == 0) & ((lane // 6) % 2 == 0)
    last = (lane % 2 == 1) & ((lane // 6) % 2 == 1)
    faces = []
    for a, axes in enumerate(("yz", "xz", "xy", "xyz")):
        factor = 0.125 if a == 3 else 0.0625
        faces.append(fold_level([children(fields(a, g), axes) * factor for g in range(ny)]))
    inside = faces[3] > 0.0
    high_x = bottom_neighbours(faces[0])[1]
    high_y = jnp.where(last & (y == 2), 0.0, bottom_neighbours(faces[1])[3])
    high_z = jnp.where(row == 61, 0.0, bottom_neighbours(faces[2])[5])
    sides = [faces[0], high_x, faces[1], high_y, faces[2], high_z]
    total = functools.reduce(lambda a, b: a + b, sides) + faces[3]
    sides[2] = jnp.where(first & (y == 0), 0.0, sides[2])
    sides[4] = jnp.where(row == 0, 0.0, sides[4])
    for i, value in enumerate(sides + [total]):
        bottom[i] = jnp.where(inside, value, 0.0)


def coarse_solve(ny, coefs, diagonal, inverse, f, bottom, xa, xb, ds, g3):
    def rows(x, g, offset=0):
        return x[g, pl.ds(PAD + offset, 128)]

    def scaled(x):
        near = whole_neighbours(ny, lambda g: rows(x, g), lambda g, d: rows(x, g, d))
        out = []
        for g in range(ny):
            parts = [coefs[i, g] * near[g][i] for i in range(6)]
            total = ((parts[0] + parts[1]) + (parts[2] + parts[3])) + (parts[4] + parts[5])
            out.append((g3[g] - rows(x, g)) + total)
        return out

    def advance(x, to, coef, first, keep=True):
        for g, value in enumerate(scaled(x)):
            update = value * (1.0 / THETA) if first else coef[0] * ds[g] + coef[1] * value
            if keep:
                ds[g] = update
            to[g, pl.ds(PAD, 128)] = rows(x, g) + update

    for x in (xa, xb):
        for g in range(ny):
            x[g, pl.ds(0, PAD)] = jnp.zeros((PAD, 128), F32)
            x[g, pl.ds(PAD + 128, PAD)] = jnp.zeros((PAD, 128), F32)
    for g in range(ny):
        g3[g] = inverse[g] * f(g)
        ds[g] = g3[g] * (1.0 / THETA)
        xa[g, pl.ds(PAD, 128)] = ds[g]
    advance(xa, xb, STEP1, False)
    advance(xb, xa, STEP2, False, False)
    remainder = scaled(xa)
    r = fold_level([children(remainder[g] * diagonal[g], "xyz") * 0.125 for g in range(ny)])
    r = jnp.where(bottom[6] > 0.0, r, 0.0)

    def total(value):
        value = jnp.sum(value.reshape(8, 8, 128), axis=0)
        return jnp.sum(jnp.sum(value, axis=1, keepdims=True), axis=0, keepdims=True)

    def applied(v):
        near = bottom_neighbours(v)
        parts = [bottom[i] * near[i] for i in range(6)]
        return bottom[6] * v - (((parts[0] + parts[1]) + (parts[2] + parts[3])) + (parts[4] + parts[5]))

    e = jnp.zeros((64, 128), F32)
    p, norm = r, total(r * r)
    for i in range(BOTTOM):
        q = applied(p)
        size = norm / total(p * q)
        e = e + size * p
        if i + 1 < BOTTOM:
            r = r - size * q
            after = total(r * r)
            p = r + after / norm * p
            norm = after
    for g, value in enumerate(unfold_level(e)):
        value = value + roll_lanes(value, 1)
        value = value + roll_lanes(value, 6)
        xa[g, pl.ds(PAD, 128)] = rows(xa, g) + (value + roll_rows(value, 1))
    advance(xa, xb, None, True)
    advance(xb, xa, STEP1, False)
    advance(xa, xb, STEP2, False, False)


def window(lv, gx, gy, gz, ny, xs, padded, turned, corner, x):
    nz = 16
    padded[...] = jnp.zeros_like(padded)
    for g in range(ny):
        padded[g + 1, pl.ds(1, nz)] = xs[g, pl.ds(PAD, 128)].reshape(nz, 8, 128)
    for dy in range(3):
        tiles = padded[gy + dy, pl.ds(gz, 3)].reshape(24, 128)
        tiles = jnp.concatenate([tiles, jnp.zeros((104, 128), F32)], axis=0)
        turned[dy, pl.ds(0, 24), :] = jnp.zeros((24, 128), F32)
        turned[dy, pl.ds(24, 128), :] = tiles.T
    lane = lanes(16)
    cell = lane - lv.zo + 6
    inside = (cell >= 0) & (cell < 24)
    coarse = jnp.where(inside, cell // 2 + 3, 0)
    source = (coarse // 6) * 8 + coarse % 6

    def body(i, carry):
        base = 6 + 36 * gx + 6 * i
        corner[pl.ds(0, 3), :] = turned[0, pl.ds(base + 3, 3), :]
        corner[pl.ds(3, 6), :] = turned[1, pl.ds(base, 6), :]
        corner[pl.ds(9, 3), :] = turned[2, pl.ds(base, 3), :]
        value = jnp.where(inside, gather_lanes(corner[...], source), 0.0)[0:12]
        for plane in range(2):
            at = (lv.e - 6 + 2 * i + plane) * lv.rows + lv.e - 6
            for odd in range(2):
                where = pl.ds(at + odd, 12, stride=2)
                x[0, where, :] = x[0, where, :] + value
        return carry

    loop(0, 12, body, 0, 4)


def hops(t, nz):
    return sum(min(d, 4 - d) for d in (t // nz % 4, t % nz // 4, t % 4))


def cycle(ny, nz, names, *refs):
    refs = list(refs)
    right_hbm, faces_hbm, cells_hbm, solution_hbm, residual_hbm, norm_out = refs[:6]
    s = dict(zip(names, refs[6:]))
    gx, gy, gz = lax.axis_index("gx"), lax.axis_index("gy"), lax.axis_index("gz")
    here = (gx, gy, gz, ny, nz)
    scope = jax.named_scope

    loads = [pltpu.make_async_copy(faces_hbm.at[d], s["land"].at[d], s["load_sem"].at[d]) for d in range(3)]
    loads.append(pltpu.make_async_copy(cells_hbm, s["land"].at[3], s["load_sem"].at[3]))
    loads.append(pltpu.make_async_copy(right_hbm, s["land"].at[4], s["load_sem"].at[4]))
    for copy in loads:
        copy.start()

    def other(t):
        return lax.rem(gy + t // nz, ny), lax.rem(gz + t % nz, nz)

    order = sorted(range(1, ny * nz), key=lambda t: -hops(t, nz))
    barrier = pltpu.get_barrier_semaphore()
    with scope("greet"):
        for t in order:
            oy, oz = other(t)
            for ox in (gx, 1 - gx):
                pl.semaphore_signal(barrier, inc=1, device_id=(ox, oy, oz), device_id_type=MESH)
        pl.semaphore_signal(barrier, inc=1, device_id=(1 - gx, gy, gz), device_id_type=MESH)

    f0, f1, f2 = s["f0"], s["f1"], s["f2"]
    ex = {k: Exchange(*v) for k, v in EXCHANGES.items()}
    targets = {"e0": f0, "c1": f1, "c2": f2, "e1": f1, "e2": f2, "x0": s["x0a"], "x1": s["x1a"], "x2": s["x2a"]}
    for k, target in targets.items():
        ex[k].bind(here, target, [s[k + str(i)] for i in range(7)])

    def partner(src, dst, i):
        return pltpu.make_async_remote_copy(
            src_ref=src,
            dst_ref=dst,
            send_sem=s["pair_send"].at[i],
            recv_sem=s["pair_recv"].at[i],
            device_id=(1 - gx, gy, gz),
            device_id_type=MESH,
        )

    me = gy * nz + gz

    def spread(src, whole, i):
        def copy(src, dst, oy, oz):
            return pltpu.make_async_remote_copy(
                src_ref=src,
                dst_ref=dst,
                send_sem=s["all_send"].at[i],
                recv_sem=s["all_recv"].at[i],
                device_id=(gx, oy, oz),
                device_id_type=MESH,
            )

        def start():
            for t in order:
                copy(src, whole.at[me], *other(t)).start()

        def finish():
            most = whole.at[pl.ds(0, ny * nz - 1)]
            copy(most, most, *other(1)).wait()

        return start, finish

    f1[...] = jnp.zeros_like(f1)
    f2[...] = jnp.zeros_like(f2)
    block = s["block"]
    block[...] = jnp.zeros_like(block)

    def block_put(field, plane, value):
        block[field, pl.ds(plane * 6, 6), :] = value

    for a in range(5):
        with scope("load_wait"):
            loads[a].wait()

        def load(i, carry, a=a):
            first = jnp.pad(s["land"][a, i], ((0, 0), (0, 80)))
            second = jnp.pad(s["land"][a, i + 24], ((0, 0), (0, 80)))
            value = roll_lanes(first, L0.zo) + roll_lanes(second, 64 + L0.zo)
            f0[a, pl.ds((L0.e + i) * L0.rows + L0.e, 48), :] = value
            return carry

        with scope("layout"):
            loop(0, 24, load, 0, 6)

    with scope("e0_pack"):
        ex["e0"].pack_yz(False)
    with scope("barrier"):
        pl.semaphore_wait(barrier, 2 * ny * nz - 1)
    ex["e0"].send_yz()
    with scope("coarsen_0"):
        coarsen_fields(L0, L1, f0, fields_put(L1, f1))
    with scope("c1_pack"):
        ex["c1"].start_yz()
    with scope("coarsen_1"):
        coarsen_fields(L1, L2, f1, fields_put(L2, f2))
    with scope("c2_pack"):
        ex["c2"].pack_yz(False)
    with scope("coarsen_2"):
        coarsen_fields(L2, None, f2, block_put)

    def tile_of(field):
        return roll_lanes(block[field].T[0:8], gx * 36)

    own4, pair4, own1, pair1, own_n = (s[k] for k in ("own4", "pair4", "own1", "pair1", "own_n"))
    for field in range(4):
        own4[field] = tile_of(field)
    pair_coef = partner(own4, pair4, 0)
    pair_coef.start()

    def square(i, carry):
        value = f0[4, pl.ds((L0.e + i) * L0.rows + L0.e, 48), :]
        return carry + value * value

    with scope("square"):
        squares = loop(0, 24, square, jnp.zeros((48, 128), F32), 4)
    with scope("e0_finish_yz"):
        ex["e0"].finish_yz()
    ex["e0"].start_x()
    ex["c2"].send_yz()
    g4, g1, gn = s["g4"], s["g1"], s["gn"]
    with scope("pair_coef"):
        pair_coef.wait()
    merged = s["merged4"]
    merged[...] = own4[...] + pair4[...]
    mine = pl.ds(2 * gx, 2)
    g4[gy, gz, mine] = merged[mine]
    row, column = gz // 4, gz % 4

    def coef_part(stage):
        if stage == 0:
            return g4.at[gy, gz, mine]
        if stage == 1:
            return g4.at[:, gz, mine]
        return g4.at[:, pl.ds(4 * row, 4), mine]

    def coef_copy(stage, src, oy, oz):
        return pltpu.make_async_remote_copy(
            src_ref=src,
            dst_ref=src,
            send_sem=s["coef_send"].at[stage],
            recv_sem=s["coef_recv"].at[stage],
            device_id=(gx, oy, oz),
            device_id_type=MESH,
        )

    def coef_start(stage):
        for d in (2, 1, 3):
            oy, oz = gy, gz
            if stage == 0:
                oy = lax.rem(gy + d, ny)
            elif stage == 1:
                oz = 4 * row + lax.rem(column + d, 4)
            else:
                oz = lax.rem(gz + 4 * d, nz)
            coef_copy(stage, coef_part(stage), oy, oz).start()

    def coef_wait(stage):
        two = pl.ds(0, 2)
        most = (g4.at[pl.ds(0, 3), 0, two], g4.at[:, pl.ds(0, 3), two], g4.at[:, pl.ds(0, 12), two])[stage]
        coef_copy(stage, most, lax.rem(gy + 1, ny), gz).wait()

    with scope("coef_0"):
        coef_start(0)
    with scope("c1_finish_yz"):
        ex["c1"].finish_yz()
    with scope("e0_finish_x"):
        ex["e0"].finish_x()
    ex["c1"].start_x()
    with scope("scaling_0"):
        scaling(L0, f0, s["i0"], s["u0"], 3)
    with scope("smooth_0"):
        smooth_from_zero(L0, f0, s["i0"], s["u0"], s["x0a"], s["x0b"], s["d0"], 3)
    with scope("restrict_0"):
        restrict(L0, L1, f0, s["u0"], s["x0a"], s["sums"], fields_put(L1, f1))
    with scope("e1_start_yz"):
        ex["e1"].start_yz()
    with scope("coef_1"):
        coef_wait(0)
        coef_start(1)
    with scope("x0_start_yz"):
        ex["x0"].start_yz()
    with scope("c1_finish_x"):
        ex["c1"].finish_x()
    with scope("scaling_1"):
        scaling(L1, f1, s["i1"], s["u1"], 4)
    with scope("c2_finish_yz"):
        ex["c2"].finish_yz()
    with scope("e1_finish_yz"):
        ex["e1"].finish_yz()
    ex["e1"].start_x()
    with scope("e1_finish_x"):
        ex["e1"].finish_x()
    with scope("coef_2"):
        coef_wait(1)
        coef_start(2)
    with scope("smooth_1"):
        smooth_from_zero(L1, f1, s["i1"], s["u1"], s["x1a"], s["x1b"], s["d1"], 3)
    with scope("restrict_1"):
        restrict(L1, L2, f1, s["u1"], s["x1a"], s["sums"], fields_put(L2, f2))
    with scope("e2_start_yz"):
        ex["e2"].start_yz()
    ex["c2"].start_x()
    with scope("x1_start_yz"):
        ex["x1"].start_yz()
    with scope("c2_finish_x"):
        ex["c2"].finish_x()
    with scope("scaling_2"):
        scaling(L2, f2, s["i2"], s["u2"], 5)
    other_half = pltpu.make_async_remote_copy(
        src_ref=g4.at[:, :, mine],
        dst_ref=g4.at[:, :, mine],
        send_sem=s["pair_send"].at[3],
        recv_sem=s["pair_recv"].at[3],
        device_id=(1 - gx, gy, gz),
        device_id_type=MESH,
    )
    with scope("x0_finish_yz"):
        ex["x0"].finish_yz()
    with scope("e2_finish_yz"):
        ex["e2"].finish_yz()
    ex["e2"].start_x()
    with scope("e2_finish_x"):
        ex["e2"].finish_x()
    with scope("smooth_2"):
        smooth_from_zero(L2, f2, s["i2"], s["u2"], s["x2a"], s["x2b"], s["d2"], 3)
    with scope("restrict_2"):
        restrict(L2, None, f2, s["u2"], s["x2a"], s["sums"], block_put)
    own1[...] = tile_of(4)
    pair_source = partner(own1, pair1, 1)
    pair_source.start()
    ex["x0"].start_x()
    with scope("coef_finish"):
        coef_wait(2)
    other_half.start()
    with scope("x2_start_yz"):
        ex["x2"].start_yz()
    with scope("pair_source"):
        pair_source.wait()
    s["merged1"][...] = own1[...] + pair1[...]
    g1[me] = s["merged1"][...]
    source_start, source_finish = spread(s["merged1"], g1, 1)
    with scope("source_start"):
        source_start()
    with scope("hidden"):
        ex["x1"].finish_yz()
        ex["x1"].start_x()
        ex["x0"].finish_x()
        ex["x2"].finish_yz()
        ex["x2"].start_x()
        ex["x1"].finish_x()
        ex["x2"].finish_x()
    with scope("other_half"):
        other_half.wait()
    gathered = lambda a, g: g4[g, :, a].reshape(128, 128)
    with scope("coarse_fields"):
        whole_prepare(ny, gathered, s["c3"], s["w3"], s["i3"])
        bottom_prepare(ny, gathered, s["bottom"])
    with scope("source_finish"):
        source_finish()
    with scope("coarse_solve"):
        source = lambda g: g1[pl.ds(g * nz, nz)].reshape(128, 128)
        whole = [s[k] for k in ("c3", "w3", "i3")]
        coarse_solve(ny, *whole, source, s["bottom"], s["x3a"], s["x3b"], s["d3"], s["g3"])
    with scope("window"):
        window(L2, gx, gy, gz, ny, s["x3b"], s["padded"], s["turned"], s["corner"], s["x2a"])
    with scope("post_2"):
        smooth(L2, f2, s["i2"], s["u2"], s["x2a"], s["x2b"], s["d2"], 6)
    with scope("prolong_1"):
        prolong(L1, L2, s["x2b"], s["x1a"], 3)
    with scope("post_1"):
        smooth(L1, f1, s["i1"], s["u1"], s["x1a"], s["x1b"], s["d1"], 5)
    with scope("prolong_0"):
        prolong(L0, L1, s["x1b"], s["x0a"], 2)
    with scope("post_0"):
        smooth(L0, f0, s["i0"], s["u0"], s["x0a"], s["x0b"], s["d0"], 4)

    land = s["land"]
    r0 = L0.rows
    lane48 = lanes(48) % 64
    inside = (lane48 >= L0.zo) & (lane48 < L0.zo + 48)

    def final(p, row, here_x, applied, kept):
        s["sums"][0, pl.ds((p - L0.e) * r0, r0), :] = f0[4, pl.ds(row, r0), :] - applied
        return kept

    with scope("final"):
        sweep(L0, f0, s["u0"], s["x0b"], 0, final)

    def out_square(i, carry):
        value = jnp.where(inside, s["sums"][0, pl.ds(i * r0 + L0.e, 48), :], 0.0)
        return carry + value * value

    with scope("square"):
        ends = loop(0, 24, out_square, jnp.zeros((48, 128), F32), 4)

    def fold(value):
        return jnp.sum(value, axis=0, keepdims=True)

    def squares_of(value):
        return jnp.sum(fold(value), axis=1, keepdims=True)

    lane1 = lax.broadcasted_iota(jnp.int32, (1, 128), 1)
    pair = jnp.where(lane1 == 0, squares_of(squares), jnp.where(lane1 == 1, squares_of(ends), 0.0))
    own_n[...] = pair
    mine_n = gx * (ny * nz) + me
    gn[mine_n] = pair

    def norm_copy(src, dst, ox, oy, oz):
        return pltpu.make_async_remote_copy(
            src_ref=src,
            dst_ref=dst,
            send_sem=s["all_send"].at[2],
            recv_sem=s["all_recv"].at[2],
            device_id=(ox, oy, oz),
            device_id_type=MESH,
        )

    with scope("norm_start"):
        for t in order:
            for ox in (gx, 1 - gx):
                norm_copy(own_n, gn.at[mine_n], ox, *other(t)).start()
        norm_copy(own_n, gn.at[mine_n], 1 - gx, gy, gz).start()

    def unload(slot, i, value):
        for half in range(2):
            moved = roll_lanes(value, -(L0.zo + 64 * half))
            land[slot, i + 24 * half] = moved[:, 0:48]

    def out_solution(i, carry):
        unload(0, i, s["x0b"][0, pl.ds((L0.e + i) * r0 + L0.e, 48), :])
        return carry

    def out_residual(i, carry):
        unload(1, i, s["sums"][0, pl.ds(i * r0 + L0.e, 48), :])
        return carry

    with scope("unload_solution"):
        loop(0, 24, out_solution, 0, 6)
    out0 = pltpu.make_async_copy(land.at[0], solution_hbm, s["out_sem"].at[0])
    out0.start()
    with scope("unload_residual"):
        loop(0, 24, out_residual, 0, 6)
    out1 = pltpu.make_async_copy(land.at[1], residual_hbm, s["out_sem"].at[1])
    out1.start()
    with scope("norm_finish"):
        most = gn.at[pl.ds(0, 2 * ny * nz - 1)]
        norm_copy(most, most, 1 - gx, gy, gz).wait()
    sums = jnp.sum(gn[...], axis=0)
    norm = jnp.sqrt(sums[:, 1:2] / sums[:, 0:1])
    norm_out[0, 0] = norm[0, 0]
    with scope("out_wait"):
        out0.wait()
        out1.wait()


EXCHANGES = {
    "e0": (L0, 0, 5),
    "c1": (L1, 0, 4),
    "c2": (L2, 0, 4),
    "e1": (L1, 4, 1),
    "e2": (L2, 4, 1),
    "x0": (L0, 0, 1),
    "x1": (L1, 0, 1),
    "x2": (L2, 0, 1),
}


def scratch_of(ny, nz):
    vmem = lambda *shape: pltpu.VMEM(shape, F32)
    size = lambda lv: lv.planes * lv.rows
    scratch = {"land": vmem(5, 48, 48, 48), "load_sem": pltpu.SemaphoreType.DMA((5,)), "out_sem": pltpu.SemaphoreType.DMA((2,))}
    for i, lv in enumerate((L0, L1, L2)):
        scratch[f"f{i}"] = vmem(5, size(lv), 128)
        for k in ("i", "d", "u"):
            scratch[f"{k}{i}"] = vmem(1, size(lv), 128)
        scratch[f"x{i}a"] = vmem(1, size(lv), 128)
        scratch[f"x{i}b"] = vmem(1, size(lv), 128)
    scratch["sums"] = vmem(1, 24 * 56, 128)
    scratch["block"] = vmem(5, 128, 128)
    for k in ("own4", "pair4", "merged4"):
        scratch[k] = vmem(4, 8, 128)
    for k in ("own1", "pair1", "merged1"):
        scratch[k] = vmem(8, 128)
    scratch["g4"] = vmem(ny, nz, 4, 8, 128)
    scratch["g1"] = vmem(ny * nz, 8, 128)
    scratch["gn"] = vmem(2 * ny * nz, 1, 128)
    scratch["own_n"] = vmem(1, 128)
    for k in ("pair_send", "pair_recv"):
        scratch[k] = pltpu.SemaphoreType.DMA((4,))
    for k in ("all_send", "all_recv", "coef_send", "coef_recv"):
        scratch[k] = pltpu.SemaphoreType.DMA((3,))
    for k in ("i3", "w3", "d3", "g3"):
        scratch[k] = vmem(ny, 128, 128)
    for k in ("x3a", "x3b"):
        scratch[k] = vmem(ny, 128 + 2 * PAD, 128)
    scratch["c3"] = vmem(6, ny, 128, 128)
    scratch["bottom"] = vmem(7, 64, 128)
    scratch["padded"] = vmem(ny + 2, nz + 2, 8, 128)
    scratch["turned"] = vmem(3, 152, 128)
    scratch["corner"] = vmem(16, 128)
    for k, v in EXCHANGES.items():
        for i, shape in enumerate(Exchange(*v).scratch()):
            scratch[k + str(i)] = shape
    return scratch


def solution(mesh):
    ny, nz = mesh.shape["gy"], mesh.shape["gz"]
    scratch = scratch_of(ny, nz)

    def shards(right_side, face_coef, absorption):
        field = jax.ShapeDtypeStruct((48, 48, 48), F32)
        solved, residual, norm = pl.pallas_call(
            functools.partial(cycle, ny, nz, tuple(scratch)),
            out_shape=(pltpu.VMEM((48, 48, 48), F32), pltpu.VMEM((48, 48, 48), F32), jax.ShapeDtypeStruct((1, 1), F32)),
            in_specs=[pl.BlockSpec(memory_space=pltpu.HBM)] * 3,
            out_specs=(
                pl.BlockSpec(memory_space=pl.ANY),
                pl.BlockSpec(memory_space=pl.ANY),
                pl.BlockSpec(memory_space=pltpu.SMEM),
            ),
            scratch_shapes=list(scratch.values()),
            compiler_params=pltpu.CompilerParams(
                collective_id=0, has_side_effects=True, vmem_limit_bytes=57000 * 1024
            ),
        )(right_side, face_coef, absorption)
        return solved, residual, norm[0, 0]

    in_specs = (P("gx", "gy", "gz"), P(None, "gx", "gy", "gz"), P("gx", "gy", "gz"))
    out_specs = (P("gx", "gy", "gz"), P("gx", "gy", "gz"), P())
    return jax.shard_map(shards, mesh=mesh, in_specs=in_specs, out_specs=out_specs, check_vma=False)
```

```python
import functools

import jax
import jax.numpy as jnp
from jax import lax
from jax.experimental import pallas as pl
from jax.experimental.pallas import tpu as pltpu
from jax.sharding import PartitionSpec as P

BOTTOM = 6
THETA = 1.125
DELTA = 0.875
SIGMA = THETA / DELTA
RHO0 = 1.0 / SIGMA
RHO1 = 1.0 / (2.0 * SIGMA - RHO0)
RHO2 = 1.0 / (2.0 * SIGMA - RHO1)
STEP1 = (RHO1 * RHO0, 2.0 * RHO1 / DELTA)
STEP2 = (RHO2 * RHO1, 2.0 * RHO2 / DELTA)

F32 = jnp.float32
MESH = pl.DeviceIdType.MESH


class Level:
    def __init__(self, n, e, ways, rows, zo, width, width_y, unroll):
        self.n, self.e, self.ways, self.rows, self.zo, self.width = n, e, ways, rows, zo, width
        self.width_y, self.unroll = width_y, unroll
        self.half = n // ways
        self.planes = self.half + 2 * e
        self.span = 128 // ways
        self.slots, self.slots_y = self.span // width, self.span // width_y
        self.packs, self.packs_y = -(-self.half // self.slots), -(-self.half // self.slots_y)


L0 = Level(48, 4, 2, 56, 8, 4, 64, 4)
L1 = Level(24, 6, 2, 40, 16, 8, 32, 4)
L2 = Level(12, 6, 1, 24, 16, 8, 16, 6)


def lanes(rows):
    return lax.broadcasted_iota(jnp.int32, (rows, 128), 1)


def gather_lanes(value, index):
    return jnp.take_along_axis(value, index, axis=1)


def roll_lanes(value, shift):
    return pltpu.roll(value, shift % 128, 1)


def roll_rows(value, shift):
    return pltpu.roll(value, shift % value.shape[0], 0)


def tile_rows(start, size):
    return pl.ds(pl.multiple_of(start, 8), size)


def loop(lo, hi, body, carry, unroll):
    count = (hi - lo) // unroll

    def chunk(i, carry):
        for k in range(unroll):
            carry = body(lo + i * unroll + k, carry)
        return carry

    carry = lax.fori_loop(0, count, chunk, carry)
    for k in range(lo + count * unroll, hi):
        carry = body(k, carry)
    return carry


class Exchange:
    def __init__(self, level, first, count):
        self.level, self.first, self.count = level, first, count
        lv = level
        sizes = [-(-rows // 8) * 8 for rows in (lv.packs_y * lv.e, lv.packs * lv.n, lv.packs * lv.e)]
        self.sizes = [sizes[0]] * 2 + [sizes[1]] * 2 + [sizes[2]] * 4
        self.starts = [sum(self.sizes[:i]) for i in range(9)]

    def scratch(self):
        lv, na = self.level, self.count
        shapes = [
            (na, lv.e * lv.rows, 128),
            (na, self.starts[8], 128),
            (na, self.starts[8], 128),
            (na, self.starts[8], 128),
            (2, na, lv.packs * lv.rows, 128),
        ]
        return [pltpu.VMEM(s, F32) for s in shapes] + [pltpu.SemaphoreType.DMA((2,)), pltpu.SemaphoreType.DMA((2,))]

    def bind(self, here, ref, scratch):
        self.here, self.ref = here, ref
        self.xr, self.out, self.got, self.spare, self.zf, self.ssem, self.rsem = scratch
        gx, gy, gz, ny, nz = here
        lv = self.level
        start = lv.e + (1 - gx) * (lv.half - lv.e if lv.ways == 2 else lv.n - lv.e)

        def copy(src, dst, i, gx, gy, gz):
            return pltpu.make_async_remote_copy(
                src_ref=src,
                dst_ref=dst,
                send_sem=self.ssem.at[i],
                recv_sem=self.rsem.at[i],
                device_id=(gx, gy, gz),
                device_id_type=MESH,
            )

        src = ref.at[pl.ds(self.first, self.count), tile_rows(start * lv.rows, lv.e * lv.rows), :]
        self.copy_x = copy(src, self.xr, 0, 1 - gx, gy, gz)
        ys = [lax.rem(gy + ny - 1, ny), lax.rem(gy + 1, ny)]
        zs = [lax.rem(gz + nz - 1, nz), lax.rem(gz + 1, nz)]
        targets = [(ys[0], gz), (ys[1], gz), (gy, zs[0]), (gy, zs[1])] + [(y, z) for y in ys for z in zs]
        lands = [1, 0, 3, 2, 7, 6, 5, 4]
        self.copies = [
            copy(
                self.out.at[:, pl.ds(self.starts[i], self.sizes[i]), :],
                self.got.at[:, pl.ds(self.starts[lands[i]], self.sizes[i]), :],
                1,
                gx,
                *targets[i],
            )
            for i in range(8)
        ]
        y_side, z_side = [gy > 0, gy < ny - 1], [gz > 0, gz < nz - 1]
        self.exists = y_side + z_side + [a & b for a in y_side for b in z_side]
        self.all = copy(self.out, self.got, 1, gx, *targets[0])
        self.has_y = [jnp.where(gy > 0, 1.0, 0.0).astype(F32), jnp.where(gy < ny - 1, 1.0, 0.0).astype(F32)]
        self.has_z = [jnp.where(gz > 0, 1.0, 0.0).astype(F32), jnp.where(gz < nz - 1, 1.0, 0.0).astype(F32)]
        self.has_x = [gx.astype(F32), (1 - gx).astype(F32)]
        return self

    def send(self, i):
        part = (slice(None), pl.ds(self.starts[i], self.sizes[i]), slice(None))

        @pl.when(self.exists[i])
        def _():
            self.copies[i].start()

        @pl.when(jnp.logical_not(self.exists[i]))
        def _():
            pltpu.make_async_copy(self.out.at[part], self.got.at[part], self.rsem.at[1]).start()
            pltpu.make_async_copy(self.out.at[part], self.spare.at[part], self.ssem.at[1]).start()

    def start_x(self):
        self.copy_x.start()

    def finish_x(self):
        lv, ref = self.level, self.ref
        e, r = lv.e, lv.rows
        self.copy_x.wait()
        low = lanes(r) < 64

        def finish(a, j):
            got = self.xr[a, tile_rows(j * r, r), :]
            if lv.ways == 2:
                got = roll_lanes(got, 64)
                below = roll_lanes(ref[self.first + a, tile_rows((lv.half + j) * r, r), :], 64)
                above = roll_lanes(ref[self.first + a, tile_rows((e + j) * r, r), :], 64)
                below = jnp.where(low, got * self.has_x[0], below)
                above = jnp.where(low, above, got * self.has_x[1])
            else:
                below = got * self.has_x[0]
                above = got * self.has_x[1]
            return below, above

        def body(a, carry):
            for first in range(0, e, 2):
                planes = range(first, min(first + 2, e))
                values = [finish(a, j) for j in planes]
                for j, (below, above) in zip(planes, values):
                    ref[self.first + a, tile_rows(j * r, r), :] = below
                    ref[self.first + a, tile_rows((e + lv.half + j) * r, r), :] = above
            return carry

        lax.fori_loop(0, self.count, body, 0)

    def pack(self, plane, rows, width, shifts, put):
        lv = self.level
        slot = (lanes(rows) % lv.span) // width
        slots = lv.span // width
        for k in range(-(-lv.half // slots)):
            acc = None
            for s in range(min(slots, lv.half - k * slots)):
                moved = [roll_lanes(v, s * width - shift) for v, shift in zip(plane(lv.e + k * slots + s), shifts)]
                acc = moved if s == 0 else [jnp.where(slot == s, new, old) for new, old in zip(moved, acc)]
            put(k, acc)

    def pack_yz(self, send):
        lv, ref = self.level, self.ref
        r, n, e, zo = lv.rows, lv.n, lv.e, lv.zo
        z_shifts = (zo, zo + n - e)

        def put_at(first, rows, a):
            def put(k, values):
                for i, value in enumerate(values):
                    self.out[a, pl.ds(self.starts[first + i] + k * rows, rows), :] = value

            return put

        def edges(a, p):
            return [ref[self.first + a, pl.ds(p * r + row, e), :] for row in (e, n)]

        def pack_d(a, carry):
            def plane(p):
                low, high = edges(a, p)
                return low, low, high, high

            self.pack(plane, e, lv.width, z_shifts * 2, put_at(4, e, a))
            return carry

        def pack_z(a, carry):
            def plane(p):
                return [ref[self.first + a, pl.ds(p * r + e, n), :]] * 2

            self.pack(plane, n, lv.width, z_shifts, put_at(2, n, a))
            return carry

        def pack_y(a, carry):
            if lv.slots_y == 1:
                for k in range(lv.half):
                    put_at(0, e, a)(k, edges(a, e + k))
            else:
                self.pack(lambda p: edges(a, p), e, lv.width_y, (zo, zo), put_at(0, e, a))
            return carry

        for body, which in ((pack_d, range(4, 8)), (pack_z, (2, 3)), (pack_y, (0, 1))):
            lax.fori_loop(0, self.count, body, 0)
            if send:
                for i in which:
                    self.send(i)

    def send_yz(self):
        for i in (4, 5, 6, 7, 2, 3, 0, 1):
            self.send(i)

    def start_yz(self):
        self.pack_yz(True)

    def finish_yz(self):
        lv, ref = self.level, self.ref
        r, n, e, zo = lv.rows, lv.n, lv.e, lv.zo
        with jax.named_scope("arrive"):
            self.all.wait()
        lane = lanes(r) % lv.span
        at_low = (lane >= zo - e) & (lane < zo)
        at_high = (lane >= zo + n) & (lane < zo + n + e)

        def unpack(a, carry):
            def got(i, row, rows):
                return self.got[a, pl.ds(self.starts[i] + row, rows), :]

            for s in range(2):
                for k in range(lv.packs_y):
                    value = got(s, k * e, e) * self.has_y[s]
                    for slot in range(min(lv.slots_y, lv.half - k * lv.slots_y)):
                        row = (e + k * lv.slots_y + slot) * r + (e + n) * s
                        moved = roll_lanes(value, zo - slot * lv.width_y) if lv.slots_y > 1 else value
                        ref[self.first + a, pl.ds(row, e), :] = moved
            for k in range(lv.packs):
                for t in range(2):
                    self.zf[t, a, pl.ds(k * r + e, n), :] = got(2 + t, k * n, n) * self.has_z[t]
                    for s in range(2):
                        both = self.has_y[s] * self.has_z[t]
                        self.zf[t, a, pl.ds(k * r + (e + n) * s, e), :] = got(4 + 2 * s + t, k * e, e) * both
            for k in range(lv.packs):
                sides = [self.zf[t, a, pl.ds(k * r, r), :] for t in range(2)]
                count = min(lv.slots, lv.half - k * lv.slots)
                for first in range(0, count, 4):
                    slots = range(first, min(first + 4, count))
                    values = []
                    for s in slots:
                        value = ref[self.first + a, pl.ds((e + k * lv.slots + s) * r, r), :]
                        value = jnp.where(at_low, roll_lanes(sides[0], zo - e - s * lv.width), value)
                        values.append(jnp.where(at_high, roll_lanes(sides[1], zo + n - s * lv.width), value))
                    for s, value in zip(slots, values):
                        ref[self.first + a, pl.ds((e + k * lv.slots + s) * r, r), :] = value
            return carry

        lax.fori_loop(0, self.count, unpack, 0)


def scaling(lv, fields, inverse, upper, extent):
    r = lv.rows

    def body(p, carry):
        row = pl.multiple_of(p * r, 8)
        cells = fields[3, pl.ds(row, r), :]
        face_z = fields[2, pl.ds(row, r), :]
        total = cells + fields[0, pl.ds(row, r), :] + fields[0, pl.ds(row + r, r), :]
        total = total + fields[1, pl.ds(row, r), :] + fields[1, pl.ds(row + 1, r), :]
        above = roll_lanes(face_z, -1)
        upper[0, pl.ds(row, r), :] = above
        total = total + face_z + above
        inverse[0, pl.ds(row, r), :] = jnp.where(cells > 0.0, 1.0 / total, 0.0)
        return carry

    loop(lv.e - extent, lv.e + lv.half + extent, body, 0, lv.unroll)


def sweep(lv, fields, upper, x, extent, emit, carry=0):
    r = lv.rows
    lo, hi = lv.e - extent, lv.e + lv.half + extent

    def body(p, carry):
        here, flux, kept = carry
        row = pl.multiple_of(p * r, 8)
        after = x[0, pl.ds(row + r, r), :]
        flux_after = fields[0, pl.ds(row + r, r), :] * (after - here)
        flux_y = fields[1, pl.ds(row, r), :] * (here - roll_rows(here, 1))
        flux_y = flux_y - fields[1, pl.ds(row + 1, r), :] * (roll_rows(here, -1) - here)
        flux_z = fields[2, pl.ds(row, r), :] * (here - roll_lanes(here, 1))
        flux_z = flux_z - upper[0, pl.ds(row, r), :] * (roll_lanes(here, -1) - here)
        applied = fields[3, pl.ds(row, r), :] * here + ((flux - flux_after) + flux_y + flux_z)
        return after, flux_after, emit(p, row, here, applied, kept)

    row = lo * r
    here = x[0, pl.ds(row, r), :]
    flux = fields[0, pl.ds(row, r), :] * (here - x[0, pl.ds(row - r, r), :])
    return loop(lo, hi, body, (here, flux, carry), lv.unroll)[2]


def step(lv, fields, inverse, upper, x, out, d, extent, first, coefs, keep):
    r = lv.rows

    def emit(p, row, here, applied, kept):
        scaled = inverse[0, pl.ds(row, r), :] * (fields[4, pl.ds(row, r), :] - applied)
        if first == 0:
            update = scaled * (1.0 / THETA)
        elif first == 1:
            update = coefs[0] * here + coefs[1] * scaled
        else:
            update = coefs[0] * d[0, pl.ds(row, r), :] + coefs[1] * scaled
        if keep:
            d[0, pl.ds(row, r), :] = update
        out[0, pl.ds(row, r), :] = here + update
        return kept

    sweep(lv, fields, upper, x, extent, emit)


def smooth_from_zero(lv, fields, inverse, upper, xa, xb, d, extent):
    r = lv.rows

    def body(p, carry):
        row = pl.multiple_of(p * r, 8)
        xa[0, pl.ds(row, r), :] = inverse[0, pl.ds(row, r), :] * fields[4, pl.ds(row, r), :] * (1.0 / THETA)
        return carry

    loop(lv.e - extent, lv.e + lv.half + extent, body, 0, lv.unroll)
    step(lv, fields, inverse, upper, xa, xb, d, extent - 1, 1, STEP1, True)
    step(lv, fields, inverse, upper, xb, xa, d, extent - 2, 2, STEP2, False)


def smooth(lv, fields, inverse, upper, xa, xb, d, extent):
    step(lv, fields, inverse, upper, xa, xb, d, extent - 1, 0, None, True)
    step(lv, fields, inverse, upper, xb, xa, d, extent - 2, 2, STEP1, True)
    step(lv, fields, inverse, upper, xa, xb, d, extent - 3, 2, STEP2, False)


def coarse_lanes(lv, below, rows, half):
    lane = lanes(rows)
    if below is None:
        cell, at = lane, 0
    else:
        at = (lane // below.span) * 64 if below.ways == 2 else 0
        cell = lane % below.span - below.zo
    if lv.ways == 2 and half is not None:
        at = 64 * half
    inside = (cell >= 0) & (cell < lv.n // 2)
    index = jnp.where(inside, at + lv.zo + 2 * cell, 0)
    return index, inside


def place(lv, below, put, plane, value, pair):
    rows = value.shape[0]
    if pair:
        value = value + roll_lanes(value, -1)
    halves = [None] if below is not None and below.ways == lv.ways else range(lv.ways)
    for half in halves:
        index, inside = coarse_lanes(lv, below, rows, half)
        got = jnp.where(inside, gather_lanes(value, index), 0.0)
        put(plane if half is None else plane + half * (lv.half // 2), got)


def coarsen_fields(lv, below, fields, put):
    n2, e, r = lv.n // 2, lv.e, lv.rows

    def body(i, carry):
        row = (e + 2 * i) * r + e

        def rows(a, plane, odd):
            return fields[a, pl.ds(row + plane * r + odd, n2, stride=2), :]

        put_x = functools.partial(put, 0)
        put_y = functools.partial(put, 1)
        put_z = functools.partial(put, 2)
        put_c = functools.partial(put, 3)
        place(lv, below, put_x, i, (rows(0, 0, 0) + rows(0, 0, 1)) * 0.0625, True)
        place(lv, below, put_y, i, (rows(1, 0, 0) + rows(1, 1, 0)) * 0.0625, True)
        place(lv, below, put_z, i, (rows(2, 0, 0) + rows(2, 0, 1) + rows(2, 1, 0) + rows(2, 1, 1)) * 0.0625, False)
        place(lv, below, put_c, i, (rows(3, 0, 0) + rows(3, 0, 1) + rows(3, 1, 0) + rows(3, 1, 1)) * 0.125, True)
        return carry

    loop(0, lv.half // 2, body, 0, 3)


def restrict(lv, below, fields, upper, x, sums, put):
    r, n2 = lv.rows, lv.n // 2

    def emit(p, row, here, applied, kept):
        sums[0, pl.ds((p - lv.e) * r, r), :] = fields[4, pl.ds(row, r), :] - applied
        return kept

    sweep(lv, fields, upper, x, 0, emit)

    def body(i, carry):
        total = None
        for plane in range(2):
            for odd in range(2):
                part = sums[0, pl.ds((2 * i + plane) * r + lv.e + odd, n2, stride=2), :]
                total = part if total is None else total + part
        place(lv, below, functools.partial(put, 4), i, total * 0.125, True)
        return carry

    loop(0, lv.half // 2, body, 0, 6)


def fields_put(below, fields):
    def put(field, plane, value):
        fields[field, pl.ds((below.e + plane) * below.rows + below.e, below.n), :] = value

    return put


def prolong(lv, above, e, x, reach):
    r, rows = lv.rows, lv.n // 2 + 2 * reach
    lane = lanes(rows)
    cell = lane % 64 - lv.zo + 2 * reach
    inside = (cell >= 0) & (cell < 2 * rows)
    source = above.zo - reach + cell // 2
    if above.ways == 2:
        source = source + (lane // 64) * 64
    source = jnp.where(inside, source, 0)

    def body(i, carry):
        row = (above.e - reach + i) * above.rows + above.e - reach
        value = gather_lanes(e[0, pl.ds(row, rows), :], source)
        if above.ways == 1:
            other = gather_lanes(e[0, pl.ds(row + (lv.half // 2) * above.rows, rows), :], source)
            value = jnp.where(lane < 64, value, other)
        value = jnp.where(inside, value, 0.0)
        for plane in range(2):
            at = (lv.e - 2 * reach + 2 * i + plane) * r + lv.e - 2 * reach
            for odd in range(2):
                where = pl.ds(at + odd, rows, stride=2)
                x[0, where, :] = x[0, where, :] + value
        return carry

    loop(0, lv.half // 2 + 2 * reach, body, 0, 4)


PAD = 8


def row_of(rows):
    return lax.broadcasted_iota(jnp.int32, (rows, 128), 0)


def whole_neighbours(ny, value, rows):
    z, y = row_of(128) % 8, lanes(128) % 6
    out = []
    for g in range(ny):
        here = value(g)
        low_y, high_y = roll_lanes(here, 1), roll_lanes(here, -1)
        if g:
            low_y = jnp.where(y == 0, roll_lanes(value(g - 1), -5), low_y)
        if g + 1 < ny:
            high_y = jnp.where(y == 5, roll_lanes(value(g + 1), 5), high_y)
        low_z = jnp.where(z == 0, rows(g, -3), rows(g, -1))
        high_z = jnp.where(z == 5, rows(g, 3), rows(g, 1))
        out.append((roll_lanes(here, 6), roll_lanes(here, -6), low_y, high_y, low_z, high_z))
    return out


def whole_prepare(ny, fields, coefs, diagonal, inverse):
    z, y, row = row_of(128) % 8, lanes(128) % 6, row_of(128)
    moved = lambda a: whole_neighbours(ny, lambda g: fields(a, g), lambda g, d: roll_rows(fields(a, g), -d))
    high = [[near[1] for near in moved(0)], [near[3] for near in moved(1)], [near[5] for near in moved(2)]]
    for g in range(ny):
        inside = fields(3, g) > 0.0
        high_y = jnp.where(y == 5, 0.0, high[1][g]) if g + 1 == ny else high[1][g]
        high_z = jnp.where(row == 125, 0.0, high[2][g])
        sides = [fields(0, g), high[0][g], fields(1, g), high_y, fields(2, g), high_z]
        total = functools.reduce(lambda a, b: a + b, sides) + fields(3, g)
        scale = jnp.where(inside, 1.0 / total, 0.0)
        diagonal[g] = jnp.where(inside, total, 0.0)
        inverse[g] = scale
        if g == 0:
            sides[2] = jnp.where(y == 0, 0.0, sides[2])
        sides[4] = jnp.where(row == 0, 0.0, sides[4])
        for i in range(6):
            coefs[i, g] = sides[i] * scale


def children(value, axes):
    if "y" in axes:
        value = value + roll_lanes(value, -1)
    if "x" in axes:
        value = value + roll_lanes(value, -6)
    if "z" in axes:
        value = value + roll_rows(value, -1)
    return value


def even_cells():
    row, lane = row_of(128), lanes(128)
    return (row % 2 == 0) & (row % 8 < 6) & (lane % 2 == 0) & ((lane // 6) % 2 == 0) & (lane < 72)


def fold_level(values):
    even = even_cells()
    values = [jnp.where(even, v, 0.0) for v in values]
    both = (values[0] + roll_lanes(values[1], 1)) + (roll_lanes(values[2], 6) + roll_lanes(values[3], 7))
    return both[0:64] + roll_rows(both[64:128], 1)


def unfold_level(value):
    both = jnp.concatenate([value, roll_rows(value, -1)], axis=0)
    even = even_cells()
    return [jnp.where(even, roll_lanes(both, -shift), 0.0) for shift in (0, 1, 6, 7)]


def bottom_neighbours(v):
    row, lane = row_of(64), lanes(64)
    z, y = (row % 8) // 2, (lane % 6) // 2
    odd = lane % 2 == 1
    low_y = jnp.where(y > 0, roll_lanes(v, 2), jnp.where(odd, roll_lanes(v, -3), roll_lanes(v, 1)))
    high_y = jnp.where(y < 2, roll_lanes(v, -2), jnp.where(odd, roll_lanes(v, -1), roll_lanes(v, 3)))
    low_z = jnp.where(z > 0, roll_rows(v, 2), jnp.where(row == 1, roll_rows(v, 5), roll_rows(v, 4)))
    high_z = jnp.where(z < 2, roll_rows(v, -2), jnp.where(row == 60, roll_rows(v, -5), roll_rows(v, -4)))
    return roll_lanes(v, 12), roll_lanes(v, -12), low_y, high_y, low_z, high_z


def bottom_prepare(ny, fields, bottom):
    row, lane = row_of(64), lanes(64)
    y = (lane % 6) // 2
    first = (lane % 2 == 0) & ((lane // 6) % 2 == 0)
    last = (lane % 2 == 1) & ((lane // 6) % 2 == 1)
    faces = []
    for a, axes in enumerate(("yz", "xz", "xy", "xyz")):
        factor = 0.125 if a == 3 else 0.0625
        faces.append(fold_level([children(fields(a, g), axes) * factor for g in range(ny)]))
    inside = faces[3] > 0.0
    high_x = bottom_neighbours(faces[0])[1]
    high_y = jnp.where(last & (y == 2), 0.0, bottom_neighbours(faces[1])[3])
    high_z = jnp.where(row == 61, 0.0, bottom_neighbours(faces[2])[5])
    sides = [faces[0], high_x, faces[1], high_y, faces[2], high_z]
    total = functools.reduce(lambda a, b: a + b, sides) + faces[3]
    sides[2] = jnp.where(first & (y == 0), 0.0, sides[2])
    sides[4] = jnp.where(row == 0, 0.0, sides[4])
    for i, value in enumerate(sides + [total]):
        bottom[i] = jnp.where(inside, value, 0.0)


def coarse_solve(ny, coefs, diagonal, inverse, f, bottom, xa, xb, ds, g3):
    def rows(x, g, offset=0):
        return x[g, pl.ds(PAD + offset, 128)]

    def scaled(x):
        near = whole_neighbours(ny, lambda g: rows(x, g), lambda g, d: rows(x, g, d))
        out = []
        for g in range(ny):
            parts = [coefs[i, g] * near[g][i] for i in range(6)]
            total = ((parts[0] + parts[1]) + (parts[2] + parts[3])) + (parts[4] + parts[5])
            out.append((g3[g] - rows(x, g)) + total)
        return out

    def advance(x, to, coef, first, keep=True):
        for g, value in enumerate(scaled(x)):
            update = value * (1.0 / THETA) if first else coef[0] * ds[g] + coef[1] * value
            if keep:
                ds[g] = update
            to[g, pl.ds(PAD, 128)] = rows(x, g) + update

    for x in (xa, xb):
        for g in range(ny):
            x[g, pl.ds(0, PAD)] = jnp.zeros((PAD, 128), F32)
            x[g, pl.ds(PAD + 128, PAD)] = jnp.zeros((PAD, 128), F32)
    for g in range(ny):
        g3[g] = inverse[g] * f(g)
        ds[g] = g3[g] * (1.0 / THETA)
        xa[g, pl.ds(PAD, 128)] = ds[g]
    advance(xa, xb, STEP1, False)
    advance(xb, xa, STEP2, False, False)
    remainder = scaled(xa)
    r = fold_level([children(remainder[g] * diagonal[g], "xyz") * 0.125 for g in range(ny)])
    r = jnp.where(bottom[6] > 0.0, r, 0.0)

    def total(value):
        value = jnp.sum(value.reshape(8, 8, 128), axis=0)
        return jnp.sum(jnp.sum(value, axis=1, keepdims=True), axis=0, keepdims=True)

    def applied(v):
        near = bottom_neighbours(v)
        parts = [bottom[i] * near[i] for i in range(6)]
        return bottom[6] * v - (((parts[0] + parts[1]) + (parts[2] + parts[3])) + (parts[4] + parts[5]))

    e = jnp.zeros((64, 128), F32)
    p, norm = r, total(r * r)
    for i in range(BOTTOM):
        q = applied(p)
        size = norm / total(p * q)
        e = e + size * p
        if i + 1 < BOTTOM:
            r = r - size * q
            after = total(r * r)
            p = r + after / norm * p
            norm = after
    for g, value in enumerate(unfold_level(e)):
        value = value + roll_lanes(value, 1)
        value = value + roll_lanes(value, 6)
        xa[g, pl.ds(PAD, 128)] = rows(xa, g) + (value + roll_rows(value, 1))
    advance(xa, xb, None, True)
    advance(xb, xa, STEP1, False)
    advance(xa, xb, STEP2, False, False)


def window(lv, gx, gy, gz, ny, xs, padded, turned, corner, x):
    nz = 16
    padded[...] = jnp.zeros_like(padded)
    for g in range(ny):
        padded[g + 1, pl.ds(1, nz)] = xs[g, pl.ds(PAD, 128)].reshape(nz, 8, 128)
    for dy in range(3):
        tiles = padded[gy + dy, pl.ds(gz, 3)].reshape(24, 128)
        tiles = jnp.concatenate([tiles, jnp.zeros((104, 128), F32)], axis=0)
        turned[dy, pl.ds(0, 24), :] = jnp.zeros((24, 128), F32)
        turned[dy, pl.ds(24, 128), :] = tiles.T
    lane = lanes(16)
    cell = lane - lv.zo + 6
    inside = (cell >= 0) & (cell < 24)
    coarse = jnp.where(inside, cell // 2 + 3, 0)
    source = (coarse // 6) * 8 + coarse % 6

    def body(i, carry):
        base = 6 + 36 * gx + 6 * i
        corner[pl.ds(0, 3), :] = turned[0, pl.ds(base + 3, 3), :]
        corner[pl.ds(3, 6), :] = turned[1, pl.ds(base, 6), :]
        corner[pl.ds(9, 3), :] = turned[2, pl.ds(base, 3), :]
        value = jnp.where(inside, gather_lanes(corner[...], source), 0.0)[0:12]
        for plane in range(2):
            at = (lv.e - 6 + 2 * i + plane) * lv.rows + lv.e - 6
            for odd in range(2):
                where = pl.ds(at + odd, 12, stride=2)
                x[0, where, :] = x[0, where, :] + value
        return carry

    loop(0, 12, body, 0, 4)


def hops(t, nz):
    return sum(min(d, 4 - d) for d in (t // nz % 4, t % nz // 4, t % 4))


def cycle(ny, nz, names, *refs):
    refs = list(refs)
    right_hbm, faces_hbm, cells_hbm, solution_hbm, residual_hbm, norm_out = refs[:6]
    s = dict(zip(names, refs[6:]))
    gx, gy, gz = lax.axis_index("gx"), lax.axis_index("gy"), lax.axis_index("gz")
    here = (gx, gy, gz, ny, nz)
    scope = jax.named_scope

    loads = [pltpu.make_async_copy(faces_hbm.at[d], s["land"].at[d], s["load_sem"].at[d]) for d in range(3)]
    loads.append(pltpu.make_async_copy(cells_hbm, s["land"].at[3], s["load_sem"].at[3]))
    loads.append(pltpu.make_async_copy(right_hbm, s["land"].at[4], s["load_sem"].at[4]))
    for copy in loads:
        copy.start()

    def other(t):
        return lax.rem(gy + t // nz, ny), lax.rem(gz + t % nz, nz)

    order = sorted(range(1, ny * nz), key=lambda t: -hops(t, nz))
    barrier = pltpu.get_barrier_semaphore()
    with scope("greet"):
        for t in order:
            oy, oz = other(t)
            for ox in (gx, 1 - gx):
                pl.semaphore_signal(barrier, inc=1, device_id=(ox, oy, oz), device_id_type=MESH)
        pl.semaphore_signal(barrier, inc=1, device_id=(1 - gx, gy, gz), device_id_type=MESH)

    f0, f1, f2 = s["f0"], s["f1"], s["f2"]
    ex = {k: Exchange(*v) for k, v in EXCHANGES.items()}
    targets = {"e0a": f0, "e0b": f0, "e0c": f0, "c1": f1, "c2": f2, "e1": f1, "e2": f2, "x0": s["x0a"], "x1": s["x1a"], "x2": s["x2a"]}
    for k, target in targets.items():
        ex[k].bind(here, target, [s[k + str(i)] for i in range(7)])

    def partner(src, dst, i):
        return pltpu.make_async_remote_copy(
            src_ref=src,
            dst_ref=dst,
            send_sem=s["pair_send"].at[i],
            recv_sem=s["pair_recv"].at[i],
            device_id=(1 - gx, gy, gz),
            device_id_type=MESH,
        )

    me = gy * nz + gz

    def spread(src, whole, i):
        def copy(src, dst, oy, oz):
            return pltpu.make_async_remote_copy(
                src_ref=src,
                dst_ref=dst,
                send_sem=s["all_send"].at[i],
                recv_sem=s["all_recv"].at[i],
                device_id=(gx, oy, oz),
                device_id_type=MESH,
            )

        def start():
            for t in order:
                copy(src, whole.at[me], *other(t)).start()

        def finish():
            most = whole.at[pl.ds(0, ny * nz - 1)]
            copy(most, most, *other(1)).wait()

        return start, finish

    f1[...] = jnp.zeros_like(f1)
    f2[...] = jnp.zeros_like(f2)
    block = s["block"]
    block[...] = jnp.zeros_like(block)

    def block_put(field, plane, value):
        block[field, pl.ds(plane * 6, 6), :] = value

    for a in range(5):
        with scope("load_wait"):
            loads[a].wait()

        def load(i, carry, a=a):
            first = jnp.pad(s["land"][a, i], ((0, 0), (0, 80)))
            second = jnp.pad(s["land"][a, i + 24], ((0, 0), (0, 80)))
            value = roll_lanes(first, L0.zo) + roll_lanes(second, 64 + L0.zo)
            f0[a, pl.ds((L0.e + i) * L0.rows + L0.e, 48), :] = value
            return carry

        with scope("layout"):
            loop(0, 24, load, 0, 12)

    with scope("e0_pack"):
        ex["e0a"].pack_yz(False)
    with scope("barrier"):
        pl.semaphore_wait(barrier, 2 * ny * nz - 1)
    ex["e0a"].send_yz()
    with scope("e0_start_yz"):
        ex["e0b"].start_yz()
        ex["e0c"].start_yz()
    with scope("coarsen_0"):
        coarsen_fields(L0, L1, f0, fields_put(L1, f1))
    with scope("c1_pack"):
        ex["c1"].pack_yz(False)
    with scope("coarsen_1"):
        coarsen_fields(L1, L2, f1, fields_put(L2, f2))
    with scope("c2_pack"):
        ex["c2"].pack_yz(False)
    with scope("coarsen_2"):
        coarsen_fields(L2, None, f2, block_put)

    def tile_of(field):
        return roll_lanes(block[field].T[0:8], gx * 36)

    own4, pair4, own1, pair1, own_n = (s[k] for k in ("own4", "pair4", "own1", "pair1", "own_n"))
    for field in range(4):
        own4[field] = tile_of(field)
    pair_coef = partner(own4, pair4, 0)
    pair_coef.start()

    def square(i, carry):
        value = f0[4, pl.ds((L0.e + i) * L0.rows + L0.e, 48), :]
        return carry + value * value

    with scope("square"):
        squares = loop(0, 24, square, jnp.zeros((48, 128), F32), 4)
    for k in ("e0a", "e0b", "e0c"):
        with scope(k + "_finish_yz"):
            ex[k].finish_yz()
        ex[k].start_x()
    ex["c1"].send_yz()
    ex["c2"].send_yz()
    g4, g1, gn = s["g4"], s["g1"], s["gn"]
    with scope("pair_coef"):
        pair_coef.wait()
    merged = s["merged4"]
    merged[...] = own4[...] + pair4[...]
    mine = pl.ds(2 * gx, 2)
    g4[gy, gz, mine] = merged[mine]
    row, column = gz // 4, gz % 4

    def coef_part(stage):
        if stage == 0:
            return g4.at[gy, gz, mine]
        if stage == 1:
            return g4.at[:, gz, mine]
        return g4.at[:, pl.ds(4 * row, 4), mine]

    def coef_copy(stage, src, oy, oz):
        return pltpu.make_async_remote_copy(
            src_ref=src,
            dst_ref=src,
            send_sem=s["coef_send"].at[stage],
            recv_sem=s["coef_recv"].at[stage],
            device_id=(gx, oy, oz),
            device_id_type=MESH,
        )

    def coef_start(stage):
        for d in (2, 1, 3):
            oy, oz = gy, gz
            if stage == 0:
                oy = lax.rem(gy + d, ny)
            elif stage == 1:
                oz = 4 * row + lax.rem(column + d, 4)
            else:
                oz = lax.rem(gz + 4 * d, nz)
            coef_copy(stage, coef_part(stage), oy, oz).start()

    def coef_wait(stage):
        two = pl.ds(0, 2)
        most = (g4.at[pl.ds(0, 3), 0, two], g4.at[:, pl.ds(0, 3), two], g4.at[:, pl.ds(0, 12), two])[stage]
        coef_copy(stage, most, lax.rem(gy + 1, ny), gz).wait()

    with scope("coef_0"):
        coef_start(0)
    with scope("e0_finish_x"):
        ex["e0a"].finish_x()
        ex["e0b"].finish_x()
    with scope("scaling_0"):
        scaling(L0, f0, s["i0"], s["u0"], 3)
    with scope("e0c_finish_x"):
        ex["e0c"].finish_x()
    with scope("smooth_0"):
        smooth_from_zero(L0, f0, s["i0"], s["u0"], s["x0a"], s["x0b"], s["d0"], 3)
    with scope("restrict_0"):
        restrict(L0, L1, f0, s["u0"], s["x0a"], s["sums"], fields_put(L1, f1))
    with scope("e1_start_yz"):
        ex["e1"].start_yz()
    with scope("coef_1"):
        coef_wait(0)
        coef_start(1)
    with scope("c1_finish_yz"):
        ex["c1"].finish_yz()
    ex["c1"].start_x()
    with scope("c2_finish_yz"):
        ex["c2"].finish_yz()
    with scope("c1_finish_x"):
        ex["c1"].finish_x()
    with scope("scaling_1"):
        scaling(L1, f1, s["i1"], s["u1"], 4)
    with scope("e1_finish_yz"):
        ex["e1"].finish_yz()
    ex["e1"].start_x()
    with scope("x0_start_yz"):
        ex["x0"].start_yz()
    with scope("e1_finish_x"):
        ex["e1"].finish_x()
    with scope("coef_2"):
        coef_wait(1)
        coef_start(2)
    with scope("smooth_1"):
        smooth_from_zero(L1, f1, s["i1"], s["u1"], s["x1a"], s["x1b"], s["d1"], 3)
    with scope("restrict_1"):
        restrict(L1, L2, f1, s["u1"], s["x1a"], s["sums"], fields_put(L2, f2))
    with scope("e2_start_yz"):
        ex["e2"].start_yz()
    ex["c2"].start_x()
    with scope("x1_start_yz"):
        ex["x1"].start_yz()
    with scope("c2_finish_x"):
        ex["c2"].finish_x()
    with scope("scaling_2"):
        scaling(L2, f2, s["i2"], s["u2"], 5)
    other_half = pltpu.make_async_remote_copy(
        src_ref=g4.at[:, :, mine],
        dst_ref=g4.at[:, :, mine],
        send_sem=s["pair_send"].at[3],
        recv_sem=s["pair_recv"].at[3],
        device_id=(1 - gx, gy, gz),
        device_id_type=MESH,
    )
    with scope("x0_finish_yz"):
        ex["x0"].finish_yz()
    with scope("e2_finish_yz"):
        ex["e2"].finish_yz()
    ex["e2"].start_x()
    with scope("e2_finish_x"):
        ex["e2"].finish_x()
    with scope("smooth_2"):
        smooth_from_zero(L2, f2, s["i2"], s["u2"], s["x2a"], s["x2b"], s["d2"], 3)
    with scope("restrict_2"):
        restrict(L2, None, f2, s["u2"], s["x2a"], s["sums"], block_put)
    own1[...] = tile_of(4)
    pair_source = partner(own1, pair1, 1)
    pair_source.start()
    ex["x0"].start_x()
    with scope("coef_finish"):
        coef_wait(2)
    other_half.start()
    with scope("x2_start_yz"):
        ex["x2"].start_yz()
    with scope("pair_source"):
        pair_source.wait()
    s["merged1"][...] = own1[...] + pair1[...]
    g1[me] = s["merged1"][...]
    source_start, source_finish = spread(s["merged1"], g1, 1)
    with scope("source_start"):
        source_start()
    with scope("hidden"):
        ex["x1"].finish_yz()
        ex["x1"].start_x()
        ex["x0"].finish_x()
        ex["x2"].finish_yz()
        ex["x2"].start_x()
        ex["x1"].finish_x()
        ex["x2"].finish_x()
    with scope("other_half"):
        other_half.wait()
    gathered = lambda a, g: g4[g, :, a].reshape(128, 128)
    with scope("coarse_fields"):
        whole_prepare(ny, gathered, s["c3"], s["w3"], s["i3"])
        bottom_prepare(ny, gathered, s["bottom"])
    with scope("source_finish"):
        source_finish()
    with scope("coarse_solve"):
        source = lambda g: g1[pl.ds(g * nz, nz)].reshape(128, 128)
        whole = [s[k] for k in ("c3", "w3", "i3")]
        coarse_solve(ny, *whole, source, s["bottom"], s["x3a"], s["x3b"], s["d3"], s["g3"])
    with scope("window"):
        window(L2, gx, gy, gz, ny, s["x3b"], s["padded"], s["turned"], s["corner"], s["x2a"])
    with scope("post_2"):
        smooth(L2, f2, s["i2"], s["u2"], s["x2a"], s["x2b"], s["d2"], 6)
    with scope("prolong_1"):
        prolong(L1, L2, s["x2b"], s["x1a"], 3)
    with scope("post_1"):
        smooth(L1, f1, s["i1"], s["u1"], s["x1a"], s["x1b"], s["d1"], 5)
    with scope("prolong_0"):
        prolong(L0, L1, s["x1b"], s["x0a"], 2)
    with scope("post_0"):
        smooth(L0, f0, s["i0"], s["u0"], s["x0a"], s["x0b"], s["d0"], 4)

    land = s["land"]
    r0 = L0.rows
    lane48 = lanes(48) % 64
    inside = (lane48 >= L0.zo) & (lane48 < L0.zo + 48)

    def final(p, row, here_x, applied, kept):
        s["sums"][0, pl.ds((p - L0.e) * r0, r0), :] = f0[4, pl.ds(row, r0), :] - applied
        return kept

    with scope("final"):
        sweep(L0, f0, s["u0"], s["x0b"], 0, final)

    def out_square(i, carry):
        value = jnp.where(inside, s["sums"][0, pl.ds(i * r0 + L0.e, 48), :], 0.0)
        return carry + value * value

    with scope("square"):
        ends = loop(0, 24, out_square, jnp.zeros((48, 128), F32), 4)

    def fold(value):
        return jnp.sum(value, axis=0, keepdims=True)

    def squares_of(value):
        return jnp.sum(fold(value), axis=1, keepdims=True)

    lane1 = lax.broadcasted_iota(jnp.int32, (1, 128), 1)
    pair = jnp.where(lane1 == 0, squares_of(squares), jnp.where(lane1 == 1, squares_of(ends), 0.0))
    own_n[...] = pair
    mine_n = gx * (ny * nz) + me
    gn[mine_n] = pair

    def norm_copy(src, dst, ox, oy, oz):
        return pltpu.make_async_remote_copy(
            src_ref=src,
            dst_ref=dst,
            send_sem=s["all_send"].at[2],
            recv_sem=s["all_recv"].at[2],
            device_id=(ox, oy, oz),
            device_id_type=MESH,
        )

    with scope("norm_start"):
        for t in order:
            for ox in (gx, 1 - gx):
                norm_copy(own_n, gn.at[mine_n], ox, *other(t)).start()
        norm_copy(own_n, gn.at[mine_n], 1 - gx, gy, gz).start()

    def unload(slot, i, value):
        for half in range(2):
            moved = roll_lanes(value, -(L0.zo + 64 * half))
            land[slot, i + 24 * half] = moved[:, 0:48]

    def out_solution(i, carry):
        unload(0, i, s["x0b"][0, pl.ds((L0.e + i) * r0 + L0.e, 48), :])
        return carry

    def out_residual(i, carry):
        unload(1, i, s["sums"][0, pl.ds(i * r0 + L0.e, 48), :])
        return carry

    with scope("unload_solution"):
        loop(0, 24, out_solution, 0, 6)
    out0 = pltpu.make_async_copy(land.at[0], solution_hbm, s["out_sem"].at[0])
    out0.start()
    with scope("unload_residual"):
        loop(0, 24, out_residual, 0, 6)
    out1 = pltpu.make_async_copy(land.at[1], residual_hbm, s["out_sem"].at[1])
    out1.start()
    with scope("norm_finish"):
        most = gn.at[pl.ds(0, 2 * ny * nz - 1)]
        norm_copy(most, most, 1 - gx, gy, gz).wait()
    sums = jnp.sum(gn[...], axis=0)
    norm = jnp.sqrt(sums[:, 1:2] / sums[:, 0:1])
    norm_out[0, 0] = norm[0, 0]
    with scope("out_wait"):
        out0.wait()
        out1.wait()


EXCHANGES = {
    "e0a": (L0, 0, 2),
    "e0b": (L0, 2, 2),
    "e0c": (L0, 4, 1),
    "c1": (L1, 0, 4),
    "c2": (L2, 0, 4),
    "e1": (L1, 4, 1),
    "e2": (L2, 4, 1),
    "x0": (L0, 0, 1),
    "x1": (L1, 0, 1),
    "x2": (L2, 0, 1),
}


def scratch_of(ny, nz):
    vmem = lambda *shape: pltpu.VMEM(shape, F32)
    size = lambda lv: lv.planes * lv.rows
    scratch = {"land": vmem(5, 48, 48, 48), "load_sem": pltpu.SemaphoreType.DMA((5,)), "out_sem": pltpu.SemaphoreType.DMA((2,))}
    for i, lv in enumerate((L0, L1, L2)):
        scratch[f"f{i}"] = vmem(5, size(lv), 128)
        for k in ("i", "d", "u"):
            scratch[f"{k}{i}"] = vmem(1, size(lv), 128)
        scratch[f"x{i}a"] = vmem(1, size(lv), 128)
        scratch[f"x{i}b"] = vmem(1, size(lv), 128)
    scratch["sums"] = vmem(1, 24 * 56, 128)
    scratch["block"] = vmem(5, 128, 128)
    for k in ("own4", "pair4", "merged4"):
        scratch[k] = vmem(4, 8, 128)
    for k in ("own1", "pair1", "merged1"):
        scratch[k] = vmem(8, 128)
    scratch["g4"] = vmem(ny, nz, 4, 8, 128)
    scratch["g1"] = vmem(ny * nz, 8, 128)
    scratch["gn"] = vmem(2 * ny * nz, 1, 128)
    scratch["own_n"] = vmem(1, 128)
    for k in ("pair_send", "pair_recv"):
        scratch[k] = pltpu.SemaphoreType.DMA((4,))
    for k in ("all_send", "all_recv", "coef_send", "coef_recv"):
        scratch[k] = pltpu.SemaphoreType.DMA((3,))
    for k in ("i3", "w3", "d3", "g3"):
        scratch[k] = vmem(ny, 128, 128)
    for k in ("x3a", "x3b"):
        scratch[k] = vmem(ny, 128 + 2 * PAD, 128)
    scratch["c3"] = vmem(6, ny, 128, 128)
    scratch["bottom"] = vmem(7, 64, 128)
    scratch["padded"] = vmem(ny + 2, nz + 2, 8, 128)
    scratch["turned"] = vmem(3, 152, 128)
    scratch["corner"] = vmem(16, 128)
    for k, v in EXCHANGES.items():
        for i, shape in enumerate(Exchange(*v).scratch()):
            scratch[k + str(i)] = shape
    return scratch


def solution(mesh):
    ny, nz = mesh.shape["gy"], mesh.shape["gz"]
    scratch = scratch_of(ny, nz)

    def shards(right_side, face_coef, absorption):
        field = jax.ShapeDtypeStruct((48, 48, 48), F32)
        solved, residual, norm = pl.pallas_call(
            functools.partial(cycle, ny, nz, tuple(scratch)),
            out_shape=(pltpu.VMEM((48, 48, 48), F32), pltpu.VMEM((48, 48, 48), F32), jax.ShapeDtypeStruct((1, 1), F32)),
            in_specs=[pl.BlockSpec(memory_space=pltpu.HBM)] * 3,
            out_specs=(
                pl.BlockSpec(memory_space=pl.ANY),
                pl.BlockSpec(memory_space=pl.ANY),
                pl.BlockSpec(memory_space=pltpu.SMEM),
            ),
            scratch_shapes=list(scratch.values()),
            compiler_params=pltpu.CompilerParams(
                collective_id=0, has_side_effects=True, vmem_limit_bytes=57000 * 1024
            ),
        )(right_side, face_coef, absorption)
        return solved, residual, norm[0, 0]

    in_specs = (P("gx", "gy", "gz"), P(None, "gx", "gy", "gz"), P("gx", "gy", "gz"))
    out_specs = (P("gx", "gy", "gz"), P("gx", "gy", "gz"), P())
    return jax.shard_map(shards, mesh=mesh, in_specs=in_specs, out_specs=out_specs, check_vma=False)
```

```python
import functools

import jax
import jax.numpy as jnp
from jax import lax
from jax.experimental import pallas as pl
from jax.experimental.pallas import tpu as pltpu
from jax.sharding import PartitionSpec as P

BOTTOM = 6
THETA = 1.125
DELTA = 0.875
SIGMA = THETA / DELTA
RHO0 = 1.0 / SIGMA
RHO1 = 1.0 / (2.0 * SIGMA - RHO0)
RHO2 = 1.0 / (2.0 * SIGMA - RHO1)
STEP1 = (RHO1 * RHO0, 2.0 * RHO1 / DELTA)
STEP2 = (RHO2 * RHO1, 2.0 * RHO2 / DELTA)

F32 = jnp.float32
MESH = pl.DeviceIdType.MESH


class Level:
    def __init__(self, n, e, ways, rows, zo, width, width_y, unroll):
        self.n, self.e, self.ways, self.rows, self.zo, self.width = n, e, ways, rows, zo, width
        self.width_y, self.unroll = width_y, unroll
        self.half = n // ways
        self.planes = self.half + 2 * e
        self.span = 128 // ways
        self.slots, self.slots_y = self.span // width, self.span // width_y
        self.packs, self.packs_y = -(-self.half // self.slots), -(-self.half // self.slots_y)


L0 = Level(48, 4, 2, 56, 8, 4, 64, 4)
L1 = Level(24, 6, 2, 40, 16, 8, 32, 4)
L2 = Level(12, 6, 1, 24, 16, 8, 16, 6)


def lanes(rows):
    return lax.broadcasted_iota(jnp.int32, (rows, 128), 1)


def gather_lanes(value, index):
    return jnp.take_along_axis(value, index, axis=1)


def roll_lanes(value, shift):
    return pltpu.roll(value, shift % 128, 1)


def roll_rows(value, shift):
    return pltpu.roll(value, shift % value.shape[0], 0)


def tile_rows(start, size):
    return pl.ds(pl.multiple_of(start, 8), size)


def loop(lo, hi, body, carry, unroll):
    count = (hi - lo) // unroll

    def chunk(i, carry):
        for k in range(unroll):
            carry = body(lo + i * unroll + k, carry)
        return carry

    carry = lax.fori_loop(0, count, chunk, carry)
    for k in range(lo + count * unroll, hi):
        carry = body(k, carry)
    return carry


class Exchange:
    def __init__(self, level, first, count):
        self.level, self.first, self.count = level, first, count
        lv = level
        sizes = [-(-rows // 8) * 8 for rows in (lv.packs_y * lv.e, lv.packs * lv.n, lv.packs * lv.e)]
        self.sizes = [sizes[0]] * 2 + [sizes[1]] * 2 + [sizes[2]] * 4
        self.starts = [sum(self.sizes[:i]) for i in range(9)]

    def scratch(self):
        lv, na = self.level, self.count
        shapes = [
            (na, lv.e * lv.rows, 128),
            (na, self.starts[8], 128),
            (na, self.starts[8], 128),
            (na, self.starts[8], 128),
            (2, na, lv.packs * lv.rows, 128),
        ]
        return [pltpu.VMEM(s, F32) for s in shapes] + [pltpu.SemaphoreType.DMA((2,)), pltpu.SemaphoreType.DMA((2,))]

    def bind(self, here, ref, scratch):
        self.here, self.ref = here, ref
        self.xr, self.out, self.got, self.spare, self.zf, self.ssem, self.rsem = scratch
        gx, gy, gz, ny, nz = here
        lv = self.level
        start = lv.e + (1 - gx) * (lv.half - lv.e if lv.ways == 2 else lv.n - lv.e)

        def copy(src, dst, i, gx, gy, gz):
            return pltpu.make_async_remote_copy(
                src_ref=src,
                dst_ref=dst,
                send_sem=self.ssem.at[i],
                recv_sem=self.rsem.at[i],
                device_id=(gx, gy, gz),
                device_id_type=MESH,
            )

        src = ref.at[pl.ds(self.first, self.count), tile_rows(start * lv.rows, lv.e * lv.rows), :]
        self.copy_x = copy(src, self.xr, 0, 1 - gx, gy, gz)
        ys = [lax.rem(gy + ny - 1, ny), lax.rem(gy + 1, ny)]
        zs = [lax.rem(gz + nz - 1, nz), lax.rem(gz + 1, nz)]
        targets = [(ys[0], gz), (ys[1], gz), (gy, zs[0]), (gy, zs[1])] + [(y, z) for y in ys for z in zs]
        lands = [1, 0, 3, 2, 7, 6, 5, 4]
        self.copies = [
            copy(
                self.out.at[:, pl.ds(self.starts[i], self.sizes[i]), :],
                self.got.at[:, pl.ds(self.starts[lands[i]], self.sizes[i]), :],
                1,
                gx,
                *targets[i],
            )
            for i in range(8)
        ]
        y_side, z_side = [gy > 0, gy < ny - 1], [gz > 0, gz < nz - 1]
        self.exists = y_side + z_side + [a & b for a in y_side for b in z_side]
        self.all = copy(self.out, self.got, 1, gx, *targets[0])
        self.has_y = [jnp.where(gy > 0, 1.0, 0.0).astype(F32), jnp.where(gy < ny - 1, 1.0, 0.0).astype(F32)]
        self.has_z = [jnp.where(gz > 0, 1.0, 0.0).astype(F32), jnp.where(gz < nz - 1, 1.0, 0.0).astype(F32)]
        self.has_x = [gx.astype(F32), (1 - gx).astype(F32)]
        return self

    def send(self, i):
        part = (slice(None), pl.ds(self.starts[i], self.sizes[i]), slice(None))

        @pl.when(self.exists[i])
        def _():
            self.copies[i].start()

        @pl.when(jnp.logical_not(self.exists[i]))
        def _():
            pltpu.make_async_copy(self.out.at[part], self.got.at[part], self.rsem.at[1]).start()
            pltpu.make_async_copy(self.out.at[part], self.spare.at[part], self.ssem.at[1]).start()

    def start_x(self):
        self.copy_x.start()

    def finish_x(self):
        lv, ref = self.level, self.ref
        e, r = lv.e, lv.rows
        self.copy_x.wait()
        low = lanes(r) < 64

        def finish(a, j):
            got = self.xr[a, tile_rows(j * r, r), :]
            if lv.ways == 2:
                got = roll_lanes(got, 64)
                below = roll_lanes(ref[self.first + a, tile_rows((lv.half + j) * r, r), :], 64)
                above = roll_lanes(ref[self.first + a, tile_rows((e + j) * r, r), :], 64)
                below = jnp.where(low, got * self.has_x[0], below)
                above = jnp.where(low, above, got * self.has_x[1])
            else:
                below = got * self.has_x[0]
                above = got * self.has_x[1]
            return below, above

        def body(a, carry):
            for first in range(0, e, 2):
                planes = range(first, min(first + 2, e))
                values = [finish(a, j) for j in planes]
                for j, (below, above) in zip(planes, values):
                    ref[self.first + a, tile_rows(j * r, r), :] = below
                    ref[self.first + a, tile_rows((e + lv.half + j) * r, r), :] = above
            return carry

        lax.fori_loop(0, self.count, body, 0)

    def pack(self, plane, rows, width, shifts, put):
        lv = self.level
        slot = (lanes(rows) % lv.span) // width
        slots = lv.span // width
        for k in range(-(-lv.half // slots)):
            acc = None
            for s in range(min(slots, lv.half - k * slots)):
                moved = [roll_lanes(v, s * width - shift) for v, shift in zip(plane(lv.e + k * slots + s), shifts)]
                acc = moved if s == 0 else [jnp.where(slot == s, new, old) for new, old in zip(moved, acc)]
            put(k, acc)

    def pack_yz(self, send):
        lv, ref = self.level, self.ref
        r, n, e, zo = lv.rows, lv.n, lv.e, lv.zo
        z_shifts = (zo, zo + n - e)

        def put_at(first, rows, a):
            def put(k, values):
                for i, value in enumerate(values):
                    self.out[a, pl.ds(self.starts[first + i] + k * rows, rows), :] = value

            return put

        def edges(a, p):
            return [ref[self.first + a, pl.ds(p * r + row, e), :] for row in (e, n)]

        def pack_d(a, carry):
            def plane(p):
                low, high = edges(a, p)
                return low, low, high, high

            self.pack(plane, e, lv.width, z_shifts * 2, put_at(4, e, a))
            return carry

        def pack_z(a, carry):
            def plane(p):
                return [ref[self.first + a, pl.ds(p * r + e, n), :]] * 2

            self.pack(plane, n, lv.width, z_shifts, put_at(2, n, a))
            return carry

        def pack_y(a, carry):
            if lv.slots_y == 1:
                for k in range(lv.half):
                    put_at(0, e, a)(k, edges(a, e + k))
            else:
                self.pack(lambda p: edges(a, p), e, lv.width_y, (zo, zo), put_at(0, e, a))
            return carry

        for body, which in ((pack_d, range(4, 8)), (pack_z, (2, 3)), (pack_y, (0, 1))):
            lax.fori_loop(0, self.count, body, 0)
            if send:
                for i in which:
                    self.send(i)

    def send_yz(self):
        for i in (4, 5, 6, 7, 2, 3, 0, 1):
            self.send(i)

    def start_yz(self):
        self.pack_yz(True)

    def finish_yz(self):
        lv, ref = self.level, self.ref
        r, n, e, zo = lv.rows, lv.n, lv.e, lv.zo
        with jax.named_scope("arrive"):
            self.all.wait()
        lane = lanes(r) % lv.span
        at_low = (lane >= zo - e) & (lane < zo)
        at_high = (lane >= zo + n) & (lane < zo + n + e)

        def unpack(a, carry):
            def got(i, row, rows):
                return self.got[a, pl.ds(self.starts[i] + row, rows), :]

            for s in range(2):
                for k in range(lv.packs_y):
                    value = got(s, k * e, e) * self.has_y[s]
                    for slot in range(min(lv.slots_y, lv.half - k * lv.slots_y)):
                        row = (e + k * lv.slots_y + slot) * r + (e + n) * s
                        moved = roll_lanes(value, zo - slot * lv.width_y) if lv.slots_y > 1 else value
                        ref[self.first + a, pl.ds(row, e), :] = moved
            for k in range(lv.packs):
                for t in range(2):
                    self.zf[t, a, pl.ds(k * r + e, n), :] = got(2 + t, k * n, n) * self.has_z[t]
                    for s in range(2):
                        both = self.has_y[s] * self.has_z[t]
                        self.zf[t, a, pl.ds(k * r + (e + n) * s, e), :] = got(4 + 2 * s + t, k * e, e) * both
            for k in range(lv.packs):
                sides = [self.zf[t, a, pl.ds(k * r, r), :] for t in range(2)]
                count = min(lv.slots, lv.half - k * lv.slots)
                for first in range(0, count, 4):
                    slots = range(first, min(first + 4, count))
                    values = []
                    for s in slots:
                        value = ref[self.first + a, pl.ds((e + k * lv.slots + s) * r, r), :]
                        value = jnp.where(at_low, roll_lanes(sides[0], zo - e - s * lv.width), value)
                        values.append(jnp.where(at_high, roll_lanes(sides[1], zo + n - s * lv.width), value))
                    for s, value in zip(slots, values):
                        ref[self.first + a, pl.ds((e + k * lv.slots + s) * r, r), :] = value
            return carry

        lax.fori_loop(0, self.count, unpack, 0)


def scaling(lv, fields, inverse, upper, extent):
    r = lv.rows

    def body(p, carry):
        row = pl.multiple_of(p * r, 8)
        cells = fields[3, pl.ds(row, r), :]
        face_z = fields[2, pl.ds(row, r), :]
        total = cells + fields[0, pl.ds(row, r), :] + fields[0, pl.ds(row + r, r), :]
        total = total + fields[1, pl.ds(row, r), :] + fields[1, pl.ds(row + 1, r), :]
        above = roll_lanes(face_z, -1)
        upper[0, pl.ds(row, r), :] = above
        total = total + face_z + above
        inverse[0, pl.ds(row, r), :] = jnp.where(cells > 0.0, 1.0 / total, 0.0)
        return carry

    loop(lv.e - extent, lv.e + lv.half + extent, body, 0, lv.unroll)


def sweep(lv, fields, upper, x, extent, emit, carry=0):
    r = lv.rows
    lo, hi = lv.e - extent, lv.e + lv.half + extent

    def body(p, carry):
        here, flux, kept = carry
        row = pl.multiple_of(p * r, 8)
        after = x[0, pl.ds(row + r, r), :]
        flux_after = fields[0, pl.ds(row + r, r), :] * (after - here)
        flux_y = fields[1, pl.ds(row, r), :] * (here - roll_rows(here, 1))
        flux_y = flux_y - fields[1, pl.ds(row + 1, r), :] * (roll_rows(here, -1) - here)
        flux_z = fields[2, pl.ds(row, r), :] * (here - roll_lanes(here, 1))
        flux_z = flux_z - upper[0, pl.ds(row, r), :] * (roll_lanes(here, -1) - here)
        applied = fields[3, pl.ds(row, r), :] * here + ((flux - flux_after) + flux_y + flux_z)
        return after, flux_after, emit(p, row, here, applied, kept)

    row = lo * r
    here = x[0, pl.ds(row, r), :]
    flux = fields[0, pl.ds(row, r), :] * (here - x[0, pl.ds(row - r, r), :])
    return loop(lo, hi, body, (here, flux, carry), lv.unroll)[2]


def step(lv, fields, inverse, upper, x, out, d, extent, first, coefs, keep):
    r = lv.rows

    def emit(p, row, here, applied, kept):
        scaled = inverse[0, pl.ds(row, r), :] * (fields[4, pl.ds(row, r), :] - applied)
        if first == 0:
            update = scaled * (1.0 / THETA)
        elif first == 1:
            update = coefs[0] * here + coefs[1] * scaled
        else:
            update = coefs[0] * d[0, pl.ds(row, r), :] + coefs[1] * scaled
        if keep:
            d[0, pl.ds(row, r), :] = update
        out[0, pl.ds(row, r), :] = here + update
        return kept

    sweep(lv, fields, upper, x, extent, emit)


def smooth_from_zero(lv, fields, inverse, upper, xa, xb, d, extent):
    r = lv.rows

    def body(p, carry):
        row = pl.multiple_of(p * r, 8)
        xa[0, pl.ds(row, r), :] = inverse[0, pl.ds(row, r), :] * fields[4, pl.ds(row, r), :] * (1.0 / THETA)
        return carry

    loop(lv.e - extent, lv.e + lv.half + extent, body, 0, lv.unroll)
    step(lv, fields, inverse, upper, xa, xb, d, extent - 1, 1, STEP1, True)
    step(lv, fields, inverse, upper, xb, xa, d, extent - 2, 2, STEP2, False)


def smooth(lv, fields, inverse, upper, xa, xb, d, extent):
    step(lv, fields, inverse, upper, xa, xb, d, extent - 1, 0, None, True)
    step(lv, fields, inverse, upper, xb, xa, d, extent - 2, 2, STEP1, True)
    step(lv, fields, inverse, upper, xa, xb, d, extent - 3, 2, STEP2, False)


def coarse_lanes(lv, below, rows, half):
    lane = lanes(rows)
    if below is None:
        cell, at = lane, 0
    else:
        at = (lane // below.span) * 64 if below.ways == 2 else 0
        cell = lane % below.span - below.zo
    if lv.ways == 2 and half is not None:
        at = 64 * half
    inside = (cell >= 0) & (cell < lv.n // 2)
    index = jnp.where(inside, at + lv.zo + 2 * cell, 0)
    return index, inside


def place(lv, below, put, plane, value, pair):
    rows = value.shape[0]
    if pair:
        value = value + roll_lanes(value, -1)
    halves = [None] if below is not None and below.ways == lv.ways else range(lv.ways)
    for half in halves:
        index, inside = coarse_lanes(lv, below, rows, half)
        got = jnp.where(inside, gather_lanes(value, index), 0.0)
        put(plane if half is None else plane + half * (lv.half // 2), got)


def coarsen_fields(lv, below, fields, put):
    n2, e, r = lv.n // 2, lv.e, lv.rows

    def body(i, carry):
        row = (e + 2 * i) * r + e

        def rows(a, plane, odd):
            return fields[a, pl.ds(row + plane * r + odd, n2, stride=2), :]

        put_x = functools.partial(put, 0)
        put_y = functools.partial(put, 1)
        put_z = functools.partial(put, 2)
        put_c = functools.partial(put, 3)
        place(lv, below, put_x, i, (rows(0, 0, 0) + rows(0, 0, 1)) * 0.0625, True)
        place(lv, below, put_y, i, (rows(1, 0, 0) + rows(1, 1, 0)) * 0.0625, True)
        place(lv, below, put_z, i, (rows(2, 0, 0) + rows(2, 0, 1) + rows(2, 1, 0) + rows(2, 1, 1)) * 0.0625, False)
        place(lv, below, put_c, i, (rows(3, 0, 0) + rows(3, 0, 1) + rows(3, 1, 0) + rows(3, 1, 1)) * 0.125, True)
        return carry

    loop(0, lv.half // 2, body, 0, 3)


def restrict(lv, below, fields, upper, x, sums, put):
    r, n2 = lv.rows, lv.n // 2

    def emit(p, row, here, applied, kept):
        sums[0, pl.ds((p - lv.e) * r, r), :] = fields[4, pl.ds(row, r), :] - applied
        return kept

    sweep(lv, fields, upper, x, 0, emit)

    def body(i, carry):
        total = None
        for plane in range(2):
            for odd in range(2):
                part = sums[0, pl.ds((2 * i + plane) * r + lv.e + odd, n2, stride=2), :]
                total = part if total is None else total + part
        place(lv, below, functools.partial(put, 4), i, total * 0.125, True)
        return carry

    loop(0, lv.half // 2, body, 0, 6)


def fields_put(below, fields):
    def put(field, plane, value):
        fields[field, pl.ds((below.e + plane) * below.rows + below.e, below.n), :] = value

    return put


def prolong(lv, above, e, x, reach):
    r, rows = lv.rows, lv.n // 2 + 2 * reach
    lane = lanes(rows)
    cell = lane % 64 - lv.zo + 2 * reach
    inside = (cell >= 0) & (cell < 2 * rows)
    source = above.zo - reach + cell // 2
    if above.ways == 2:
        source = source + (lane // 64) * 64
    source = jnp.where(inside, source, 0)

    def body(i, carry):
        row = (above.e - reach + i) * above.rows + above.e - reach
        value = gather_lanes(e[0, pl.ds(row, rows), :], source)
        if above.ways == 1:
            other = gather_lanes(e[0, pl.ds(row + (lv.half // 2) * above.rows, rows), :], source)
            value = jnp.where(lane < 64, value, other)
        value = jnp.where(inside, value, 0.0)
        for plane in range(2):
            at = (lv.e - 2 * reach + 2 * i + plane) * r + lv.e - 2 * reach
            for odd in range(2):
                where = pl.ds(at + odd, rows, stride=2)
                x[0, where, :] = x[0, where, :] + value
        return carry

    loop(0, lv.half // 2 + 2 * reach, body, 0, 4)


PAD = 8


def row_of(rows):
    return lax.broadcasted_iota(jnp.int32, (rows, 128), 0)


def whole_neighbours(ny, value, rows):
    z, y = row_of(128) % 8, lanes(128) % 6
    out = []
    for g in range(ny):
        here = value(g)
        low_y, high_y = roll_lanes(here, 1), roll_lanes(here, -1)
        if g:
            low_y = jnp.where(y == 0, roll_lanes(value(g - 1), -5), low_y)
        if g + 1 < ny:
            high_y = jnp.where(y == 5, roll_lanes(value(g + 1), 5), high_y)
        low_z = jnp.where(z == 0, rows(g, -3), rows(g, -1))
        high_z = jnp.where(z == 5, rows(g, 3), rows(g, 1))
        out.append((roll_lanes(here, 6), roll_lanes(here, -6), low_y, high_y, low_z, high_z))
    return out


def whole_prepare(ny, fields, coefs, diagonal, inverse):
    z, y, row = row_of(128) % 8, lanes(128) % 6, row_of(128)
    moved = lambda a: whole_neighbours(ny, lambda g: fields(a, g), lambda g, d: roll_rows(fields(a, g), -d))
    high = [[near[1] for near in moved(0)], [near[3] for near in moved(1)], [near[5] for near in moved(2)]]
    for g in range(ny):
        inside = fields(3, g) > 0.0
        high_y = jnp.where(y == 5, 0.0, high[1][g]) if g + 1 == ny else high[1][g]
        high_z = jnp.where(row == 125, 0.0, high[2][g])
        sides = [fields(0, g), high[0][g], fields(1, g), high_y, fields(2, g), high_z]
        total = functools.reduce(lambda a, b: a + b, sides) + fields(3, g)
        scale = jnp.where(inside, 1.0 / total, 0.0)
        diagonal[g] = jnp.where(inside, total, 0.0)
        inverse[g] = scale
        if g == 0:
            sides[2] = jnp.where(y == 0, 0.0, sides[2])
        sides[4] = jnp.where(row == 0, 0.0, sides[4])
        for i in range(6):
            coefs[i, g] = sides[i] * scale


def children(value, axes):
    if "y" in axes:
        value = value + roll_lanes(value, -1)
    if "x" in axes:
        value = value + roll_lanes(value, -6)
    if "z" in axes:
        value = value + roll_rows(value, -1)
    return value


def even_cells():
    row, lane = row_of(128), lanes(128)
    return (row % 2 == 0) & (row % 8 < 6) & (lane % 2 == 0) & ((lane // 6) % 2 == 0) & (lane < 72)


def fold_level(values):
    even = even_cells()
    values = [jnp.where(even, v, 0.0) for v in values]
    both = (values[0] + roll_lanes(values[1], 1)) + (roll_lanes(values[2], 6) + roll_lanes(values[3], 7))
    return both[0:64] + roll_rows(both[64:128], 1)


def unfold_level(value):
    both = jnp.concatenate([value, roll_rows(value, -1)], axis=0)
    even = even_cells()
    return [jnp.where(even, roll_lanes(both, -shift), 0.0) for shift in (0, 1, 6, 7)]


def bottom_neighbours(v):
    row, lane = row_of(64), lanes(64)
    z, y = (row % 8) // 2, (lane % 6) // 2
    odd = lane % 2 == 1
    low_y = jnp.where(y > 0, roll_lanes(v, 2), jnp.where(odd, roll_lanes(v, -3), roll_lanes(v, 1)))
    high_y = jnp.where(y < 2, roll_lanes(v, -2), jnp.where(odd, roll_lanes(v, -1), roll_lanes(v, 3)))
    low_z = jnp.where(z > 0, roll_rows(v, 2), jnp.where(row == 1, roll_rows(v, 5), roll_rows(v, 4)))
    high_z = jnp.where(z < 2, roll_rows(v, -2), jnp.where(row == 60, roll_rows(v, -5), roll_rows(v, -4)))
    return roll_lanes(v, 12), roll_lanes(v, -12), low_y, high_y, low_z, high_z


def bottom_prepare(ny, fields, bottom):
    row, lane = row_of(64), lanes(64)
    y = (lane % 6) // 2
    first = (lane % 2 == 0) & ((lane // 6) % 2 == 0)
    last = (lane % 2 == 1) & ((lane // 6) % 2 == 1)
    faces = []
    for a, axes in enumerate(("yz", "xz", "xy", "xyz")):
        factor = 0.125 if a == 3 else 0.0625
        faces.append(fold_level([children(fields(a, g), axes) * factor for g in range(ny)]))
    inside = faces[3] > 0.0
    high_x = bottom_neighbours(faces[0])[1]
    high_y = jnp.where(last & (y == 2), 0.0, bottom_neighbours(faces[1])[3])
    high_z = jnp.where(row == 61, 0.0, bottom_neighbours(faces[2])[5])
    sides = [faces[0], high_x, faces[1], high_y, faces[2], high_z]
    total = functools.reduce(lambda a, b: a + b, sides) + faces[3]
    sides[2] = jnp.where(first & (y == 0), 0.0, sides[2])
    sides[4] = jnp.where(row == 0, 0.0, sides[4])
    for i, value in enumerate(sides + [total]):
        bottom[i] = jnp.where(inside, value, 0.0)


def coarse_solve(ny, coefs, diagonal, inverse, f, bottom, xa, xb, ds, g3):
    def rows(x, g, offset=0):
        return x[g, pl.ds(PAD + offset, 128)]

    def scaled(x):
        near = whole_neighbours(ny, lambda g: rows(x, g), lambda g, d: rows(x, g, d))
        out = []
        for g in range(ny):
            parts = [coefs[i, g] * near[g][i] for i in range(6)]
            total = ((parts[0] + parts[1]) + (parts[2] + parts[3])) + (parts[4] + parts[5])
            out.append((g3[g] - rows(x, g)) + total)
        return out

    def advance(x, to, coef, first, keep=True):
        for g, value in enumerate(scaled(x)):
            update = value * (1.0 / THETA) if first else coef[0] * ds[g] + coef[1] * value
            if keep:
                ds[g] = update
            to[g, pl.ds(PAD, 128)] = rows(x, g) + update

    for x in (xa, xb):
        for g in range(ny):
            x[g, pl.ds(0, PAD)] = jnp.zeros((PAD, 128), F32)
            x[g, pl.ds(PAD + 128, PAD)] = jnp.zeros((PAD, 128), F32)
    for g in range(ny):
        g3[g] = inverse[g] * f(g)
        ds[g] = g3[g] * (1.0 / THETA)
        xa[g, pl.ds(PAD, 128)] = ds[g]
    advance(xa, xb, STEP1, False)
    advance(xb, xa, STEP2, False, False)
    remainder = scaled(xa)
    r = fold_level([children(remainder[g] * diagonal[g], "xyz") * 0.125 for g in range(ny)])
    r = jnp.where(bottom[6] > 0.0, r, 0.0)

    def total(value):
        value = jnp.sum(value.reshape(8, 8, 128), axis=0)
        return jnp.sum(jnp.sum(value, axis=1, keepdims=True), axis=0, keepdims=True)

    def applied(v):
        near = bottom_neighbours(v)
        parts = [bottom[i] * near[i] for i in range(6)]
        return bottom[6] * v - (((parts[0] + parts[1]) + (parts[2] + parts[3])) + (parts[4] + parts[5]))

    e = jnp.zeros((64, 128), F32)
    p, norm = r, total(r * r)
    for i in range(BOTTOM):
        q = applied(p)
        size = norm / total(p * q)
        e = e + size * p
        if i + 1 < BOTTOM:
            r = r - size * q
            after = total(r * r)
            p = r + after / norm * p
            norm = after
    for g, value in enumerate(unfold_level(e)):
        value = value + roll_lanes(value, 1)
        value = value + roll_lanes(value, 6)
        xa[g, pl.ds(PAD, 128)] = rows(xa, g) + (value + roll_rows(value, 1))
    advance(xa, xb, None, True)
    advance(xb, xa, STEP1, False)
    advance(xa, xb, STEP2, False, False)


def window(lv, gx, gy, gz, ny, xs, padded, turned, corner, x):
    nz = 16
    padded[...] = jnp.zeros_like(padded)
    for g in range(ny):
        padded[g + 1, pl.ds(1, nz)] = xs[g, pl.ds(PAD, 128)].reshape(nz, 8, 128)
    for dy in range(3):
        tiles = padded[gy + dy, pl.ds(gz, 3)].reshape(24, 128)
        tiles = jnp.concatenate([tiles, jnp.zeros((104, 128), F32)], axis=0)
        turned[dy, pl.ds(0, 24), :] = jnp.zeros((24, 128), F32)
        turned[dy, pl.ds(24, 128), :] = tiles.T
    lane = lanes(16)
    cell = lane - lv.zo + 6
    inside = (cell >= 0) & (cell < 24)
    coarse = jnp.where(inside, cell // 2 + 3, 0)
    source = (coarse // 6) * 8 + coarse % 6

    def body(i, carry):
        base = 6 + 36 * gx + 6 * i
        corner[pl.ds(0, 3), :] = turned[0, pl.ds(base + 3, 3), :]
        corner[pl.ds(3, 6), :] = turned[1, pl.ds(base, 6), :]
        corner[pl.ds(9, 3), :] = turned[2, pl.ds(base, 3), :]
        value = jnp.where(inside, gather_lanes(corner[...], source), 0.0)[0:12]
        for plane in range(2):
            at = (lv.e - 6 + 2 * i + plane) * lv.rows + lv.e - 6
            for odd in range(2):
                where = pl.ds(at + odd, 12, stride=2)
                x[0, where, :] = x[0, where, :] + value
        return carry

    loop(0, 12, body, 0, 4)


def hops(t, nz):
    return sum(min(d, 4 - d) for d in (t // nz % 4, t % nz // 4, t % 4))


def cycle(ny, nz, names, *refs):
    refs = list(refs)
    right_hbm, faces_hbm, cells_hbm, solution_hbm, residual_hbm, norm_out = refs[:6]
    s = dict(zip(names, refs[6:]))
    gx, gy, gz = lax.axis_index("gx"), lax.axis_index("gy"), lax.axis_index("gz")
    here = (gx, gy, gz, ny, nz)
    scope = jax.named_scope

    loads = [pltpu.make_async_copy(faces_hbm.at[d], s["land"].at[d], s["load_sem"].at[d]) for d in range(3)]
    loads.append(pltpu.make_async_copy(cells_hbm, s["land"].at[3], s["load_sem"].at[3]))
    loads.append(pltpu.make_async_copy(right_hbm, s["land"].at[4], s["load_sem"].at[4]))
    for copy in loads:
        copy.start()

    def other(t):
        return lax.rem(gy + t // nz, ny), lax.rem(gz + t % nz, nz)

    order = sorted(range(1, ny * nz), key=lambda t: -hops(t, nz))
    barrier = pltpu.get_barrier_semaphore()
    with scope("greet"):
        for t in order:
            oy, oz = other(t)
            for ox in (gx, 1 - gx):
                pl.semaphore_signal(barrier, inc=1, device_id=(ox, oy, oz), device_id_type=MESH)
        pl.semaphore_signal(barrier, inc=1, device_id=(1 - gx, gy, gz), device_id_type=MESH)

    f0, f1, f2 = s["f0"], s["f1"], s["f2"]
    ex = {k: Exchange(*v) for k, v in EXCHANGES.items()}
    targets = {"e0a": f0, "e0b": f0, "e0c": f0, "c1": f1, "c2": f2, "e1": f1, "e2": f2, "x0": s["x0a"], "x1": s["x1a"], "x2": s["x2a"]}
    for k, target in targets.items():
        ex[k].bind(here, target, [s[k + str(i)] for i in range(7)])

    def partner(src, dst, i):
        return pltpu.make_async_remote_copy(
            src_ref=src,
            dst_ref=dst,
            send_sem=s["pair_send"].at[i],
            recv_sem=s["pair_recv"].at[i],
            device_id=(1 - gx, gy, gz),
            device_id_type=MESH,
        )

    me = gy * nz + gz

    def spread(src, whole, i):
        def copy(src, dst, oy, oz):
            return pltpu.make_async_remote_copy(
                src_ref=src,
                dst_ref=dst,
                send_sem=s["all_send"].at[i],
                recv_sem=s["all_recv"].at[i],
                device_id=(gx, oy, oz),
                device_id_type=MESH,
            )

        def start():
            for t in order:
                copy(src, whole.at[me], *other(t)).start()

        def finish():
            most = whole.at[pl.ds(0, ny * nz - 1)]
            copy(most, most, *other(1)).wait()

        return start, finish

    block = s["block"]

    def block_put(field, plane, value):
        block[field, pl.ds(plane * 6, 6), :] = value

    for a in range(5):
        with scope("load_wait"):
            loads[a].wait()

        def load(i, carry, a=a):
            first = jnp.pad(s["land"][a, i], ((0, 0), (0, 80)))
            second = jnp.pad(s["land"][a, i + 24], ((0, 0), (0, 80)))
            value = roll_lanes(first, L0.zo) + roll_lanes(second, 64 + L0.zo)
            f0[a, pl.ds((L0.e + i) * L0.rows + L0.e, 48), :] = value
            return carry

        with scope("layout"):
            loop(0, 24, load, 0, 12)

    with scope("e0_pack"):
        ex["e0a"].pack_yz(False)
    with scope("barrier"):
        pl.semaphore_wait(barrier, 2 * ny * nz - 1)
    ex["e0a"].send_yz()
    with scope("e0_start_yz"):
        ex["e0b"].start_yz()
        ex["e0c"].start_yz()
    f1[...] = jnp.zeros_like(f1)
    f2[...] = jnp.zeros_like(f2)
    block[...] = jnp.zeros_like(block)
    with scope("coarsen_0"):
        coarsen_fields(L0, L1, f0, fields_put(L1, f1))
    with scope("c1_pack"):
        ex["c1"].pack_yz(False)
    with scope("coarsen_1"):
        coarsen_fields(L1, L2, f1, fields_put(L2, f2))
    with scope("c2_pack"):
        ex["c2"].pack_yz(False)
    with scope("coarsen_2"):
        coarsen_fields(L2, None, f2, block_put)

    def tile_of(field):
        return roll_lanes(block[field].T[0:8], gx * 36)

    own4, pair4, own1, pair1, own_n = (s[k] for k in ("own4", "pair4", "own1", "pair1", "own_n"))
    for field in range(4):
        own4[field] = tile_of(field)
    pair_coef = partner(own4, pair4, 0)
    pair_coef.start()

    def square(i, carry):
        value = f0[4, pl.ds((L0.e + i) * L0.rows + L0.e, 48), :]
        return carry + value * value

    with scope("square"):
        squares = loop(0, 24, square, jnp.zeros((48, 128), F32), 4)
    for k in ("e0a", "e0b", "e0c"):
        with scope(k + "_finish_yz"):
            ex[k].finish_yz()
        ex[k].start_x()
    ex["c1"].send_yz()
    g4, g1, gn = s["g4"], s["g1"], s["gn"]
    with scope("pair_coef"):
        pair_coef.wait()
    merged = s["merged4"]
    merged[...] = own4[...] + pair4[...]
    mine = pl.ds(2 * gx, 2)
    g4[gy, gz, mine] = merged[mine]
    row, column = gz // 4, gz % 4

    def coef_part(stage):
        if stage == 0:
            return g4.at[gy, gz, mine]
        if stage == 1:
            return g4.at[:, gz, mine]
        return g4.at[:, pl.ds(4 * row, 4), mine]

    def coef_copy(stage, src, oy, oz):
        return pltpu.make_async_remote_copy(
            src_ref=src,
            dst_ref=src,
            send_sem=s["coef_send"].at[stage],
            recv_sem=s["coef_recv"].at[stage],
            device_id=(gx, oy, oz),
            device_id_type=MESH,
        )

    def coef_start(stage):
        for d in (2, 1, 3):
            oy, oz = gy, gz
            if stage == 0:
                oy = lax.rem(gy + d, ny)
            elif stage == 1:
                oz = 4 * row + lax.rem(column + d, 4)
            else:
                oz = lax.rem(gz + 4 * d, nz)
            coef_copy(stage, coef_part(stage), oy, oz).start()

    def coef_wait(stage):
        two = pl.ds(0, 2)
        most = (g4.at[pl.ds(0, 3), 0, two], g4.at[:, pl.ds(0, 3), two], g4.at[:, pl.ds(0, 12), two])[stage]
        coef_copy(stage, most, lax.rem(gy + 1, ny), gz).wait()

    with scope("coef_0"):
        coef_start(0)
    with scope("e0_finish_x"):
        ex["e0a"].finish_x()
        ex["e0b"].finish_x()
    with scope("scaling_0"):
        scaling(L0, f0, s["i0"], s["u0"], 3)
    with scope("e0c_finish_x"):
        ex["e0c"].finish_x()
    with scope("smooth_0"):
        smooth_from_zero(L0, f0, s["i0"], s["u0"], s["x0a"], s["x0b"], s["d0"], 3)
    with scope("restrict_0"):
        restrict(L0, L1, f0, s["u0"], s["x0a"], s["sums"], fields_put(L1, f1))
    with scope("e1_start_yz"):
        ex["e1"].start_yz()
    ex["c2"].send_yz()
    with scope("c1_finish_yz"):
        ex["c1"].finish_yz()
    ex["c1"].start_x()
    with scope("coef_1"):
        coef_wait(0)
        coef_start(1)
    with scope("x0_start_yz"):
        ex["x0"].start_yz()
    with scope("c1_finish_x"):
        ex["c1"].finish_x()
    with scope("scaling_1"):
        scaling(L1, f1, s["i1"], s["u1"], 4)
    with scope("e1_finish_yz"):
        ex["e1"].finish_yz()
    ex["e1"].start_x()
    with scope("e1_finish_x"):
        ex["e1"].finish_x()
    with scope("coef_2"):
        coef_wait(1)
        coef_start(2)
    with scope("smooth_1"):
        smooth_from_zero(L1, f1, s["i1"], s["u1"], s["x1a"], s["x1b"], s["d1"], 3)
    with scope("restrict_1"):
        restrict(L1, L2, f1, s["u1"], s["x1a"], s["sums"], fields_put(L2, f2))
    with scope("e2_start_yz"):
        ex["e2"].start_yz()
    with scope("c2_finish_yz"):
        ex["c2"].finish_yz()
    ex["c2"].start_x()
    with scope("x1_start_yz"):
        ex["x1"].start_yz()
    with scope("c2_finish_x"):
        ex["c2"].finish_x()
    with scope("scaling_2"):
        scaling(L2, f2, s["i2"], s["u2"], 5)
    other_half = pltpu.make_async_remote_copy(
        src_ref=g4.at[:, :, mine],
        dst_ref=g4.at[:, :, mine],
        send_sem=s["pair_send"].at[3],
        recv_sem=s["pair_recv"].at[3],
        device_id=(1 - gx, gy, gz),
        device_id_type=MESH,
    )
    with scope("e2_finish_yz"):
        ex["e2"].finish_yz()
    ex["e2"].start_x()
    with scope("x0_finish_yz"):
        ex["x0"].finish_yz()
    with scope("e2_finish_x"):
        ex["e2"].finish_x()
    with scope("smooth_2"):
        smooth_from_zero(L2, f2, s["i2"], s["u2"], s["x2a"], s["x2b"], s["d2"], 3)
    with scope("restrict_2"):
        restrict(L2, None, f2, s["u2"], s["x2a"], s["sums"], block_put)
    own1[...] = tile_of(4)
    pair_source = partner(own1, pair1, 1)
    pair_source.start()
    ex["x0"].start_x()
    with scope("x2_start_yz"):
        ex["x2"].start_yz()
    with scope("pair_source"):
        pair_source.wait()
    s["merged1"][...] = own1[...] + pair1[...]
    g1[me] = s["merged1"][...]
    source_start, source_finish = spread(s["merged1"], g1, 1)
    with scope("source_start"):
        source_start()
    with scope("coef_finish"):
        coef_wait(2)
    other_half.start()
    with scope("hidden_1"):
        ex["x1"].finish_yz()
        ex["x1"].start_x()
        ex["x0"].finish_x()
    with scope("other_half"):
        other_half.wait()
    gathered = lambda a, g: g4[g, :, a].reshape(128, 128)
    with scope("coarse_fields"):
        whole_prepare(ny, gathered, s["c3"], s["w3"], s["i3"])
        bottom_prepare(ny, gathered, s["bottom"])
    with scope("hidden_2"):
        ex["x1"].finish_x()
        ex["x2"].finish_yz()
        ex["x2"].start_x()
    with scope("source_finish"):
        source_finish()
    with scope("coarse_solve"):
        source = lambda g: g1[pl.ds(g * nz, nz)].reshape(128, 128)
        whole = [s[k] for k in ("c3", "w3", "i3")]
        coarse_solve(ny, *whole, source, s["bottom"], s["x3a"], s["x3b"], s["d3"], s["g3"])
    with scope("x2_finish_x"):
        ex["x2"].finish_x()
    with scope("window"):
        window(L2, gx, gy, gz, ny, s["x3b"], s["padded"], s["turned"], s["corner"], s["x2a"])
    with scope("post_2"):
        smooth(L2, f2, s["i2"], s["u2"], s["x2a"], s["x2b"], s["d2"], 6)
    with scope("prolong_1"):
        prolong(L1, L2, s["x2b"], s["x1a"], 3)
    with scope("post_1"):
        smooth(L1, f1, s["i1"], s["u1"], s["x1a"], s["x1b"], s["d1"], 5)
    with scope("prolong_0"):
        prolong(L0, L1, s["x1b"], s["x0a"], 2)
    with scope("post_0"):
        smooth(L0, f0, s["i0"], s["u0"], s["x0a"], s["x0b"], s["d0"], 4)

    land = s["land"]
    r0 = L0.rows
    lane48 = lanes(48) % 64
    inside = (lane48 >= L0.zo) & (lane48 < L0.zo + 48)

    def final(p, row, here_x, applied, kept):
        s["sums"][0, pl.ds((p - L0.e) * r0, r0), :] = f0[4, pl.ds(row, r0), :] - applied
        return kept

    with scope("final"):
        sweep(L0, f0, s["u0"], s["x0b"], 0, final)

    def out_square(i, carry):
        value = jnp.where(inside, s["sums"][0, pl.ds(i * r0 + L0.e, 48), :], 0.0)
        return carry + value * value

    with scope("square"):
        ends = loop(0, 24, out_square, jnp.zeros((48, 128), F32), 4)

    def fold(value):
        return jnp.sum(value, axis=0, keepdims=True)

    def squares_of(value):
        return jnp.sum(fold(value), axis=1, keepdims=True)

    lane1 = lax.broadcasted_iota(jnp.int32, (1, 128), 1)
    pair = jnp.where(lane1 == 0, squares_of(squares), jnp.where(lane1 == 1, squares_of(ends), 0.0))
    own_n[...] = pair
    mine_n = gx * (ny * nz) + me
    gn[mine_n] = pair

    def norm_copy(src, dst, ox, oy, oz):
        return pltpu.make_async_remote_copy(
            src_ref=src,
            dst_ref=dst,
            send_sem=s["all_send"].at[2],
            recv_sem=s["all_recv"].at[2],
            device_id=(ox, oy, oz),
            device_id_type=MESH,
        )

    with scope("norm_start"):
        for t in order:
            for ox in (gx, 1 - gx):
                norm_copy(own_n, gn.at[mine_n], ox, *other(t)).start()
        norm_copy(own_n, gn.at[mine_n], 1 - gx, gy, gz).start()

    def unload(slot, i, value):
        for half in range(2):
            moved = roll_lanes(value, -(L0.zo + 64 * half))
            land[slot, i + 24 * half] = moved[:, 0:48]

    def out_solution(i, carry):
        unload(0, i, s["x0b"][0, pl.ds((L0.e + i) * r0 + L0.e, 48), :])
        return carry

    def out_residual(i, carry):
        unload(1, i, s["sums"][0, pl.ds(i * r0 + L0.e, 48), :])
        return carry

    with scope("unload_solution"):
        loop(0, 24, out_solution, 0, 6)
    out0 = pltpu.make_async_copy(land.at[0], solution_hbm, s["out_sem"].at[0])
    out0.start()
    with scope("unload_residual"):
        loop(0, 24, out_residual, 0, 6)
    out1 = pltpu.make_async_copy(land.at[1], residual_hbm, s["out_sem"].at[1])
    out1.start()
    with scope("norm_finish"):
        most = gn.at[pl.ds(0, 2 * ny * nz - 1)]
        norm_copy(most, most, 1 - gx, gy, gz).wait()
    sums = jnp.sum(gn[...], axis=0)
    norm = jnp.sqrt(sums[:, 1:2] / sums[:, 0:1])
    norm_out[0, 0] = norm[0, 0]
    with scope("out_wait"):
        out0.wait()
        out1.wait()


EXCHANGES = {
    "e0a": (L0, 0, 2),
    "e0b": (L0, 2, 2),
    "e0c": (L0, 4, 1),
    "c1": (L1, 0, 4),
    "c2": (L2, 0, 4),
    "e1": (L1, 4, 1),
    "e2": (L2, 4, 1),
    "x0": (L0, 0, 1),
    "x1": (L1, 0, 1),
    "x2": (L2, 0, 1),
}


def scratch_of(ny, nz):
    vmem = lambda *shape: pltpu.VMEM(shape, F32)
    size = lambda lv: lv.planes * lv.rows
    scratch = {"land": vmem(5, 48, 48, 48), "load_sem": pltpu.SemaphoreType.DMA((5,)), "out_sem": pltpu.SemaphoreType.DMA((2,))}
    for i, lv in enumerate((L0, L1, L2)):
        scratch[f"f{i}"] = vmem(5, size(lv), 128)
        for k in ("i", "d", "u"):
            scratch[f"{k}{i}"] = vmem(1, size(lv), 128)
        scratch[f"x{i}a"] = vmem(1, size(lv), 128)
        scratch[f"x{i}b"] = vmem(1, size(lv), 128)
    scratch["sums"] = vmem(1, 24 * 56, 128)
    scratch["block"] = vmem(5, 128, 128)
    for k in ("own4", "pair4", "merged4"):
        scratch[k] = vmem(4, 8, 128)
    for k in ("own1", "pair1", "merged1"):
        scratch[k] = vmem(8, 128)
    scratch["g4"] = vmem(ny, nz, 4, 8, 128)
    scratch["g1"] = vmem(ny * nz, 8, 128)
    scratch["gn"] = vmem(2 * ny * nz, 1, 128)
    scratch["own_n"] = vmem(1, 128)
    for k in ("pair_send", "pair_recv"):
        scratch[k] = pltpu.SemaphoreType.DMA((4,))
    for k in ("all_send", "all_recv", "coef_send", "coef_recv"):
        scratch[k] = pltpu.SemaphoreType.DMA((3,))
    for k in ("i3", "w3", "d3", "g3"):
        scratch[k] = vmem(ny, 128, 128)
    for k in ("x3a", "x3b"):
        scratch[k] = vmem(ny, 128 + 2 * PAD, 128)
    scratch["c3"] = vmem(6, ny, 128, 128)
    scratch["bottom"] = vmem(7, 64, 128)
    scratch["padded"] = vmem(ny + 2, nz + 2, 8, 128)
    scratch["turned"] = vmem(3, 152, 128)
    scratch["corner"] = vmem(16, 128)
    for k, v in EXCHANGES.items():
        for i, shape in enumerate(Exchange(*v).scratch()):
            scratch[k + str(i)] = shape
    return scratch


def solution(mesh):
    ny, nz = mesh.shape["gy"], mesh.shape["gz"]
    scratch = scratch_of(ny, nz)

    def shards(right_side, face_coef, absorption):
        field = jax.ShapeDtypeStruct((48, 48, 48), F32)
        solved, residual, norm = pl.pallas_call(
            functools.partial(cycle, ny, nz, tuple(scratch)),
            out_shape=(pltpu.VMEM((48, 48, 48), F32), pltpu.VMEM((48, 48, 48), F32), jax.ShapeDtypeStruct((1, 1), F32)),
            in_specs=[pl.BlockSpec(memory_space=pltpu.HBM)] * 3,
            out_specs=(
                pl.BlockSpec(memory_space=pl.ANY),
                pl.BlockSpec(memory_space=pl.ANY),
                pl.BlockSpec(memory_space=pltpu.SMEM),
            ),
            scratch_shapes=list(scratch.values()),
            compiler_params=pltpu.CompilerParams(
                collective_id=0, has_side_effects=True, vmem_limit_bytes=57000 * 1024
            ),
        )(right_side, face_coef, absorption)
        return solved, residual, norm[0, 0]

    in_specs = (P("gx", "gy", "gz"), P(None, "gx", "gy", "gz"), P("gx", "gy", "gz"))
    out_specs = (P("gx", "gy", "gz"), P("gx", "gy", "gz"), P())
    return jax.shard_map(shards, mesh=mesh, in_specs=in_specs, out_specs=out_specs, check_vma=False)
```

```python
import functools

import jax
import jax.numpy as jnp
from jax import lax
from jax.experimental import pallas as pl
from jax.experimental.pallas import tpu as pltpu
from jax.sharding import PartitionSpec as P

BOTTOM = 6
THETA = 1.125
DELTA = 0.875
SIGMA = THETA / DELTA
RHO0 = 1.0 / SIGMA
RHO1 = 1.0 / (2.0 * SIGMA - RHO0)
RHO2 = 1.0 / (2.0 * SIGMA - RHO1)
STEP1 = (RHO1 * RHO0, 2.0 * RHO1 / DELTA)
STEP2 = (RHO2 * RHO1, 2.0 * RHO2 / DELTA)

F32 = jnp.float32
MESH = pl.DeviceIdType.MESH


class Level:
    def __init__(self, n, e, ways, rows, zo, width, width_y, unroll):
        self.n, self.e, self.ways, self.rows, self.zo, self.width = n, e, ways, rows, zo, width
        self.width_y, self.unroll = width_y, unroll
        self.half = n // ways
        self.planes = self.half + 2 * e
        self.span = 128 // ways
        self.slots, self.slots_y = self.span // width, self.span // width_y
        self.packs, self.packs_y = -(-self.half // self.slots), -(-self.half // self.slots_y)


L0 = Level(48, 4, 2, 56, 8, 4, 64, 4)
L1 = Level(24, 6, 2, 40, 16, 8, 32, 4)
L2 = Level(12, 6, 1, 24, 16, 8, 16, 6)


def lanes(rows):
    return lax.broadcasted_iota(jnp.int32, (rows, 128), 1)


def gather_lanes(value, index):
    return jnp.take_along_axis(value, index, axis=1)


def roll_lanes(value, shift):
    return pltpu.roll(value, shift % 128, 1)


def roll_rows(value, shift):
    return pltpu.roll(value, shift % value.shape[0], 0)


def tile_rows(start, size):
    return pl.ds(pl.multiple_of(start, 8), size)


def loop(lo, hi, body, carry, unroll):
    count = (hi - lo) // unroll

    def chunk(i, carry):
        for k in range(unroll):
            carry = body(lo + i * unroll + k, carry)
        return carry

    carry = lax.fori_loop(0, count, chunk, carry)
    for k in range(lo + count * unroll, hi):
        carry = body(k, carry)
    return carry


class Exchange:
    def __init__(self, level, first, count):
        self.level, self.first, self.count = level, first, count
        lv = level
        sizes = [-(-rows // 8) * 8 for rows in (lv.packs_y * lv.e, lv.packs * lv.n, lv.packs * lv.e)]
        self.sizes = [sizes[0]] * 2 + [sizes[1]] * 2 + [sizes[2]] * 4
        self.starts = [sum(self.sizes[:i]) for i in range(9)]

    def scratch(self):
        lv, na = self.level, self.count
        shapes = [
            (na, lv.e * lv.rows, 128),
            (na, self.starts[8] + 8, 128),
            (na, self.starts[8] + 8, 128),
            (na, self.starts[8] + 8, 128),
            (2, na, lv.packs * lv.rows + 8, 128),
        ]
        return [pltpu.VMEM(s, F32) for s in shapes] + [pltpu.SemaphoreType.DMA((2,)), pltpu.SemaphoreType.DMA((2,))]

    def bind(self, here, ref, scratch):
        self.here, self.ref = here, ref
        self.xr, self.out, self.got, self.spare, self.zf, self.ssem, self.rsem = scratch
        gx, gy, gz, ny, nz = here
        lv = self.level
        start = lv.e + (1 - gx) * (lv.half - lv.e if lv.ways == 2 else lv.n - lv.e)

        def copy(src, dst, i, gx, gy, gz):
            return pltpu.make_async_remote_copy(
                src_ref=src,
                dst_ref=dst,
                send_sem=self.ssem.at[i],
                recv_sem=self.rsem.at[i],
                device_id=(gx, gy, gz),
                device_id_type=MESH,
            )

        src = ref.at[pl.ds(self.first, self.count), tile_rows(start * lv.rows, lv.e * lv.rows), :]
        self.copy_x = copy(src, self.xr, 0, 1 - gx, gy, gz)
        ys = [lax.rem(gy + ny - 1, ny), lax.rem(gy + 1, ny)]
        zs = [lax.rem(gz + nz - 1, nz), lax.rem(gz + 1, nz)]
        targets = [(ys[0], gz), (ys[1], gz), (gy, zs[0]), (gy, zs[1])] + [(y, z) for y in ys for z in zs]
        lands = [1, 0, 3, 2, 7, 6, 5, 4]
        self.copies = [
            copy(
                self.out.at[:, pl.ds(self.starts[i], self.sizes[i]), :],
                self.got.at[:, pl.ds(self.starts[lands[i]], self.sizes[i]), :],
                1,
                gx,
                *targets[i],
            )
            for i in range(8)
        ]
        y_side, z_side = [gy > 0, gy < ny - 1], [gz > 0, gz < nz - 1]
        self.exists = y_side + z_side + [a & b for a in y_side for b in z_side]
        whole = pl.ds(0, self.starts[8])
        self.all = copy(self.out.at[:, whole, :], self.got.at[:, whole, :], 1, gx, *targets[0])
        self.has_y = [jnp.where(gy > 0, 1.0, 0.0).astype(F32), jnp.where(gy < ny - 1, 1.0, 0.0).astype(F32)]
        self.has_z = [jnp.where(gz > 0, 1.0, 0.0).astype(F32), jnp.where(gz < nz - 1, 1.0, 0.0).astype(F32)]
        self.has_x = [gx.astype(F32), (1 - gx).astype(F32)]
        return self

    def send(self, i):
        part = (slice(None), pl.ds(self.starts[i], self.sizes[i]), slice(None))

        @pl.when(self.exists[i])
        def _():
            self.copies[i].start()

        @pl.when(jnp.logical_not(self.exists[i]))
        def _():
            pltpu.make_async_copy(self.out.at[part], self.got.at[part], self.rsem.at[1]).start()
            pltpu.make_async_copy(self.out.at[part], self.spare.at[part], self.ssem.at[1]).start()

    def start_x(self):
        self.copy_x.start()

    def finish_x(self):
        lv, ref = self.level, self.ref
        e, r = lv.e, lv.rows
        self.copy_x.wait()
        low = lanes(r) < 64

        def finish(a, j):
            got = self.xr[a, tile_rows(j * r, r), :]
            if lv.ways == 2:
                got = roll_lanes(got, 64)
                below = roll_lanes(ref[self.first + a, tile_rows((lv.half + j) * r, r), :], 64)
                above = roll_lanes(ref[self.first + a, tile_rows((e + j) * r, r), :], 64)
                below = jnp.where(low, got * self.has_x[0], below)
                above = jnp.where(low, above, got * self.has_x[1])
            else:
                below = got * self.has_x[0]
                above = got * self.has_x[1]
            return below, above

        def body(a, carry):
            for first in range(0, e, 2):
                planes = range(first, min(first + 2, e))
                values = [finish(a, j) for j in planes]
                for j, (below, above) in zip(planes, values):
                    ref[self.first + a, tile_rows(j * r, r), :] = below
                    ref[self.first + a, tile_rows((e + lv.half + j) * r, r), :] = above
            return carry

        lax.fori_loop(0, self.count, body, 0)

    def pack(self, plane, rows, width, shifts, put):
        lv = self.level
        slot = (lanes(rows) % lv.span) // width
        slots = lv.span // width
        for k in range(-(-lv.half // slots)):
            acc = None
            for s in range(min(slots, lv.half - k * slots)):
                moved = [roll_lanes(v, s * width - shift) for v, shift in zip(plane(lv.e + k * slots + s), shifts)]
                acc = moved if s == 0 else [jnp.where(slot == s, new, old) for new, old in zip(moved, acc)]
            put(k, acc)

    def pack_yz(self, send):
        lv, ref = self.level, self.ref
        r, n, e, zo = lv.rows, lv.n, lv.e, lv.zo
        z_shifts = (zo, zo + n - e)

        def put_at(first, rows, a):
            def put(k, values):
                for i, value in enumerate(values):
                    self.out[a, pl.ds(self.starts[first + i] + k * rows, rows), :] = value

            return put

        def edges(a, p):
            return [ref[self.first + a, pl.ds(p * r + row, e), :] for row in (e, n)]

        def pack_d(a, carry):
            def plane(p):
                low, high = edges(a, p)
                return low, low, high, high

            self.pack(plane, e, lv.width, z_shifts * 2, put_at(4, e, a))
            return carry

        def pack_z(a, carry):
            def plane(p):
                return [ref[self.first + a, pl.ds(p * r + e, n), :]] * 2

            self.pack(plane, n, lv.width, z_shifts, put_at(2, n, a))
            return carry

        def pack_y(a, carry):
            if lv.slots_y == 1:
                for k in range(lv.half):
                    put_at(0, e, a)(k, edges(a, e + k))
            else:
                self.pack(lambda p: edges(a, p), e, lv.width_y, (zo, zo), put_at(0, e, a))
            return carry

        for body, which in ((pack_d, range(4, 8)), (pack_z, (2, 3)), (pack_y, (0, 1))):
            lax.fori_loop(0, self.count, body, 0)
            if send:
                for i in which:
                    self.send(i)

    def send_yz(self):
        for i in (4, 5, 6, 7, 2, 3, 0, 1):
            self.send(i)

    def start_yz(self):
        self.pack_yz(True)

    def finish_yz(self):
        lv, ref = self.level, self.ref
        r, n, e, zo = lv.rows, lv.n, lv.e, lv.zo
        with jax.named_scope("arrive"):
            self.all.wait()
        lane = lanes(r) % lv.span
        at_low = (lane >= zo - e) & (lane < zo)
        at_high = (lane >= zo + n) & (lane < zo + n + e)

        def unpack(a, carry):
            def got(i, row, rows):
                return self.got[a, pl.ds(self.starts[i] + row, rows), :]

            for s in range(2):
                for k in range(lv.packs_y):
                    value = got(s, k * e, e) * self.has_y[s]
                    for slot in range(min(lv.slots_y, lv.half - k * lv.slots_y)):
                        row = (e + k * lv.slots_y + slot) * r + (e + n) * s
                        moved = roll_lanes(value, zo - slot * lv.width_y) if lv.slots_y > 1 else value
                        ref[self.first + a, pl.ds(row, e), :] = moved
            for k in range(lv.packs):
                for t in range(2):
                    self.zf[t, a, pl.ds(k * r + e, n), :] = got(2 + t, k * n, n) * self.has_z[t]
                    for s in range(2):
                        both = self.has_y[s] * self.has_z[t]
                        self.zf[t, a, pl.ds(k * r + (e + n) * s, e), :] = got(4 + 2 * s + t, k * e, e) * both
            for k in range(lv.packs):
                sides = [self.zf[t, a, pl.ds(k * r, r), :] for t in range(2)]
                count = min(lv.slots, lv.half - k * lv.slots)
                for first in range(0, count, 4):
                    slots = range(first, min(first + 4, count))
                    values = []
                    for s in slots:
                        value = ref[self.first + a, pl.ds((e + k * lv.slots + s) * r, r), :]
                        value = jnp.where(at_low, roll_lanes(sides[0], zo - e - s * lv.width), value)
                        values.append(jnp.where(at_high, roll_lanes(sides[1], zo + n - s * lv.width), value))
                    for s, value in zip(slots, values):
                        ref[self.first + a, pl.ds((e + k * lv.slots + s) * r, r), :] = value
            return carry

        lax.fori_loop(0, self.count, unpack, 0)


def scaling(lv, fields, inverse, upper, extent):
    r = lv.rows

    def body(p, carry):
        row = pl.multiple_of(p * r, 8)
        cells = fields[3, pl.ds(row, r), :]
        face_z = fields[2, pl.ds(row, r), :]
        total = cells + fields[0, pl.ds(row, r), :] + fields[0, pl.ds(row + r, r), :]
        total = total + fields[1, pl.ds(row, r), :] + fields[1, pl.ds(row + 1, r), :]
        above = roll_lanes(face_z, -1)
        upper[0, pl.ds(row, r), :] = above
        total = total + face_z + above
        inverse[0, pl.ds(row, r), :] = jnp.where(cells > 0.0, 1.0 / total, 0.0)
        return carry

    loop(lv.e - extent, lv.e + lv.half + extent, body, 0, lv.unroll)


def sweep(lv, fields, upper, x, extent, emit, carry=0):
    r = lv.rows
    lo, hi = lv.e - extent, lv.e + lv.half + extent

    def body(p, carry):
        here, flux, kept = carry
        row = pl.multiple_of(p * r, 8)
        after = x[0, pl.ds(row + r, r), :]
        flux_after = fields[0, pl.ds(row + r, r), :] * (after - here)
        flux_y = fields[1, pl.ds(row, r), :] * (here - roll_rows(here, 1))
        flux_y = flux_y - fields[1, pl.ds(row + 1, r), :] * (roll_rows(here, -1) - here)
        flux_z = fields[2, pl.ds(row, r), :] * (here - roll_lanes(here, 1))
        flux_z = flux_z - upper[0, pl.ds(row, r), :] * (roll_lanes(here, -1) - here)
        applied = fields[3, pl.ds(row, r), :] * here + ((flux - flux_after) + flux_y + flux_z)
        return after, flux_after, emit(p, row, here, applied, kept)

    row = lo * r
    here = x[0, pl.ds(row, r), :]
    flux = fields[0, pl.ds(row, r), :] * (here - x[0, pl.ds(row - r, r), :])
    return loop(lo, hi, body, (here, flux, carry), lv.unroll)[2]


def step(lv, fields, inverse, upper, x, out, d, extent, first, coefs, keep):
    r = lv.rows

    def emit(p, row, here, applied, kept):
        scaled = inverse[0, pl.ds(row, r), :] * (fields[4, pl.ds(row, r), :] - applied)
        if first == 0:
            update = scaled * (1.0 / THETA)
        elif first == 1:
            update = coefs[0] * here + coefs[1] * scaled
        else:
            update = coefs[0] * d[0, pl.ds(row, r), :] + coefs[1] * scaled
        if keep:
            d[0, pl.ds(row, r), :] = update
        out[0, pl.ds(row, r), :] = here + update
        return kept

    sweep(lv, fields, upper, x, extent, emit)


def smooth_from_zero(lv, fields, inverse, upper, xa, xb, d, extent):
    r = lv.rows

    def body(p, carry):
        row = pl.multiple_of(p * r, 8)
        xa[0, pl.ds(row, r), :] = inverse[0, pl.ds(row, r), :] * fields[4, pl.ds(row, r), :] * (1.0 / THETA)
        return carry

    loop(lv.e - extent, lv.e + lv.half + extent, body, 0, lv.unroll)
    step(lv, fields, inverse, upper, xa, xb, d, extent - 1, 1, STEP1, True)
    step(lv, fields, inverse, upper, xb, xa, d, extent - 2, 2, STEP2, False)


def smooth(lv, fields, inverse, upper, xa, xb, d, extent):
    step(lv, fields, inverse, upper, xa, xb, d, extent - 1, 0, None, True)
    step(lv, fields, inverse, upper, xb, xa, d, extent - 2, 2, STEP1, True)
    step(lv, fields, inverse, upper, xa, xb, d, extent - 3, 2, STEP2, False)


def coarse_lanes(lv, below, rows, half):
    lane = lanes(rows)
    if below is None:
        cell, at = lane, 0
    else:
        at = (lane // below.span) * 64 if below.ways == 2 else 0
        cell = lane % below.span - below.zo
    if lv.ways == 2 and half is not None:
        at = 64 * half
    inside = (cell >= 0) & (cell < lv.n // 2)
    index = jnp.where(inside, at + lv.zo + 2 * cell, 0)
    return index, inside


def place(lv, below, put, plane, value, pair):
    rows = value.shape[0]
    if pair:
        value = value + roll_lanes(value, -1)
    halves = [None] if below is not None and below.ways == lv.ways else range(lv.ways)
    for half in halves:
        index, inside = coarse_lanes(lv, below, rows, half)
        got = jnp.where(inside, gather_lanes(value, index), 0.0)
        put(plane if half is None else plane + half * (lv.half // 2), got)


def coarsen_fields(lv, below, fields, put):
    n2, e, r = lv.n // 2, lv.e, lv.rows

    def body(i, carry):
        row = (e + 2 * i) * r + e

        def rows(a, plane, odd):
            return fields[a, pl.ds(row + plane * r + odd, n2, stride=2), :]

        put_x = functools.partial(put, 0)
        put_y = functools.partial(put, 1)
        put_z = functools.partial(put, 2)
        put_c = functools.partial(put, 3)
        place(lv, below, put_x, i, (rows(0, 0, 0) + rows(0, 0, 1)) * 0.0625, True)
        place(lv, below, put_y, i, (rows(1, 0, 0) + rows(1, 1, 0)) * 0.0625, True)
        place(lv, below, put_z, i, (rows(2, 0, 0) + rows(2, 0, 1) + rows(2, 1, 0) + rows(2, 1, 1)) * 0.0625, False)
        place(lv, below, put_c, i, (rows(3, 0, 0) + rows(3, 0, 1) + rows(3, 1, 0) + rows(3, 1, 1)) * 0.125, True)
        return carry

    loop(0, lv.half // 2, body, 0, 3)


def restrict(lv, below, fields, upper, x, sums, put):
    r, n2 = lv.rows, lv.n // 2

    def emit(p, row, here, applied, kept):
        sums[0, pl.ds((p - lv.e) * r, r), :] = fields[4, pl.ds(row, r), :] - applied
        return kept

    sweep(lv, fields, upper, x, 0, emit)

    def body(i, carry):
        total = None
        for plane in range(2):
            for odd in range(2):
                part = sums[0, pl.ds((2 * i + plane) * r + lv.e + odd, n2, stride=2), :]
                total = part if total is None else total + part
        place(lv, below, functools.partial(put, 4), i, total * 0.125, True)
        return carry

    loop(0, lv.half // 2, body, 0, 6)


def fields_put(below, fields):
    def put(field, plane, value):
        fields[field, pl.ds((below.e + plane) * below.rows + below.e, below.n), :] = value

    return put


def prolong(lv, above, e, x, reach):
    r, rows = lv.rows, lv.n // 2 + 2 * reach
    lane = lanes(rows)
    cell = lane % 64 - lv.zo + 2 * reach
    inside = (cell >= 0) & (cell < 2 * rows)
    source = above.zo - reach + cell // 2
    if above.ways == 2:
        source = source + (lane // 64) * 64
    source = jnp.where(inside, source, 0)

    def body(i, carry):
        row = (above.e - reach + i) * above.rows + above.e - reach
        value = gather_lanes(e[0, pl.ds(row, rows), :], source)
        if above.ways == 1:
            other = gather_lanes(e[0, pl.ds(row + (lv.half // 2) * above.rows, rows), :], source)
            value = jnp.where(lane < 64, value, other)
        value = jnp.where(inside, value, 0.0)
        for plane in range(2):
            at = (lv.e - 2 * reach + 2 * i + plane) * r + lv.e - 2 * reach
            for odd in range(2):
                where = pl.ds(at + odd, rows, stride=2)
                x[0, where, :] = x[0, where, :] + value
        return carry

    loop(0, lv.half // 2 + 2 * reach, body, 0, 4)


PAD = 8


def row_of(rows):
    return lax.broadcasted_iota(jnp.int32, (rows, 128), 0)


def whole_neighbours(ny, value, rows):
    z, y = row_of(128) % 8, lanes(128) % 6
    out = []
    for g in range(ny):
        here = value(g)
        low_y, high_y = roll_lanes(here, 1), roll_lanes(here, -1)
        if g:
            low_y = jnp.where(y == 0, roll_lanes(value(g - 1), -5), low_y)
        if g + 1 < ny:
            high_y = jnp.where(y == 5, roll_lanes(value(g + 1), 5), high_y)
        low_z = jnp.where(z == 0, rows(g, -3), rows(g, -1))
        high_z = jnp.where(z == 5, rows(g, 3), rows(g, 1))
        out.append((roll_lanes(here, 6), roll_lanes(here, -6), low_y, high_y, low_z, high_z))
    return out


def whole_prepare(ny, fields, coefs, diagonal, inverse):
    z, y, row = row_of(128) % 8, lanes(128) % 6, row_of(128)
    moved = lambda a: whole_neighbours(ny, lambda g: fields(a, g), lambda g, d: roll_rows(fields(a, g), -d))
    high = [[near[1] for near in moved(0)], [near[3] for near in moved(1)], [near[5] for near in moved(2)]]
    for g in range(ny):
        inside = fields(3, g) > 0.0
        high_y = jnp.where(y == 5, 0.0, high[1][g]) if g + 1 == ny else high[1][g]
        high_z = jnp.where(row == 125, 0.0, high[2][g])
        sides = [fields(0, g), high[0][g], fields(1, g), high_y, fields(2, g), high_z]
        total = functools.reduce(lambda a, b: a + b, sides) + fields(3, g)
        scale = jnp.where(inside, 1.0 / total, 0.0)
        diagonal[g] = jnp.where(inside, total, 0.0)
        inverse[g] = scale
        if g == 0:
            sides[2] = jnp.where(y == 0, 0.0, sides[2])
        sides[4] = jnp.where(row == 0, 0.0, sides[4])
        for i in range(6):
            coefs[i, g] = sides[i] * scale


def children(value, axes):
    if "y" in axes:
        value = value + roll_lanes(value, -1)
    if "x" in axes:
        value = value + roll_lanes(value, -6)
    if "z" in axes:
        value = value + roll_rows(value, -1)
    return value


def even_cells():
    row, lane = row_of(128), lanes(128)
    return (row % 2 == 0) & (row % 8 < 6) & (lane % 2 == 0) & ((lane // 6) % 2 == 0) & (lane < 72)


def fold_level(values):
    even = even_cells()
    values = [jnp.where(even, v, 0.0) for v in values]
    both = (values[0] + roll_lanes(values[1], 1)) + (roll_lanes(values[2], 6) + roll_lanes(values[3], 7))
    return both[0:64] + roll_rows(both[64:128], 1)


def unfold_level(value):
    both = jnp.concatenate([value, roll_rows(value, -1)], axis=0)
    even = even_cells()
    return [jnp.where(even, roll_lanes(both, -shift), 0.0) for shift in (0, 1, 6, 7)]


def bottom_neighbours(v):
    row, lane = row_of(64), lanes(64)
    z, y = (row % 8) // 2, (lane % 6) // 2
    odd = lane % 2 == 1
    low_y = jnp.where(y > 0, roll_lanes(v, 2), jnp.where(odd, roll_lanes(v, -3), roll_lanes(v, 1)))
    high_y = jnp.where(y < 2, roll_lanes(v, -2), jnp.where(odd, roll_lanes(v, -1), roll_lanes(v, 3)))
    low_z = jnp.where(z > 0, roll_rows(v, 2), jnp.where(row == 1, roll_rows(v, 5), roll_rows(v, 4)))
    high_z = jnp.where(z < 2, roll_rows(v, -2), jnp.where(row == 60, roll_rows(v, -5), roll_rows(v, -4)))
    return roll_lanes(v, 12), roll_lanes(v, -12), low_y, high_y, low_z, high_z


def bottom_prepare(ny, fields, bottom):
    row, lane = row_of(64), lanes(64)
    y = (lane % 6) // 2
    first = (lane % 2 == 0) & ((lane // 6) % 2 == 0)
    last = (lane % 2 == 1) & ((lane // 6) % 2 == 1)
    faces = []
    for a, axes in enumerate(("yz", "xz", "xy", "xyz")):
        factor = 0.125 if a == 3 else 0.0625
        faces.append(fold_level([children(fields(a, g), axes) * factor for g in range(ny)]))
    inside = faces[3] > 0.0
    high_x = bottom_neighbours(faces[0])[1]
    high_y = jnp.where(last & (y == 2), 0.0, bottom_neighbours(faces[1])[3])
    high_z = jnp.where(row == 61, 0.0, bottom_neighbours(faces[2])[5])
    sides = [faces[0], high_x, faces[1], high_y, faces[2], high_z]
    total = functools.reduce(lambda a, b: a + b, sides) + faces[3]
    sides[2] = jnp.where(first & (y == 0), 0.0, sides[2])
    sides[4] = jnp.where(row == 0, 0.0, sides[4])
    for i, value in enumerate(sides + [total]):
        bottom[i] = jnp.where(inside, value, 0.0)


def coarse_solve(ny, coefs, diagonal, inverse, f, bottom, xa, xb, ds, g3):
    def rows(x, g, offset=0):
        return x[g, pl.ds(PAD + offset, 128)]

    def scaled(x):
        near = whole_neighbours(ny, lambda g: rows(x, g), lambda g, d: rows(x, g, d))
        out = []
        for g in range(ny):
            parts = [coefs[i, g] * near[g][i] for i in range(6)]
            total = ((parts[0] + parts[1]) + (parts[2] + parts[3])) + (parts[4] + parts[5])
            out.append((g3[g] - rows(x, g)) + total)
        return out

    def advance(x, to, coef, first, keep=True):
        for g, value in enumerate(scaled(x)):
            update = value * (1.0 / THETA) if first else coef[0] * ds[g] + coef[1] * value
            if keep:
                ds[g] = update
            to[g, pl.ds(PAD, 128)] = rows(x, g) + update

    for x in (xa, xb):
        for g in range(ny):
            x[g, pl.ds(0, PAD)] = jnp.zeros((PAD, 128), F32)
            x[g, pl.ds(PAD + 128, PAD)] = jnp.zeros((PAD, 128), F32)
    for g in range(ny):
        g3[g] = inverse[g] * f(g)
        ds[g] = g3[g] * (1.0 / THETA)
        xa[g, pl.ds(PAD, 128)] = ds[g]
    advance(xa, xb, STEP1, False)
    advance(xb, xa, STEP2, False, False)
    remainder = scaled(xa)
    r = fold_level([children(remainder[g] * diagonal[g], "xyz") * 0.125 for g in range(ny)])
    r = jnp.where(bottom[6] > 0.0, r, 0.0)

    def total(value):
        value = jnp.sum(value.reshape(8, 8, 128), axis=0)
        return jnp.sum(jnp.sum(value, axis=1, keepdims=True), axis=0, keepdims=True)

    def applied(v):
        near = bottom_neighbours(v)
        parts = [bottom[i] * near[i] for i in range(6)]
        return bottom[6] * v - (((parts[0] + parts[1]) + (parts[2] + parts[3])) + (parts[4] + parts[5]))

    e = jnp.zeros((64, 128), F32)
    p, norm = r, total(r * r)
    for i in range(BOTTOM):
        q = applied(p)
        size = norm / total(p * q)
        e = e + size * p
        if i + 1 < BOTTOM:
            r = r - size * q
            after = total(r * r)
            p = r + after / norm * p
            norm = after
    for g, value in enumerate(unfold_level(e)):
        value = value + roll_lanes(value, 1)
        value = value + roll_lanes(value, 6)
        xa[g, pl.ds(PAD, 128)] = rows(xa, g) + (value + roll_rows(value, 1))
    advance(xa, xb, None, True)
    advance(xb, xa, STEP1, False)
    advance(xa, xb, STEP2, False, False)


def window(lv, gx, gy, gz, ny, xs, padded, turned, corner, x):
    nz = 16
    padded[...] = jnp.zeros_like(padded)
    for g in range(ny):
        padded[g + 1, pl.ds(1, nz)] = xs[g, pl.ds(PAD, 128)].reshape(nz, 8, 128)
    for dy in range(3):
        tiles = padded[gy + dy, pl.ds(gz, 3)].reshape(24, 128)
        tiles = jnp.concatenate([tiles, jnp.zeros((104, 128), F32)], axis=0)
        turned[dy, pl.ds(0, 24), :] = jnp.zeros((24, 128), F32)
        turned[dy, pl.ds(24, 128), :] = tiles.T
    lane = lanes(16)
    cell = lane - lv.zo + 6
    inside = (cell >= 0) & (cell < 24)
    coarse = jnp.where(inside, cell // 2 + 3, 0)
    source = (coarse // 6) * 8 + coarse % 6

    def body(i, carry):
        base = 6 + 36 * gx + 6 * i
        corner[pl.ds(0, 3), :] = turned[0, pl.ds(base + 3, 3), :]
        corner[pl.ds(3, 6), :] = turned[1, pl.ds(base, 6), :]
        corner[pl.ds(9, 3), :] = turned[2, pl.ds(base, 3), :]
        value = jnp.where(inside, gather_lanes(corner[0:16], source), 0.0)[0:12]
        for plane in range(2):
            at = (lv.e - 6 + 2 * i + plane) * lv.rows + lv.e - 6
            for odd in range(2):
                where = pl.ds(at + odd, 12, stride=2)
                x[0, where, :] = x[0, where, :] + value
        return carry

    loop(0, 12, body, 0, 4)


def hops(t, nz):
    return sum(min(d, 4 - d) for d in (t // nz % 4, t % nz // 4, t % 4))


def cycle(ny, nz, names, *refs):
    refs = list(refs)
    right_hbm, faces_hbm, cells_hbm, solution_hbm, residual_hbm, norm_out = refs[:6]
    s = dict(zip(names, refs[6:]))
    gx, gy, gz = lax.axis_index("gx"), lax.axis_index("gy"), lax.axis_index("gz")
    here = (gx, gy, gz, ny, nz)
    scope = jax.named_scope

    loads = [pltpu.make_async_copy(faces_hbm.at[d], s["land"].at[d], s["load_sem"].at[d]) for d in range(3)]
    loads.append(pltpu.make_async_copy(cells_hbm, s["land"].at[3], s["load_sem"].at[3]))
    loads.append(pltpu.make_async_copy(right_hbm, s["land"].at[4], s["load_sem"].at[4]))
    for copy in loads:
        copy.start()

    def other(t):
        return lax.rem(gy + t // nz, ny), lax.rem(gz + t % nz, nz)

    order = sorted(range(1, ny * nz), key=lambda t: -hops(t, nz))
    barrier = pltpu.get_barrier_semaphore()
    with scope("greet"):
        for t in order:
            oy, oz = other(t)
            for ox in (gx, 1 - gx):
                pl.semaphore_signal(barrier, inc=1, device_id=(ox, oy, oz), device_id_type=MESH)
        pl.semaphore_signal(barrier, inc=1, device_id=(1 - gx, gy, gz), device_id_type=MESH)

    f0, f1, f2 = s["f0"], s["f1"], s["f2"]
    ex = {k: Exchange(*v) for k, v in EXCHANGES.items()}
    targets = {"e0a": f0, "e0b": f0, "e0c": f0, "c1": f1, "c2": f2, "e1": f1, "e2": f2, "x0": s["x0a"], "x1": s["x1a"], "x2": s["x2a"]}
    for k, target in targets.items():
        ex[k].bind(here, target, [s[k + str(i)] for i in range(7)])

    def partner(src, dst, i):
        return pltpu.make_async_remote_copy(
            src_ref=src,
            dst_ref=dst,
            send_sem=s["pair_send"].at[i],
            recv_sem=s["pair_recv"].at[i],
            device_id=(1 - gx, gy, gz),
            device_id_type=MESH,
        )

    me = gy * nz + gz

    def spread(src, whole, i):
        def copy(src, dst, oy, oz):
            return pltpu.make_async_remote_copy(
                src_ref=src,
                dst_ref=dst,
                send_sem=s["all_send"].at[i],
                recv_sem=s["all_recv"].at[i],
                device_id=(gx, oy, oz),
                device_id_type=MESH,
            )

        def start():
            for t in order:
                copy(src, whole.at[me], *other(t)).start()

        def finish():
            most = whole.at[pl.ds(0, ny * nz - 1)]
            copy(most, most, *other(1)).wait()

        return start, finish

    block = s["block"]

    def block_put(field, plane, value):
        block[field, pl.ds(plane * 6, 6), :] = value

    for a in range(5):
        with scope("load_wait"):
            loads[a].wait()

        def load(i, carry, a=a):
            first = jnp.pad(s["land"][a, i], ((0, 0), (0, 80)))
            second = jnp.pad(s["land"][a, i + 24], ((0, 0), (0, 80)))
            value = roll_lanes(first, L0.zo) + roll_lanes(second, 64 + L0.zo)
            f0[a, pl.ds((L0.e + i) * L0.rows + L0.e, 48), :] = value
            return carry

        with scope("layout"):
            loop(0, 24, load, 0, 12)

    with scope("e0_pack"):
        ex["e0a"].pack_yz(False)
    with scope("barrier"):
        pl.semaphore_wait(barrier, 2 * ny * nz - 1)
    ex["e0a"].send_yz()
    with scope("e0_start_yz"):
        ex["e0b"].start_yz()
        ex["e0c"].start_yz()
    f1[...] = jnp.zeros_like(f1)
    f2[...] = jnp.zeros_like(f2)
    block[...] = jnp.zeros_like(block)
    with scope("coarsen_0"):
        coarsen_fields(L0, L1, f0, fields_put(L1, f1))
    with scope("c1_pack"):
        ex["c1"].pack_yz(False)
    with scope("coarsen_1"):
        coarsen_fields(L1, L2, f1, fields_put(L2, f2))
    with scope("c2_pack"):
        ex["c2"].pack_yz(False)
    with scope("coarsen_2"):
        coarsen_fields(L2, None, f2, block_put)

    def tile_of(field):
        return roll_lanes(block[field].T[0:8], gx * 36)

    own4, pair4, own1, pair1, own_n = (s[k] for k in ("own4", "pair4", "own1", "pair1", "own_n"))
    for field in range(4):
        own4[field] = tile_of(field)
    pair_coef = partner(own4, pair4, 0)
    pair_coef.start()

    def square(i, carry):
        value = f0[4, pl.ds((L0.e + i) * L0.rows + L0.e, 48), :]
        return carry + value * value

    with scope("square"):
        squares = loop(0, 24, square, jnp.zeros((48, 128), F32), 4)
    for k in ("e0a", "e0b", "e0c"):
        with scope(k + "_finish_yz"):
            ex[k].finish_yz()
        ex[k].start_x()
    ex["c1"].send_yz()
    g4, g1, gn = s["g4"], s["g1"], s["gn"]
    with scope("pair_coef"):
        pair_coef.wait()
    merged = s["merged4"]
    merged[...] = own4[...] + pair4[...]
    mine = pl.ds(2 * gx, 2)
    g4[gy, gz, mine] = merged[mine]
    row, column = gz // 4, gz % 4

    def coef_part(stage):
        if stage == 0:
            return g4.at[gy, gz, mine]
        if stage == 1:
            return g4.at[:, gz, mine]
        return g4.at[:, pl.ds(4 * row, 4), mine]

    def coef_copy(stage, src, oy, oz):
        return pltpu.make_async_remote_copy(
            src_ref=src,
            dst_ref=src,
            send_sem=s["coef_send"].at[stage],
            recv_sem=s["coef_recv"].at[stage],
            device_id=(gx, oy, oz),
            device_id_type=MESH,
        )

    def coef_start(stage):
        for d in (2, 1, 3):
            oy, oz = gy, gz
            if stage == 0:
                oy = lax.rem(gy + d, ny)
            elif stage == 1:
                oz = 4 * row + lax.rem(column + d, 4)
            else:
                oz = lax.rem(gz + 4 * d, nz)
            coef_copy(stage, coef_part(stage), oy, oz).start()

    def coef_wait(stage):
        two = pl.ds(0, 2)
        most = (g4.at[pl.ds(0, 3), 0, two], g4.at[:, pl.ds(0, 3), two], g4.at[:, pl.ds(0, 12), two])[stage]
        coef_copy(stage, most, lax.rem(gy + 1, ny), gz).wait()

    with scope("coef_0"):
        coef_start(0)
    with scope("e0_finish_x"):
        ex["e0a"].finish_x()
        ex["e0b"].finish_x()
    with scope("scaling_0"):
        scaling(L0, f0, s["i0"], s["u0"], 3)
    with scope("e0c_finish_x"):
        ex["e0c"].finish_x()
    with scope("smooth_0"):
        smooth_from_zero(L0, f0, s["i0"], s["u0"], s["x0a"], s["x0b"], s["d0"], 3)
    with scope("restrict_0"):
        restrict(L0, L1, f0, s["u0"], s["x0a"], s["sums"], fields_put(L1, f1))
    with scope("e1_start_yz"):
        ex["e1"].start_yz()
    ex["c2"].send_yz()
    with scope("c1_finish_yz"):
        ex["c1"].finish_yz()
    ex["c1"].start_x()
    with scope("coef_1"):
        coef_wait(0)
        coef_start(1)
    with scope("x0_start_yz"):
        ex["x0"].start_yz()
    with scope("c1_finish_x"):
        ex["c1"].finish_x()
    with scope("scaling_1"):
        scaling(L1, f1, s["i1"], s["u1"], 4)
    with scope("e1_finish_yz"):
        ex["e1"].finish_yz()
    ex["e1"].start_x()
    with scope("e1_finish_x"):
        ex["e1"].finish_x()
    with scope("coef_2"):
        coef_wait(1)
        coef_start(2)
    with scope("smooth_1"):
        smooth_from_zero(L1, f1, s["i1"], s["u1"], s["x1a"], s["x1b"], s["d1"], 3)
    with scope("restrict_1"):
        restrict(L1, L2, f1, s["u1"], s["x1a"], s["sums"], fields_put(L2, f2))
    with scope("e2_start_yz"):
        ex["e2"].start_yz()
    with scope("c2_finish_yz"):
        ex["c2"].finish_yz()
    ex["c2"].start_x()
    with scope("x1_start_yz"):
        ex["x1"].start_yz()
    with scope("c2_finish_x"):
        ex["c2"].finish_x()
    with scope("scaling_2"):
        scaling(L2, f2, s["i2"], s["u2"], 5)
    other_half = pltpu.make_async_remote_copy(
        src_ref=g4.at[:, :, mine],
        dst_ref=g4.at[:, :, mine],
        send_sem=s["pair_send"].at[3],
        recv_sem=s["pair_recv"].at[3],
        device_id=(1 - gx, gy, gz),
        device_id_type=MESH,
    )
    with scope("e2_finish_yz"):
        ex["e2"].finish_yz()
    ex["e2"].start_x()
    with scope("x0_finish_yz"):
        ex["x0"].finish_yz()
    with scope("e2_finish_x"):
        ex["e2"].finish_x()
    with scope("smooth_2"):
        smooth_from_zero(L2, f2, s["i2"], s["u2"], s["x2a"], s["x2b"], s["d2"], 3)
    with scope("restrict_2"):
        restrict(L2, None, f2, s["u2"], s["x2a"], s["sums"], block_put)
    own1[...] = tile_of(4)
    pair_source = partner(own1, pair1, 1)
    pair_source.start()
    ex["x0"].start_x()
    with scope("x2_start_yz"):
        ex["x2"].start_yz()
    with scope("pair_source"):
        pair_source.wait()
    s["merged1"][...] = own1[...] + pair1[...]
    g1[me] = s["merged1"][...]
    source_start, source_finish = spread(s["merged1"], g1, 1)
    with scope("source_start"):
        source_start()
    with scope("coef_finish"):
        coef_wait(2)
    other_half.start()
    with scope("hidden_1"):
        ex["x1"].finish_yz()
        ex["x1"].start_x()
        ex["x0"].finish_x()
    with scope("other_half"):
        other_half.wait()
    gathered = lambda a, g: g4[g, :, a].reshape(128, 128)
    with scope("coarse_fields"):
        whole_prepare(ny, gathered, s["c3"], s["w3"], s["i3"])
        bottom_prepare(ny, gathered, s["bottom"])
    with scope("hidden_2"):
        ex["x1"].finish_x()
        ex["x2"].finish_yz()
        ex["x2"].start_x()
    with scope("source_finish"):
        source_finish()
    with scope("coarse_solve"):
        source = lambda g: g1[pl.ds(g * nz, nz)].reshape(128, 128)
        whole = [s[k] for k in ("c3", "w3", "i3")]
        coarse_solve(ny, *whole, source, s["bottom"], s["x3a"], s["x3b"], s["d3"], s["g3"])
    with scope("x2_finish_x"):
        ex["x2"].finish_x()
    with scope("window"):
        window(L2, gx, gy, gz, ny, s["x3b"], s["padded"], s["turned"], s["corner"], s["x2a"])
    with scope("post_2"):
        smooth(L2, f2, s["i2"], s["u2"], s["x2a"], s["x2b"], s["d2"], 6)
    with scope("prolong_1"):
        prolong(L1, L2, s["x2b"], s["x1a"], 3)
    with scope("post_1"):
        smooth(L1, f1, s["i1"], s["u1"], s["x1a"], s["x1b"], s["d1"], 5)
    with scope("prolong_0"):
        prolong(L0, L1, s["x1b"], s["x0a"], 2)
    with scope("post_0"):
        smooth(L0, f0, s["i0"], s["u0"], s["x0a"], s["x0b"], s["d0"], 4)

    land = s["land"]
    r0 = L0.rows
    lane48 = lanes(48) % 64
    inside = (lane48 >= L0.zo) & (lane48 < L0.zo + 48)

    def final(p, row, here_x, applied, kept):
        s["sums"][0, pl.ds((p - L0.e) * r0, r0), :] = f0[4, pl.ds(row, r0), :] - applied
        return kept

    with scope("final"):
        sweep(L0, f0, s["u0"], s["x0b"], 0, final)

    def out_square(i, carry):
        value = jnp.where(inside, s["sums"][0, pl.ds(i * r0 + L0.e, 48), :], 0.0)
        return carry + value * value

    with scope("square"):
        ends = loop(0, 24, out_square, jnp.zeros((48, 128), F32), 4)

    def fold(value):
        return jnp.sum(value, axis=0, keepdims=True)

    def squares_of(value):
        return jnp.sum(fold(value), axis=1, keepdims=True)

    lane1 = lax.broadcasted_iota(jnp.int32, (1, 128), 1)
    pair = jnp.where(lane1 == 0, squares_of(squares), jnp.where(lane1 == 1, squares_of(ends), 0.0))
    own_n[...] = pair
    mine_n = gx * (ny * nz) + me
    gn[mine_n] = pair

    def norm_copy(src, dst, ox, oy, oz):
        return pltpu.make_async_remote_copy(
            src_ref=src,
            dst_ref=dst,
            send_sem=s["all_send"].at[2],
            recv_sem=s["all_recv"].at[2],
            device_id=(ox, oy, oz),
            device_id_type=MESH,
        )

    with scope("norm_start"):
        for t in order:
            for ox in (gx, 1 - gx):
                norm_copy(own_n, gn.at[mine_n], ox, *other(t)).start()
        norm_copy(own_n, gn.at[mine_n], 1 - gx, gy, gz).start()

    def unload(slot, i, value):
        for half in range(2):
            moved = roll_lanes(value, -(L0.zo + 64 * half))
            land[slot, i + 24 * half] = moved[:, 0:48]

    def out_solution(i, carry):
        unload(0, i, s["x0b"][0, pl.ds((L0.e + i) * r0 + L0.e, 48), :])
        return carry

    def out_residual(i, carry):
        unload(1, i, s["sums"][0, pl.ds(i * r0 + L0.e, 48), :])
        return carry

    with scope("unload_solution"):
        loop(0, 24, out_solution, 0, 6)
    out0 = pltpu.make_async_copy(land.at[0], solution_hbm, s["out_sem"].at[0])
    out0.start()
    with scope("unload_residual"):
        loop(0, 24, out_residual, 0, 6)
    out1 = pltpu.make_async_copy(land.at[1], residual_hbm, s["out_sem"].at[1])
    out1.start()
    with scope("norm_finish"):
        most = gn.at[pl.ds(0, 2 * ny * nz - 1)]
        norm_copy(most, most, 1 - gx, gy, gz).wait()
    sums = jnp.sum(gn[...], axis=0)
    norm = jnp.sqrt(sums[:, 1:2] / sums[:, 0:1])
    norm_out[0, 0] = norm[0, 0]
    with scope("out_wait"):
        out0.wait()
        out1.wait()


EXCHANGES = {
    "e0a": (L0, 0, 2),
    "e0b": (L0, 2, 2),
    "e0c": (L0, 4, 1),
    "c1": (L1, 0, 4),
    "c2": (L2, 0, 4),
    "e1": (L1, 4, 1),
    "e2": (L2, 4, 1),
    "x0": (L0, 0, 1),
    "x1": (L1, 0, 1),
    "x2": (L2, 0, 1),
}


def scratch_of(ny, nz):
    vmem = lambda *shape: pltpu.VMEM(shape, F32)
    size = lambda lv: lv.planes * lv.rows + 16
    scratch = {"land": vmem(5, 48, 48, 48), "load_sem": pltpu.SemaphoreType.DMA((5,)), "out_sem": pltpu.SemaphoreType.DMA((2,))}
    for i, lv in enumerate((L0, L1, L2)):
        scratch[f"f{i}"] = vmem(5, size(lv), 128)
        for k in ("i", "d", "u"):
            scratch[f"{k}{i}"] = vmem(1, size(lv), 128)
        scratch[f"x{i}a"] = vmem(1, size(lv), 128)
        scratch[f"x{i}b"] = vmem(1, size(lv), 128)
    scratch["sums"] = vmem(1, 24 * 56 + 16, 128)
    scratch["block"] = vmem(5, 128, 128)
    for k in ("own4", "pair4", "merged4"):
        scratch[k] = vmem(4, 8, 128)
    for k in ("own1", "pair1", "merged1"):
        scratch[k] = vmem(8, 128)
    scratch["g4"] = vmem(ny, nz, 4, 8, 128)
    scratch["g1"] = vmem(ny * nz, 8, 128)
    scratch["gn"] = vmem(2 * ny * nz, 1, 128)
    scratch["own_n"] = vmem(1, 128)
    for k in ("pair_send", "pair_recv"):
        scratch[k] = pltpu.SemaphoreType.DMA((4,))
    for k in ("all_send", "all_recv", "coef_send", "coef_recv"):
        scratch[k] = pltpu.SemaphoreType.DMA((3,))
    for k in ("i3", "w3", "d3", "g3"):
        scratch[k] = vmem(ny, 128, 128)
    for k in ("x3a", "x3b"):
        scratch[k] = vmem(ny, 128 + 2 * PAD, 128)
    scratch["c3"] = vmem(6, ny, 128, 128)
    scratch["bottom"] = vmem(7, 64, 128)
    scratch["padded"] = vmem(ny + 2, nz + 2, 8, 128)
    scratch["turned"] = vmem(3, 160, 128)
    scratch["corner"] = vmem(24, 128)
    for k, v in EXCHANGES.items():
        for i, shape in enumerate(Exchange(*v).scratch()):
            scratch[k + str(i)] = shape
    return scratch


def solution(mesh):
    ny, nz = mesh.shape["gy"], mesh.shape["gz"]
    scratch = scratch_of(ny, nz)

    def shards(right_side, face_coef, absorption):
        field = jax.ShapeDtypeStruct((48, 48, 48), F32)
        solved, residual, norm = pl.pallas_call(
            functools.partial(cycle, ny, nz, tuple(scratch)),
            out_shape=(pltpu.VMEM((48, 48, 48), F32), pltpu.VMEM((48, 48, 48), F32), jax.ShapeDtypeStruct((1, 1), F32)),
            in_specs=[pl.BlockSpec(memory_space=pltpu.HBM)] * 3,
            out_specs=(
                pl.BlockSpec(memory_space=pl.ANY),
                pl.BlockSpec(memory_space=pl.ANY),
                pl.BlockSpec(memory_space=pltpu.SMEM),
            ),
            scratch_shapes=list(scratch.values()),
            compiler_params=pltpu.CompilerParams(
                collective_id=0, has_side_effects=True, vmem_limit_bytes=57000 * 1024
            ),
        )(right_side, face_coef, absorption)
        return solved, residual, norm[0, 0]

    in_specs = (P("gx", "gy", "gz"), P(None, "gx", "gy", "gz"), P("gx", "gy", "gz"))
    out_specs = (P("gx", "gy", "gz"), P("gx", "gy", "gz"), P())
    return jax.shard_map(shards, mesh=mesh, in_specs=in_specs, out_specs=out_specs, check_vma=False)
```

```python
import functools

import jax
import jax.numpy as jnp
from jax import lax
from jax.experimental import pallas as pl
from jax.experimental.pallas import tpu as pltpu
from jax.sharding import PartitionSpec as P

BOTTOM = 6
THETA = 1.125
DELTA = 0.875
SIGMA = THETA / DELTA
RHO0 = 1.0 / SIGMA
RHO1 = 1.0 / (2.0 * SIGMA - RHO0)
RHO2 = 1.0 / (2.0 * SIGMA - RHO1)
STEP1 = (RHO1 * RHO0, 2.0 * RHO1 / DELTA)
STEP2 = (RHO2 * RHO1, 2.0 * RHO2 / DELTA)

F32 = jnp.float32
MESH = pl.DeviceIdType.MESH


class Level:
    def __init__(self, n, e, ways, rows, zo, width, width_y, unroll):
        self.n, self.e, self.ways, self.rows, self.zo, self.width = n, e, ways, rows, zo, width
        self.width_y, self.unroll = width_y, unroll
        self.half = n // ways
        self.planes = self.half + 2 * e
        self.span = 128 // ways
        self.slots, self.slots_y = self.span // width, self.span // width_y
        self.packs, self.packs_y = -(-self.half // self.slots), -(-self.half // self.slots_y)


L0 = Level(48, 4, 2, 56, 8, 4, 64, 4)
L1 = Level(24, 6, 2, 40, 16, 8, 32, 4)
L2 = Level(12, 6, 1, 24, 16, 8, 16, 6)


def lanes(rows):
    return lax.broadcasted_iota(jnp.int32, (rows, 128), 1)


def gather_lanes(value, index):
    return jnp.take_along_axis(value, index, axis=1)


def roll_lanes(value, shift):
    return pltpu.roll(value, shift % 128, 1)


def roll_rows(value, shift):
    return pltpu.roll(value, shift % value.shape[0], 0)


def tile_rows(start, size):
    return pl.ds(pl.multiple_of(start, 8), size)


def loop(lo, hi, body, carry, unroll):
    count = (hi - lo) // unroll

    def chunk(i, carry):
        for k in range(unroll):
            carry = body(lo + i * unroll + k, carry)
        return carry

    carry = lax.fori_loop(0, count, chunk, carry)
    for k in range(lo + count * unroll, hi):
        carry = body(k, carry)
    return carry


class Exchange:
    def __init__(self, level, first, count):
        self.level, self.first, self.count = level, first, count
        lv = level
        sizes = [-(-rows // 8) * 8 for rows in (lv.packs_y * lv.e, lv.packs * lv.n, lv.packs * lv.e)]
        self.sizes = [sizes[0]] * 2 + [sizes[1]] * 2 + [sizes[2]] * 4
        self.starts = [sum(self.sizes[:i]) for i in range(9)]

    def scratch(self):
        lv, na = self.level, self.count
        shapes = [
            (na, lv.e * lv.rows, 128),
            (na, self.starts[8] + 8, 128),
            (na, self.starts[8] + 8, 128),
            (na, self.starts[8] + 8, 128),
            (2, na, lv.packs * lv.rows + 8, 128),
        ]
        return [pltpu.VMEM(s, F32) for s in shapes] + [pltpu.SemaphoreType.DMA((2,)), pltpu.SemaphoreType.DMA((2,))]

    def bind(self, here, ref, scratch):
        self.here, self.ref = here, ref
        self.xr, self.out, self.got, self.spare, self.zf, self.ssem, self.rsem = scratch
        gx, gy, gz, ny, nz = here
        lv = self.level
        start = lv.e + (1 - gx) * (lv.half - lv.e if lv.ways == 2 else lv.n - lv.e)

        def copy(src, dst, i, gx, gy, gz):
            return pltpu.make_async_remote_copy(
                src_ref=src,
                dst_ref=dst,
                send_sem=self.ssem.at[i],
                recv_sem=self.rsem.at[i],
                device_id=(gx, gy, gz),
                device_id_type=MESH,
            )

        src = ref.at[pl.ds(self.first, self.count), tile_rows(start * lv.rows, lv.e * lv.rows), :]
        self.copy_x = copy(src, self.xr, 0, 1 - gx, gy, gz)
        ys = [lax.rem(gy + ny - 1, ny), lax.rem(gy + 1, ny)]
        zs = [lax.rem(gz + nz - 1, nz), lax.rem(gz + 1, nz)]
        targets = [(ys[0], gz), (ys[1], gz), (gy, zs[0]), (gy, zs[1])] + [(y, z) for y in ys for z in zs]
        lands = [1, 0, 3, 2, 7, 6, 5, 4]
        self.copies = [
            copy(
                self.out.at[:, pl.ds(self.starts[i], self.sizes[i]), :],
                self.got.at[:, pl.ds(self.starts[lands[i]], self.sizes[i]), :],
                1,
                gx,
                *targets[i],
            )
            for i in range(8)
        ]
        y_side, z_side = [gy > 0, gy < ny - 1], [gz > 0, gz < nz - 1]
        self.exists = y_side + z_side + [a & b for a in y_side for b in z_side]
        whole = pl.ds(0, self.starts[8])
        self.all = copy(self.out.at[:, whole, :], self.got.at[:, whole, :], 1, gx, *targets[0])
        self.has_y = [jnp.where(gy > 0, 1.0, 0.0).astype(F32), jnp.where(gy < ny - 1, 1.0, 0.0).astype(F32)]
        self.has_z = [jnp.where(gz > 0, 1.0, 0.0).astype(F32), jnp.where(gz < nz - 1, 1.0, 0.0).astype(F32)]
        self.has_x = [gx.astype(F32), (1 - gx).astype(F32)]
        return self

    def send(self, i):
        part = (slice(None), pl.ds(self.starts[i], self.sizes[i]), slice(None))

        @pl.when(self.exists[i])
        def _():
            self.copies[i].start()

        @pl.when(jnp.logical_not(self.exists[i]))
        def _():
            pltpu.make_async_copy(self.out.at[part], self.got.at[part], self.rsem.at[1]).start()
            pltpu.make_async_copy(self.out.at[part], self.spare.at[part], self.ssem.at[1]).start()

    def start_x(self):
        self.copy_x.start()

    def finish_x(self):
        lv, ref = self.level, self.ref
        e, r = lv.e, lv.rows
        self.copy_x.wait()
        low = lanes(r) < 64

        def finish(a, j):
            got = self.xr[a, tile_rows(j * r, r), :]
            if lv.ways == 2:
                got = roll_lanes(got, 64)
                below = roll_lanes(ref[self.first + a, tile_rows((lv.half + j) * r, r), :], 64)
                above = roll_lanes(ref[self.first + a, tile_rows((e + j) * r, r), :], 64)
                below = jnp.where(low, got * self.has_x[0], below)
                above = jnp.where(low, above, got * self.has_x[1])
            else:
                below = got * self.has_x[0]
                above = got * self.has_x[1]
            return below, above

        def body(a, carry):
            for first in range(0, e, 2):
                planes = range(first, min(first + 2, e))
                values = [finish(a, j) for j in planes]
                for j, (below, above) in zip(planes, values):
                    ref[self.first + a, tile_rows(j * r, r), :] = below
                    ref[self.first + a, tile_rows((e + lv.half + j) * r, r), :] = above
            return carry

        lax.fori_loop(0, self.count, body, 0)

    def pack(self, plane, rows, width, shifts, put):
        lv = self.level
        slot = (lanes(rows) % lv.span) // width
        slots = lv.span // width
        for k in range(-(-lv.half // slots)):
            acc = None
            for s in range(min(slots, lv.half - k * slots)):
                moved = [roll_lanes(v, s * width - shift) for v, shift in zip(plane(lv.e + k * slots + s), shifts)]
                acc = moved if s == 0 else [jnp.where(slot == s, new, old) for new, old in zip(moved, acc)]
            put(k, acc)

    def pack_yz(self, send):
        lv, ref = self.level, self.ref
        r, n, e, zo = lv.rows, lv.n, lv.e, lv.zo
        z_shifts = (zo, zo + n - e)

        def put_at(first, rows, a):
            def put(k, values):
                for i, value in enumerate(values):
                    self.out[a, pl.ds(self.starts[first + i] + k * rows, rows), :] = value

            return put

        def edges(a, p):
            return [ref[self.first + a, pl.ds(p * r + row, e), :] for row in (e, n)]

        def pack_d(a, carry):
            def plane(p):
                low, high = edges(a, p)
                return low, low, high, high

            self.pack(plane, e, lv.width, z_shifts * 2, put_at(4, e, a))
            return carry

        def pack_z(a, carry):
            def plane(p):
                return [ref[self.first + a, pl.ds(p * r + e, n), :]] * 2

            self.pack(plane, n, lv.width, z_shifts, put_at(2, n, a))
            return carry

        def pack_y(a, carry):
            if lv.slots_y == 1:
                for k in range(lv.half):
                    put_at(0, e, a)(k, edges(a, e + k))
            else:
                self.pack(lambda p: edges(a, p), e, lv.width_y, (zo, zo), put_at(0, e, a))
            return carry

        for body, which in ((pack_d, range(4, 8)), (pack_z, (2, 3)), (pack_y, (0, 1))):
            lax.fori_loop(0, self.count, body, 0)
            if send:
                for i in which:
                    self.send(i)

    def send_yz(self):
        for i in (4, 5, 6, 7, 2, 3, 0, 1):
            self.send(i)

    def start_yz(self):
        self.pack_yz(True)

    def finish_yz(self):
        lv, ref = self.level, self.ref
        r, n, e, zo = lv.rows, lv.n, lv.e, lv.zo
        with jax.named_scope("arrive"):
            self.all.wait()
        lane = lanes(r) % lv.span
        at_low = (lane >= zo - e) & (lane < zo)
        at_high = (lane >= zo + n) & (lane < zo + n + e)

        def unpack(a, carry):
            def got(i, row, rows):
                return self.got[a, pl.ds(self.starts[i] + row, rows), :]

            for s in range(2):
                for k in range(lv.packs_y):
                    value = got(s, k * e, e) * self.has_y[s]
                    for slot in range(min(lv.slots_y, lv.half - k * lv.slots_y)):
                        row = (e + k * lv.slots_y + slot) * r + (e + n) * s
                        moved = roll_lanes(value, zo - slot * lv.width_y) if lv.slots_y > 1 else value
                        ref[self.first + a, pl.ds(row, e), :] = moved
            for k in range(lv.packs):
                for t in range(2):
                    self.zf[t, a, pl.ds(k * r + e, n), :] = got(2 + t, k * n, n) * self.has_z[t]
                    for s in range(2):
                        both = self.has_y[s] * self.has_z[t]
                        self.zf[t, a, pl.ds(k * r + (e + n) * s, e), :] = got(4 + 2 * s + t, k * e, e) * both
            for k in range(lv.packs):
                sides = [self.zf[t, a, pl.ds(k * r, r), :] for t in range(2)]
                count = min(lv.slots, lv.half - k * lv.slots)
                for first in range(0, count, 4):
                    slots = range(first, min(first + 4, count))
                    values = []
                    for s in slots:
                        value = ref[self.first + a, pl.ds((e + k * lv.slots + s) * r, r), :]
                        value = jnp.where(at_low, roll_lanes(sides[0], zo - e - s * lv.width), value)
                        values.append(jnp.where(at_high, roll_lanes(sides[1], zo + n - s * lv.width), value))
                    for s, value in zip(slots, values):
                        ref[self.first + a, pl.ds((e + k * lv.slots + s) * r, r), :] = value
            return carry

        lax.fori_loop(0, self.count, unpack, 0)


def scaling(lv, fields, inverse, upper, extent):
    r = lv.rows

    def body(p, carry):
        row = pl.multiple_of(p * r, 8)
        cells = fields[3, pl.ds(row, r), :]
        face_z = fields[2, pl.ds(row, r), :]
        total = cells + fields[0, pl.ds(row, r), :] + fields[0, pl.ds(row + r, r), :]
        total = total + fields[1, pl.ds(row, r), :] + fields[1, pl.ds(row + 1, r), :]
        above = roll_lanes(face_z, -1)
        upper[0, pl.ds(row, r), :] = above
        total = total + face_z + above
        inverse[0, pl.ds(row, r), :] = jnp.where(cells > 0.0, 1.0 / total, 0.0)
        return carry

    loop(lv.e - extent, lv.e + lv.half + extent, body, 0, lv.unroll)


def sweep(lv, fields, upper, x, extent, emit, carry=0):
    r = lv.rows
    lo, hi = lv.e - extent, lv.e + lv.half + extent

    def body(p, carry):
        here, flux, kept = carry
        row = pl.multiple_of(p * r, 8)
        after = x[0, pl.ds(row + r, r), :]
        flux_after = fields[0, pl.ds(row + r, r), :] * (after - here)
        flux_y = fields[1, pl.ds(row, r), :] * (here - roll_rows(here, 1))
        flux_y = flux_y - fields[1, pl.ds(row + 1, r), :] * (roll_rows(here, -1) - here)
        flux_z = fields[2, pl.ds(row, r), :] * (here - roll_lanes(here, 1))
        flux_z = flux_z - upper[0, pl.ds(row, r), :] * (roll_lanes(here, -1) - here)
        applied = fields[3, pl.ds(row, r), :] * here + ((flux - flux_after) + flux_y + flux_z)
        return after, flux_after, emit(p, row, here, applied, kept)

    row = lo * r
    here = x[0, pl.ds(row, r), :]
    flux = fields[0, pl.ds(row, r), :] * (here - x[0, pl.ds(row - r, r), :])
    return loop(lo, hi, body, (here, flux, carry), lv.unroll)[2]


def step(lv, fields, inverse, upper, x, out, d, extent, first, coefs, keep):
    r = lv.rows

    def emit(p, row, here, applied, kept):
        scaled = inverse[0, pl.ds(row, r), :] * (fields[4, pl.ds(row, r), :] - applied)
        if first == 0:
            update = scaled * (1.0 / THETA)
        elif first == 1:
            update = coefs[0] * here + coefs[1] * scaled
        else:
            update = coefs[0] * d[0, pl.ds(row, r), :] + coefs[1] * scaled
        if keep:
            d[0, pl.ds(row, r), :] = update
        out[0, pl.ds(row, r), :] = here + update
        return kept

    sweep(lv, fields, upper, x, extent, emit)


def smooth_from_zero(lv, fields, inverse, upper, xa, xb, d, extent):
    r = lv.rows

    def body(p, carry):
        row = pl.multiple_of(p * r, 8)
        xa[0, pl.ds(row, r), :] = inverse[0, pl.ds(row, r), :] * fields[4, pl.ds(row, r), :] * (1.0 / THETA)
        return carry

    loop(lv.e - extent, lv.e + lv.half + extent, body, 0, lv.unroll)
    step(lv, fields, inverse, upper, xa, xb, d, extent - 1, 1, STEP1, True)
    step(lv, fields, inverse, upper, xb, xa, d, extent - 2, 2, STEP2, False)


def smooth(lv, fields, inverse, upper, xa, xb, d, extent):
    step(lv, fields, inverse, upper, xa, xb, d, extent - 1, 0, None, True)
    step(lv, fields, inverse, upper, xb, xa, d, extent - 2, 2, STEP1, True)
    step(lv, fields, inverse, upper, xa, xb, d, extent - 3, 2, STEP2, False)


def coarse_lanes(lv, below, rows, half):
    lane = lanes(rows)
    if below is None:
        cell, at = lane, 0
    else:
        at = (lane // below.span) * 64 if below.ways == 2 else 0
        cell = lane % below.span - below.zo
    if lv.ways == 2 and half is not None:
        at = 64 * half
    inside = (cell >= 0) & (cell < lv.n // 2)
    index = jnp.where(inside, at + lv.zo + 2 * cell, 0)
    return index, inside


def place(lv, below, put, plane, value, pair):
    rows = value.shape[0]
    if pair:
        value = value + roll_lanes(value, -1)
    halves = [None] if below is not None and below.ways == lv.ways else range(lv.ways)
    for half in halves:
        index, inside = coarse_lanes(lv, below, rows, half)
        got = jnp.where(inside, gather_lanes(value, index), 0.0)
        put(plane if half is None else plane + half * (lv.half // 2), got)


def coarsen_fields(lv, below, fields, put):
    n2, e, r = lv.n // 2, lv.e, lv.rows

    def body(i, carry):
        row = (e + 2 * i) * r + e

        def rows(a, plane, odd):
            return fields[a, pl.ds(row + plane * r + odd, n2, stride=2), :]

        put_x = functools.partial(put, 0)
        put_y = functools.partial(put, 1)
        put_z = functools.partial(put, 2)
        put_c = functools.partial(put, 3)
        place(lv, below, put_x, i, (rows(0, 0, 0) + rows(0, 0, 1)) * 0.0625, True)
        place(lv, below, put_y, i, (rows(1, 0, 0) + rows(1, 1, 0)) * 0.0625, True)
        place(lv, below, put_z, i, (rows(2, 0, 0) + rows(2, 0, 1) + rows(2, 1, 0) + rows(2, 1, 1)) * 0.0625, False)
        place(lv, below, put_c, i, (rows(3, 0, 0) + rows(3, 0, 1) + rows(3, 1, 0) + rows(3, 1, 1)) * 0.125, True)
        return carry

    loop(0, lv.half // 2, body, 0, 3)


def restrict(lv, below, fields, upper, x, sums, put):
    r, n2 = lv.rows, lv.n // 2

    def emit(p, row, here, applied, kept):
        sums[0, pl.ds((p - lv.e) * r, r), :] = fields[4, pl.ds(row, r), :] - applied
        return kept

    sweep(lv, fields, upper, x, 0, emit)

    def body(i, carry):
        total = None
        for plane in range(2):
            for odd in range(2):
                part = sums[0, pl.ds((2 * i + plane) * r + lv.e + odd, n2, stride=2), :]
                total = part if total is None else total + part
        place(lv, below, functools.partial(put, 4), i, total * 0.125, True)
        return carry

    loop(0, lv.half // 2, body, 0, 6)


def fields_put(below, fields):
    def put(field, plane, value):
        fields[field, pl.ds((below.e + plane) * below.rows + below.e, below.n), :] = value

    return put


def prolong(lv, above, e, x, reach):
    r, rows = lv.rows, lv.n // 2 + 2 * reach
    lane = lanes(rows)
    cell = lane % 64 - lv.zo + 2 * reach
    inside = (cell >= 0) & (cell < 2 * rows)
    source = above.zo - reach + cell // 2
    if above.ways == 2:
        source = source + (lane // 64) * 64
    source = jnp.where(inside, source, 0)

    def body(i, carry):
        row = (above.e - reach + i) * above.rows + above.e - reach
        value = gather_lanes(e[0, pl.ds(row, rows), :], source)
        if above.ways == 1:
            other = gather_lanes(e[0, pl.ds(row + (lv.half // 2) * above.rows, rows), :], source)
            value = jnp.where(lane < 64, value, other)
        value = jnp.where(inside, value, 0.0)
        for plane in range(2):
            at = (lv.e - 2 * reach + 2 * i + plane) * r + lv.e - 2 * reach
            for odd in range(2):
                where = pl.ds(at + odd, rows, stride=2)
                x[0, where, :] = x[0, where, :] + value
        return carry

    loop(0, lv.half // 2 + 2 * reach, body, 0, 4)


PAD = 8


def row_of(rows):
    return lax.broadcasted_iota(jnp.int32, (rows, 128), 0)


def whole_neighbours(ny, value, rows):
    z, y = row_of(128) % 8, lanes(128) % 6
    out = []
    for g in range(ny):
        here = value(g)
        low_y, high_y = roll_lanes(here, 1), roll_lanes(here, -1)
        if g:
            low_y = jnp.where(y == 0, roll_lanes(value(g - 1), -5), low_y)
        if g + 1 < ny:
            high_y = jnp.where(y == 5, roll_lanes(value(g + 1), 5), high_y)
        low_z = jnp.where(z == 0, rows(g, -3), rows(g, -1))
        high_z = jnp.where(z == 5, rows(g, 3), rows(g, 1))
        out.append((roll_lanes(here, 6), roll_lanes(here, -6), low_y, high_y, low_z, high_z))
    return out


def whole_prepare(ny, fields, coefs, diagonal, inverse):
    z, y, row = row_of(128) % 8, lanes(128) % 6, row_of(128)
    moved = lambda a: whole_neighbours(ny, lambda g: fields(a, g), lambda g, d: roll_rows(fields(a, g), -d))
    high = [[near[1] for near in moved(0)], [near[3] for near in moved(1)], [near[5] for near in moved(2)]]
    for g in range(ny):
        inside = fields(3, g) > 0.0
        high_y = jnp.where(y == 5, 0.0, high[1][g]) if g + 1 == ny else high[1][g]
        high_z = jnp.where(row == 125, 0.0, high[2][g])
        sides = [fields(0, g), high[0][g], fields(1, g), high_y, fields(2, g), high_z]
        total = functools.reduce(lambda a, b: a + b, sides) + fields(3, g)
        scale = jnp.where(inside, 1.0 / total, 0.0)
        diagonal[g] = jnp.where(inside, total, 0.0)
        inverse[g] = scale
        if g == 0:
            sides[2] = jnp.where(y == 0, 0.0, sides[2])
        sides[4] = jnp.where(row == 0, 0.0, sides[4])
        for i in range(6):
            coefs[i, g] = sides[i] * scale


def children(value, axes):
    if "y" in axes:
        value = value + roll_lanes(value, -1)
    if "x" in axes:
        value = value + roll_lanes(value, -6)
    if "z" in axes:
        value = value + roll_rows(value, -1)
    return value


def even_cells():
    row, lane = row_of(128), lanes(128)
    return (row % 2 == 0) & (row % 8 < 6) & (lane % 2 == 0) & ((lane // 6) % 2 == 0) & (lane < 72)


def fold_level(values):
    even = even_cells()
    values = [jnp.where(even, v, 0.0) for v in values]
    both = (values[0] + roll_lanes(values[1], 1)) + (roll_lanes(values[2], 6) + roll_lanes(values[3], 7))
    return both[0:64] + roll_rows(both[64:128], 1)


def unfold_level(value):
    both = jnp.concatenate([value, roll_rows(value, -1)], axis=0)
    even = even_cells()
    return [jnp.where(even, roll_lanes(both, -shift), 0.0) for shift in (0, 1, 6, 7)]


def bottom_neighbours(v):
    row, lane = row_of(64), lanes(64)
    z, y = (row % 8) // 2, (lane % 6) // 2
    odd = lane % 2 == 1
    low_y = jnp.where(y > 0, roll_lanes(v, 2), jnp.where(odd, roll_lanes(v, -3), roll_lanes(v, 1)))
    high_y = jnp.where(y < 2, roll_lanes(v, -2), jnp.where(odd, roll_lanes(v, -1), roll_lanes(v, 3)))
    low_z = jnp.where(z > 0, roll_rows(v, 2), jnp.where(row == 1, roll_rows(v, 5), roll_rows(v, 4)))
    high_z = jnp.where(z < 2, roll_rows(v, -2), jnp.where(row == 60, roll_rows(v, -5), roll_rows(v, -4)))
    return roll_lanes(v, 12), roll_lanes(v, -12), low_y, high_y, low_z, high_z


def bottom_prepare(ny, fields, bottom):
    row, lane = row_of(64), lanes(64)
    y = (lane % 6) // 2
    first = (lane % 2 == 0) & ((lane // 6) % 2 == 0)
    last = (lane % 2 == 1) & ((lane // 6) % 2 == 1)
    faces = []
    for a, axes in enumerate(("yz", "xz", "xy", "xyz")):
        factor = 0.125 if a == 3 else 0.0625
        faces.append(fold_level([children(fields(a, g), axes) * factor for g in range(ny)]))
    inside = faces[3] > 0.0
    high_x = bottom_neighbours(faces[0])[1]
    high_y = jnp.where(last & (y == 2), 0.0, bottom_neighbours(faces[1])[3])
    high_z = jnp.where(row == 61, 0.0, bottom_neighbours(faces[2])[5])
    sides = [faces[0], high_x, faces[1], high_y, faces[2], high_z]
    total = functools.reduce(lambda a, b: a + b, sides) + faces[3]
    sides[2] = jnp.where(first & (y == 0), 0.0, sides[2])
    sides[4] = jnp.where(row == 0, 0.0, sides[4])
    for i, value in enumerate(sides + [total]):
        bottom[i] = jnp.where(inside, value, 0.0)


def coarse_solve(ny, coefs, diagonal, inverse, f, bottom, xa, xb, ds, g3):
    def rows(x, g, offset=0):
        return x[g, pl.ds(PAD + offset, 128)]

    def scaled(x):
        near = whole_neighbours(ny, lambda g: rows(x, g), lambda g, d: rows(x, g, d))
        out = []
        for g in range(ny):
            parts = [coefs[i, g] * near[g][i] for i in range(6)]
            total = ((parts[0] + parts[1]) + (parts[2] + parts[3])) + (parts[4] + parts[5])
            out.append((g3[g] - rows(x, g)) + total)
        return out

    def advance(x, to, coef, first, keep=True):
        for g, value in enumerate(scaled(x)):
            update = value * (1.0 / THETA) if first else coef[0] * ds[g] + coef[1] * value
            if keep:
                ds[g] = update
            to[g, pl.ds(PAD, 128)] = rows(x, g) + update

    for x in (xa, xb):
        for g in range(ny):
            x[g, pl.ds(0, PAD)] = jnp.zeros((PAD, 128), F32)
            x[g, pl.ds(PAD + 128, PAD)] = jnp.zeros((PAD, 128), F32)
    for g in range(ny):
        g3[g] = inverse[g] * f(g)
        ds[g] = g3[g] * (1.0 / THETA)
        xa[g, pl.ds(PAD, 128)] = ds[g]
    advance(xa, xb, STEP1, False)
    advance(xb, xa, STEP2, False, False)
    remainder = scaled(xa)
    r = fold_level([children(remainder[g] * diagonal[g], "xyz") * 0.125 for g in range(ny)])
    r = jnp.where(bottom[6] > 0.0, r, 0.0)

    def total(value):
        value = jnp.sum(value.reshape(8, 8, 128), axis=0)
        return jnp.sum(jnp.sum(value, axis=1, keepdims=True), axis=0, keepdims=True)

    def applied(v):
        near = bottom_neighbours(v)
        parts = [bottom[i] * near[i] for i in range(6)]
        return bottom[6] * v - (((parts[0] + parts[1]) + (parts[2] + parts[3])) + (parts[4] + parts[5]))

    e = jnp.zeros((64, 128), F32)
    p, norm = r, total(r * r)
    for i in range(BOTTOM):
        q = applied(p)
        size = norm / total(p * q)
        e = e + size * p
        if i + 1 < BOTTOM:
            r = r - size * q
            after = total(r * r)
            p = r + after / norm * p
            norm = after
    for g, value in enumerate(unfold_level(e)):
        value = value + roll_lanes(value, 1)
        value = value + roll_lanes(value, 6)
        xa[g, pl.ds(PAD, 128)] = rows(xa, g) + (value + roll_rows(value, 1))
    advance(xa, xb, None, True)
    advance(xb, xa, STEP1, False)
    advance(xa, xb, STEP2, False, False)


def window(lv, gx, gy, gz, ny, xs, padded, turned, corner, x):
    nz = 16
    padded[...] = jnp.zeros_like(padded)
    for g in range(ny):
        padded[g + 1, pl.ds(1, nz)] = xs[g, pl.ds(PAD, 128)].reshape(nz, 8, 128)
    for dy in range(3):
        tiles = padded[gy + dy, pl.ds(gz, 3)].reshape(24, 128)
        tiles = jnp.concatenate([tiles, jnp.zeros((104, 128), F32)], axis=0)
        turned[dy, pl.ds(0, 24), :] = jnp.zeros((24, 128), F32)
        turned[dy, pl.ds(24, 128), :] = tiles.T
    lane = lanes(16)
    cell = lane - lv.zo + 6
    inside = (cell >= 0) & (cell < 24)
    coarse = jnp.where(inside, cell // 2 + 3, 0)
    source = (coarse // 6) * 8 + coarse % 6

    def body(i, carry):
        base = 6 + 36 * gx + 6 * i
        corner[pl.ds(0, 3), :] = turned[0, pl.ds(base + 3, 3), :]
        corner[pl.ds(3, 6), :] = turned[1, pl.ds(base, 6), :]
        corner[pl.ds(9, 3), :] = turned[2, pl.ds(base, 3), :]
        value = jnp.where(inside, gather_lanes(corner[0:16], source), 0.0)[0:12]
        for plane in range(2):
            at = (lv.e - 6 + 2 * i + plane) * lv.rows + lv.e - 6
            for odd in range(2):
                where = pl.ds(at + odd, 12, stride=2)
                x[0, where, :] = x[0, where, :] + value
        return carry

    loop(0, 12, body, 0, 4)


def hops(t, nz):
    return sum(min(d, 4 - d) for d in (t // nz % 4, t % nz // 4, t % 4))


def cycle(ny, nz, names, *refs):
    refs = list(refs)
    right_hbm, faces_hbm, cells_hbm, solution_hbm, residual_hbm, norm_out = refs[:6]
    s = dict(zip(names, refs[6:]))
    gx, gy, gz = lax.axis_index("gx"), lax.axis_index("gy"), lax.axis_index("gz")
    here = (gx, gy, gz, ny, nz)
    scope = jax.named_scope

    loads = [pltpu.make_async_copy(faces_hbm.at[d], s["land"].at[d], s["load_sem"].at[d]) for d in range(3)]
    loads.append(pltpu.make_async_copy(cells_hbm, s["land"].at[3], s["load_sem"].at[3]))
    loads.append(pltpu.make_async_copy(right_hbm, s["land"].at[4], s["load_sem"].at[4]))
    for copy in loads:
        copy.start()

    def other(t):
        return lax.rem(gy + t // nz, ny), lax.rem(gz + t % nz, nz)

    order = sorted(range(1, ny * nz), key=lambda t: -hops(t, nz))
    barrier = pltpu.get_barrier_semaphore()
    with scope("greet"):
        for t in order:
            oy, oz = other(t)
            for ox in (gx, 1 - gx):
                pl.semaphore_signal(barrier, inc=1, device_id=(ox, oy, oz), device_id_type=MESH)
        pl.semaphore_signal(barrier, inc=1, device_id=(1 - gx, gy, gz), device_id_type=MESH)

    f0, f1, f2 = s["f0"], s["f1"], s["f2"]
    ex = {k: Exchange(*v) for k, v in EXCHANGES.items()}
    targets = {"e0a": f0, "e0b": f0, "e0c": f0, "c1": f1, "c2": f2, "e1": f1, "e2": f2, "x0": s["x0a"], "x1": s["x1a"], "x2": s["x2a"]}
    for k, target in targets.items():
        ex[k].bind(here, target, [s[k + str(i)] for i in range(7)])

    def partner(src, dst, i):
        return pltpu.make_async_remote_copy(
            src_ref=src,
            dst_ref=dst,
            send_sem=s["pair_send"].at[i],
            recv_sem=s["pair_recv"].at[i],
            device_id=(1 - gx, gy, gz),
            device_id_type=MESH,
        )

    me = gy * nz + gz

    def spread(src, whole, i):
        def copy(src, dst, oy, oz):
            return pltpu.make_async_remote_copy(
                src_ref=src,
                dst_ref=dst,
                send_sem=s["all_send"].at[i],
                recv_sem=s["all_recv"].at[i],
                device_id=(gx, oy, oz),
                device_id_type=MESH,
            )

        def start():
            for t in order:
                copy(src, whole.at[me], *other(t)).start()

        def finish():
            most = whole.at[pl.ds(0, ny * nz - 1)]
            copy(most, most, *other(1)).wait()

        return start, finish

    block = s["block"]

    def block_put(field, plane, value):
        block[field, pl.ds(plane * 6, 6), :] = value

    for a in range(5):
        with scope("load_wait"):
            loads[a].wait()

        def load(i, carry, a=a):
            first = jnp.pad(s["land"][a, i], ((0, 0), (0, 80)))
            second = jnp.pad(s["land"][a, i + 24], ((0, 0), (0, 80)))
            value = roll_lanes(first, L0.zo) + roll_lanes(second, 64 + L0.zo)
            f0[a, pl.ds((L0.e + i) * L0.rows + L0.e, 48), :] = value
            return carry

        with scope("layout"):
            loop(0, 24, load, 0, 12)

    with scope("e0_pack"):
        ex["e0a"].pack_yz(False)
    with scope("barrier"):
        pl.semaphore_wait(barrier, 2 * ny * nz - 1)
    ex["e0a"].send_yz()
    with scope("e0_start_yz"):
        ex["e0b"].start_yz()
        ex["e0c"].start_yz()
    f1[...] = jnp.zeros_like(f1)
    f2[...] = jnp.zeros_like(f2)
    block[...] = jnp.zeros_like(block)
    with scope("coarsen_0"):
        coarsen_fields(L0, L1, f0, fields_put(L1, f1))
    with scope("c1_pack"):
        ex["c1"].pack_yz(False)
    with scope("coarsen_1"):
        coarsen_fields(L1, L2, f1, fields_put(L2, f2))
    with scope("c2_pack"):
        ex["c2"].pack_yz(False)
    with scope("coarsen_2"):
        coarsen_fields(L2, None, f2, block_put)

    def tile_of(field):
        return roll_lanes(block[field].T[0:8], gx * 36)

    own4, pair4, own1, pair1, own_n = (s[k] for k in ("own4", "pair4", "own1", "pair1", "own_n"))
    for field in range(4):
        own4[field] = tile_of(field)
    pair_coef = partner(own4, pair4, 0)
    pair_coef.start()

    def square(i, carry):
        value = f0[4, pl.ds((L0.e + i) * L0.rows + L0.e, 48), :]
        return carry + value * value

    with scope("square"):
        squares = loop(0, 24, square, jnp.zeros((48, 128), F32), 4)
    for k in ("e0a", "e0b", "e0c"):
        with scope(k + "_finish_yz"):
            ex[k].finish_yz()
        ex[k].start_x()
    ex["c1"].send_yz()
    g4, g1, gn = s["g4"], s["g1"], s["gn"]
    with scope("pair_coef"):
        pair_coef.wait()
    merged = s["merged4"]
    merged[...] = own4[...] + pair4[...]
    mine = pl.ds(2 * gx, 2)
    g4[gy, gz, mine] = merged[mine]
    row, column = gz // 4, gz % 4

    def coef_part(stage):
        if stage == 0:
            return g4.at[gy, gz, mine]
        if stage == 1:
            return g4.at[:, gz, mine]
        return g4.at[:, pl.ds(4 * row, 4), mine]

    def coef_copy(stage, src, oy, oz):
        return pltpu.make_async_remote_copy(
            src_ref=src,
            dst_ref=src,
            send_sem=s["coef_send"].at[stage],
            recv_sem=s["coef_recv"].at[stage],
            device_id=(gx, oy, oz),
            device_id_type=MESH,
        )

    def coef_start(stage):
        for d in (2, 1, 3):
            oy, oz = gy, gz
            if stage == 0:
                oy = lax.rem(gy + d, ny)
            elif stage == 1:
                oz = 4 * row + lax.rem(column + d, 4)
            else:
                oz = lax.rem(gz + 4 * d, nz)
            coef_copy(stage, coef_part(stage), oy, oz).start()

    def coef_wait(stage):
        two = pl.ds(0, 2)
        most = (g4.at[pl.ds(0, 3), 0, two], g4.at[:, pl.ds(0, 3), two], g4.at[:, pl.ds(0, 12), two])[stage]
        coef_copy(stage, most, lax.rem(gy + 1, ny), gz).wait()

    with scope("coef_0"):
        coef_start(0)
    with scope("e0_finish_x"):
        ex["e0a"].finish_x()
        ex["e0b"].finish_x()
    with scope("scaling_0"):
        scaling(L0, f0, s["i0"], s["u0"], 3)
    with scope("e0c_finish_x"):
        ex["e0c"].finish_x()
    with scope("smooth_0"):
        smooth_from_zero(L0, f0, s["i0"], s["u0"], s["x0a"], s["x0b"], s["d0"], 3)
    with scope("restrict_0"):
        restrict(L0, L1, f0, s["u0"], s["x0a"], s["sums"], fields_put(L1, f1))
    with scope("e1_start_yz"):
        ex["e1"].start_yz()
    ex["c2"].send_yz()
    with scope("c1_finish_yz"):
        ex["c1"].finish_yz()
    ex["c1"].start_x()
    with scope("coef_1"):
        coef_wait(0)
        coef_start(1)
    with scope("x0_start_yz"):
        ex["x0"].start_yz()
    with scope("c1_finish_x"):
        ex["c1"].finish_x()
    with scope("e1_finish_yz"):
        ex["e1"].finish_yz()
    ex["e1"].start_x()
    with scope("scaling_1"):
        scaling(L1, f1, s["i1"], s["u1"], 4)
    with scope("e1_finish_x"):
        ex["e1"].finish_x()
    with scope("coef_2"):
        coef_wait(1)
        coef_start(2)
    with scope("smooth_1"):
        smooth_from_zero(L1, f1, s["i1"], s["u1"], s["x1a"], s["x1b"], s["d1"], 3)
    with scope("restrict_1"):
        restrict(L1, L2, f1, s["u1"], s["x1a"], s["sums"], fields_put(L2, f2))
    with scope("e2_start_yz"):
        ex["e2"].start_yz()
    with scope("c2_finish_yz"):
        ex["c2"].finish_yz()
    ex["c2"].start_x()
    with scope("x1_start_yz"):
        ex["x1"].start_yz()
    with scope("c2_finish_x"):
        ex["c2"].finish_x()
    other_half = pltpu.make_async_remote_copy(
        src_ref=g4.at[:, :, mine],
        dst_ref=g4.at[:, :, mine],
        send_sem=s["pair_send"].at[3],
        recv_sem=s["pair_recv"].at[3],
        device_id=(1 - gx, gy, gz),
        device_id_type=MESH,
    )
    with scope("e2_finish_yz"):
        ex["e2"].finish_yz()
    ex["e2"].start_x()
    with scope("x0_finish_yz"):
        ex["x0"].finish_yz()
    with scope("scaling_2"):
        scaling(L2, f2, s["i2"], s["u2"], 5)
    with scope("e2_finish_x"):
        ex["e2"].finish_x()
    with scope("smooth_2"):
        smooth_from_zero(L2, f2, s["i2"], s["u2"], s["x2a"], s["x2b"], s["d2"], 3)
    with scope("restrict_2"):
        restrict(L2, None, f2, s["u2"], s["x2a"], s["sums"], block_put)
    own1[...] = tile_of(4)
    pair_source = partner(own1, pair1, 1)
    pair_source.start()
    ex["x0"].start_x()
    with scope("x2_start_yz"):
        ex["x2"].start_yz()
    with scope("pair_source"):
        pair_source.wait()
    s["merged1"][...] = own1[...] + pair1[...]
    g1[me] = s["merged1"][...]
    source_start, source_finish = spread(s["merged1"], g1, 1)
    with scope("source_start"):
        source_start()
    with scope("coef_finish"):
        coef_wait(2)
    other_half.start()
    with scope("hidden_1"):
        ex["x1"].finish_yz()
        ex["x1"].start_x()
        ex["x0"].finish_x()
    with scope("other_half"):
        other_half.wait()
    gathered = lambda a, g: g4[g, :, a].reshape(128, 128)
    with scope("coarse_fields"):
        whole_prepare(ny, gathered, s["c3"], s["w3"], s["i3"])
        bottom_prepare(ny, gathered, s["bottom"])
    with scope("hidden_2"):
        ex["x1"].finish_x()
        ex["x2"].finish_yz()
        ex["x2"].start_x()
    with scope("source_finish"):
        source_finish()
    with scope("coarse_solve"):
        source = lambda g: g1[pl.ds(g * nz, nz)].reshape(128, 128)
        whole = [s[k] for k in ("c3", "w3", "i3")]
        coarse_solve(ny, *whole, source, s["bottom"], s["x3a"], s["x3b"], s["d3"], s["g3"])
    with scope("x2_finish_x"):
        ex["x2"].finish_x()
    with scope("window"):
        window(L2, gx, gy, gz, ny, s["x3b"], s["padded"], s["turned"], s["corner"], s["x2a"])
    with scope("post_2"):
        smooth(L2, f2, s["i2"], s["u2"], s["x2a"], s["x2b"], s["d2"], 6)
    with scope("prolong_1"):
        prolong(L1, L2, s["x2b"], s["x1a"], 3)
    with scope("post_1"):
        smooth(L1, f1, s["i1"], s["u1"], s["x1a"], s["x1b"], s["d1"], 5)
    with scope("prolong_0"):
        prolong(L0, L1, s["x1b"], s["x0a"], 2)
    with scope("post_0"):
        smooth(L0, f0, s["i0"], s["u0"], s["x0a"], s["x0b"], s["d0"], 4)

    land = s["land"]
    r0 = L0.rows
    lane48 = lanes(48) % 64
    inside = (lane48 >= L0.zo) & (lane48 < L0.zo + 48)

    def final(p, row, here_x, applied, kept):
        s["sums"][0, pl.ds((p - L0.e) * r0, r0), :] = f0[4, pl.ds(row, r0), :] - applied
        return kept

    with scope("final"):
        sweep(L0, f0, s["u0"], s["x0b"], 0, final)

    def out_square(i, carry):
        value = jnp.where(inside, s["sums"][0, pl.ds(i * r0 + L0.e, 48), :], 0.0)
        return carry + value * value

    with scope("square"):
        ends = loop(0, 24, out_square, jnp.zeros((48, 128), F32), 4)

    def fold(value):
        return jnp.sum(value, axis=0, keepdims=True)

    def squares_of(value):
        return jnp.sum(fold(value), axis=1, keepdims=True)

    lane1 = lax.broadcasted_iota(jnp.int32, (1, 128), 1)
    pair = jnp.where(lane1 == 0, squares_of(squares), jnp.where(lane1 == 1, squares_of(ends), 0.0))
    own_n[...] = pair
    mine_n = gx * (ny * nz) + me
    gn[mine_n] = pair

    def norm_copy(src, dst, ox, oy, oz):
        return pltpu.make_async_remote_copy(
            src_ref=src,
            dst_ref=dst,
            send_sem=s["all_send"].at[2],
            recv_sem=s["all_recv"].at[2],
            device_id=(ox, oy, oz),
            device_id_type=MESH,
        )

    with scope("norm_start"):
        for t in order:
            for ox in (gx, 1 - gx):
                norm_copy(own_n, gn.at[mine_n], ox, *other(t)).start()
        norm_copy(own_n, gn.at[mine_n], 1 - gx, gy, gz).start()

    def unload(slot, i, value):
        for half in range(2):
            moved = roll_lanes(value, -(L0.zo + 64 * half))
            land[slot, i + 24 * half] = moved[:, 0:48]

    def out_solution(i, carry):
        unload(0, i, s["x0b"][0, pl.ds((L0.e + i) * r0 + L0.e, 48), :])
        return carry

    def out_residual(i, carry):
        unload(1, i, s["sums"][0, pl.ds(i * r0 + L0.e, 48), :])
        return carry

    with scope("unload_solution"):
        loop(0, 24, out_solution, 0, 6)
    out0 = pltpu.make_async_copy(land.at[0], solution_hbm, s["out_sem"].at[0])
    out0.start()
    with scope("unload_residual"):
        loop(0, 24, out_residual, 0, 6)
    out1 = pltpu.make_async_copy(land.at[1], residual_hbm, s["out_sem"].at[1])
    out1.start()
    with scope("norm_finish"):
        most = gn.at[pl.ds(0, 2 * ny * nz - 1)]
        norm_copy(most, most, 1 - gx, gy, gz).wait()
    sums = jnp.sum(gn[...], axis=0)
    norm = jnp.sqrt(sums[:, 1:2] / sums[:, 0:1])
    norm_out[0, 0] = norm[0, 0]
    with scope("out_wait"):
        out0.wait()
        out1.wait()


EXCHANGES = {
    "e0a": (L0, 0, 2),
    "e0b": (L0, 2, 2),
    "e0c": (L0, 4, 1),
    "c1": (L1, 0, 4),
    "c2": (L2, 0, 4),
    "e1": (L1, 4, 1),
    "e2": (L2, 4, 1),
    "x0": (L0, 0, 1),
    "x1": (L1, 0, 1),
    "x2": (L2, 0, 1),
}


def scratch_of(ny, nz):
    vmem = lambda *shape: pltpu.VMEM(shape, F32)
    size = lambda lv: lv.planes * lv.rows + 16
    scratch = {"land": vmem(5, 48, 48, 48), "load_sem": pltpu.SemaphoreType.DMA((5,)), "out_sem": pltpu.SemaphoreType.DMA((2,))}
    for i, lv in enumerate((L0, L1, L2)):
        scratch[f"f{i}"] = vmem(5, size(lv), 128)
        for k in ("i", "d", "u"):
            scratch[f"{k}{i}"] = vmem(1, size(lv), 128)
        scratch[f"x{i}a"] = vmem(1, size(lv), 128)
        scratch[f"x{i}b"] = vmem(1, size(lv), 128)
    scratch["sums"] = vmem(1, 24 * 56 + 16, 128)
    scratch["block"] = vmem(5, 128, 128)
    for k in ("own4", "pair4", "merged4"):
        scratch[k] = vmem(4, 8, 128)
    for k in ("own1", "pair1", "merged1"):
        scratch[k] = vmem(8, 128)
    scratch["g4"] = vmem(ny, nz, 4, 8, 128)
    scratch["g1"] = vmem(ny * nz, 8, 128)
    scratch["gn"] = vmem(2 * ny * nz, 1, 128)
    scratch["own_n"] = vmem(1, 128)
    for k in ("pair_send", "pair_recv"):
        scratch[k] = pltpu.SemaphoreType.DMA((4,))
    for k in ("all_send", "all_recv", "coef_send", "coef_recv"):
        scratch[k] = pltpu.SemaphoreType.DMA((3,))
    for k in ("i3", "w3", "d3", "g3"):
        scratch[k] = vmem(ny, 128, 128)
    for k in ("x3a", "x3b"):
        scratch[k] = vmem(ny, 128 + 2 * PAD, 128)
    scratch["c3"] = vmem(6, ny, 128, 128)
    scratch["bottom"] = vmem(7, 64, 128)
    scratch["padded"] = vmem(ny + 2, nz + 2, 8, 128)
    scratch["turned"] = vmem(3, 160, 128)
    scratch["corner"] = vmem(24, 128)
    for k, v in EXCHANGES.items():
        for i, shape in enumerate(Exchange(*v).scratch()):
            scratch[k + str(i)] = shape
    return scratch


def solution(mesh):
    ny, nz = mesh.shape["gy"], mesh.shape["gz"]
    scratch = scratch_of(ny, nz)

    def shards(right_side, face_coef, absorption):
        field = jax.ShapeDtypeStruct((48, 48, 48), F32)
        solved, residual, norm = pl.pallas_call(
            functools.partial(cycle, ny, nz, tuple(scratch)),
            out_shape=(pltpu.VMEM((48, 48, 48), F32), pltpu.VMEM((48, 48, 48), F32), jax.ShapeDtypeStruct((1, 1), F32)),
            in_specs=[pl.BlockSpec(memory_space=pltpu.HBM)] * 3,
            out_specs=(
                pl.BlockSpec(memory_space=pl.ANY),
                pl.BlockSpec(memory_space=pl.ANY),
                pl.BlockSpec(memory_space=pltpu.SMEM),
            ),
            scratch_shapes=list(scratch.values()),
            compiler_params=pltpu.CompilerParams(
                collective_id=0, has_side_effects=True, vmem_limit_bytes=57000 * 1024
            ),
        )(right_side, face_coef, absorption)
        return solved, residual, norm[0, 0]

    in_specs = (P("gx", "gy", "gz"), P(None, "gx", "gy", "gz"), P("gx", "gy", "gz"))
    out_specs = (P("gx", "gy", "gz"), P("gx", "gy", "gz"), P())
    return jax.shard_map(shards, mesh=mesh, in_specs=in_specs, out_specs=out_specs, check_vma=False)
```
